256 devices in a mesh: tile: 32 (over y, z_lo, core), depth: 8 (over z_hi, x).
Axes of the slice: x: 4, y: 4, z: 8 (z_hi: 2, z_lo: 4; z = z_hi * 4 + z_lo), core: 2. Of those that a mesh axis runs over, the one named last changes fastest.
Arguments:
- volume: float32 [64, 64, 256, 256], P('tile', 'depth'), may hold values from 0 to 1
- transfer: float32 [64, 2, 256, 256], P('depth', None, 'tile'), may hold values from -0.9 to 0.9
- measured: float32 [64, 256, 256], P('tile'), may hold values from 0.5 to 4
- background: float32 [64, 256, 256], P('tile'), may hold values from 1 to 4
- margins: int32 [64], replicated, may hold values from 8 to 32
- phases: int32 [64], P('depth'), may hold values from 0 to 255
Outputs:
- blended: float32 [64, 64, 256, 256], P('tile', 'depth')
The draws below stay inside these ranges and needn't reach their ends.
All inputs are finite; a program needn't handle non-finite values.
Results may differ from the reference program's by a relative error of at most 0.00005.
Values sent between devices are 32-bit elements; how exact they have to be, the bound alone decides.
A program may use at most 128 MiB of HBM per device.

```python
import math
import jax
import jax.numpy as jnp
from jax import lax

TILE_N = 256
INTERSECTION = 32
TILES = 64
PLANES = 64


def place_ends(values, own_key, least, largest):
    shape = values.shape
    place = [jax.random.randint(jax.random.fold_in(own_key, axis), (), 0, shape[axis]) for axis in range(len(shape))]
    values = values.at[tuple(place)].set(least)
    longest = shape.index(max(shape))
    place[longest] = (place[longest] + 1) % shape[longest]
    return values.at[tuple(place)].set(largest)


def steps_of(own_key, extent, pieces, least, high):
    factor_of, own = 1.0, jax.random.fold_in(own_key, 6)
    for axis_at, blocks in pieces:
        steps = jnp.exp(jax.random.uniform(jax.random.fold_in(own, axis_at), (blocks,), jnp.float32, least / len(pieces), high / len(pieces)))
        factor_of = factor_of * jnp.repeat(steps, extent[axis_at] // blocks).reshape([-1 if axis == axis_at else 1 for axis in range(len(extent))])
    return factor_of


def gaussian(stream_key, shape, deviation, reach, shards=(), held_as=jnp.bfloat16):
    loudness = steps_of(stream_key, shape, shards, -0.22, 0.18) if shards else 1.0
    array = jax.random.normal(stream_key, shape, jnp.float32) * deviation * loudness
    return jnp.minimum(jnp.maximum(array, -reach), reach).astype(held_as)


def setup_inputs(seed: int = 0) -> dict:
    splits = jax.random.split(jax.random.key(seed), 7)
    volume = jnp.clip(1.0 * jax.random.uniform(splits[0], (TILES, PLANES, TILE_N, TILE_N), jnp.float32) ** steps_of(splits[0], (TILES, PLANES, TILE_N, TILE_N), ((0, 32), (1, 8)), -0.2, 0.2), 0.0, 1.0)
    transfer = gaussian(splits[1], (PLANES, 2, TILE_N, TILE_N), 0.15, 0.9, ((0, 8), (2, 32)), jnp.float32)
    measured = jnp.clip(jnp.exp(math.log(4.0) - 2.0794415 * jax.random.uniform(splits[2], (TILES, TILE_N, TILE_N), jnp.float32) ** steps_of(splits[2], (TILES, TILE_N, TILE_N), ((0, 32),), -0.2, 0.2)), 0.5, 4.0)
    background = jnp.clip(jnp.exp(math.log(4.0) - 1.3862944 * jax.random.uniform(splits[3], (TILES, TILE_N, TILE_N), jnp.float32) ** steps_of(splits[3], (TILES, TILE_N, TILE_N), ((0, 32),), -0.2, 0.2)), 1.0, 4.0)
    margins = place_ends(jax.random.randint(splits[4], (TILES,), INTERSECTION // 4, INTERSECTION + 1), jax.random.fold_in(splits[4], 1), INTERSECTION // 4, INTERSECTION).astype(jnp.int32)
    phases = place_ends(jax.random.randint(splits[5], (PLANES,), 0, TILE_N), jax.random.fold_in(splits[5], 1), 0, TILE_N - 1).astype(jnp.int32)
    return dict(volume=volume, transfer=transfer, measured=measured, background=background, margins=margins, phases=phases)


floor_level = 0.5
step_gain = 2.0


def shifted_table(transfer, phases):
    side = TILE_N
    columns = jnp.arange(side, dtype=jnp.int32)
    angle = ((phases[:, None] * columns[None, :]) % side).astype(jnp.float32) * (2.0 * math.pi / side)
    rotor = jnp.cos(angle) - 1j * jnp.sin(angle)
    return (transfer[:, 0] + 1j * transfer[:, 1]) * rotor[:, None, :]


def ramp_weights(margin_values):
    width = INTERSECTION
    offsets = jnp.arange(width, dtype=jnp.float32)
    margin_float = margin_values.astype(jnp.float32)[:, None]
    return jnp.clip((offsets[None, :] + 0.5 - (width - margin_float) / 2.0) / margin_float, 0.0, 1.0)


def reference(volume, transfer, measured, background, margins, phases):
    side = TILE_N
    width = INTERSECTION
    shifted = shifted_table(transfer, phases)

    def one_tile(operands):
        volume_tile, measured_tile, background_tile = operands
        spectra = jnp.fft.fft2(volume_tile)
        spectrum = jnp.sum(spectra * shifted, axis=0)
        projection = background_tile + jnp.real(jnp.fft.ifft2(spectrum))
        ratio = measured_tile / jnp.maximum(projection, floor_level)
        ratio_spectrum = jnp.fft.fft2(ratio - 1.0)
        correction = jnp.real(jnp.fft.ifft2(jnp.conj(shifted) * ratio_spectrum[None]))
        return jnp.maximum(volume_tile * (1.0 + step_gain * correction), 0.0)

    updated = lax.map(one_tile, (volume, measured, background))
    bottoms = updated[:, :, side - width:]
    tops = updated[:, :, :width]
    next_tops = jnp.roll(tops, -1, axis=0)
    prev_bottoms = jnp.roll(bottoms, 1, axis=0)
    weight_own = ramp_weights(margins)[:, None, :, None]
    weight_prev = ramp_weights(jnp.roll(margins, 1))[:, None, :, None]
    new_bottom = (1.0 - weight_own) * bottoms + weight_own * next_tops
    new_top = (1.0 - weight_prev) * prev_bottoms + weight_prev * tops
    return jnp.concatenate([new_top, updated[:, :, width:side - width], new_bottom], axis=2)
```

```python
import functools
import math

import jax
import jax.numpy as jnp
import numpy as np
from jax import lax
from jax.experimental import pallas as pl
from jax.experimental.pallas import tpu as pltpu
from jax.sharding import PartitionSpec as P

SIDE = 256
HALF = 128
WIDTH = 32
TILES = 64
LOCAL_TILES = 2
LOCAL_PLANES = 8
SUBS = 2
SUB_ROWS = 128 // SUBS
FLOOR_LEVEL = 0.5
STEP_GAIN = 2.0
MESH = pl.DeviceIdType.MESH
f32 = jnp.float32
bf16 = jnp.bfloat16


def packed_tables():
    place = np.arange(SIDE)
    table = np.zeros((SIDE, SIDE))
    for a in range(HALF):
        table[a] = np.cos(2 * np.pi * (a * place % SIDE) / SIDE)
    table[HALF] = 1.0 - 2.0 * (place % 2)
    for a in range(1, HALF):
        table[HALF + a] = np.sin(2 * np.pi * (a * place % SIDE) / SIDE)
    weight = np.full(SIDE, 2.0)
    weight[0] = weight[HALF] = 1.0
    inverse = table.T * weight / SIDE
    pieces = []
    for matrix in (table, table.T, inverse, inverse.T):
        high = matrix.astype(bf16)
        pieces += [high, (matrix - high.astype(np.float64)).astype(bf16)]
    return jnp.asarray(np.stack(pieces))


def pairing():
    move = np.zeros((HALF, HALF), np.float32)
    move[0, 0] = 1.0
    for b in range(1, HALF):
        move[HALF - b, b] = 1.0
    return jnp.asarray(move.astype(bf16))


def split(values):
    high = values.astype(bf16)
    return high, (values - high.astype(f32)).astype(bf16)


def dot(a, b):
    return jnp.dot(a, b, preferred_element_type=f32)


def dot3(a, b):
    return dot(a[0], b[0]) + dot(a[1], b[0]) + dot(a[0], b[1])


def special(shape, first):
    lane0 = lax.broadcasted_iota(jnp.int32, shape, 1) == 0
    row0 = None
    if first:
        row0 = jnp.logical_and(
            lax.broadcasted_iota(jnp.int32, shape, 0) == 0, jnp.logical_not(lane0)
        )
    return lane0, row0


def quads_in(cc, cs, sc, ss, first):
    lane0, row0 = special(cc.shape, first)
    pr, pi, mr, mi = cc - ss, cs + sc, cc + ss, cs - sc
    if first:
        pr = jnp.where(row0, cc, pr)
        pi = jnp.where(row0, cs, pi)
        mr = jnp.where(row0, sc, mr)
        mi = jnp.where(row0, ss, mi)
    return (
        jnp.where(lane0, cc, pr),
        jnp.where(lane0, sc, pi),
        jnp.where(lane0, cs, mr),
        jnp.where(lane0, ss, mi),
    )


def quads_out(pr, pi, mr, mi, first):
    lane0, row0 = special(pr.shape, first)
    cc, ss, cs, sc = pr + mr, mr - pr, pi + mi, pi - mi
    if first:
        cc = jnp.where(row0, pr, cc)
        cs = jnp.where(row0, pi, cs)
        sc = jnp.where(row0, mr, sc)
        ss = jnp.where(row0, mi, ss)
    return (
        jnp.where(lane0, pr, cc),
        jnp.where(lane0, mr, cs),
        jnp.where(lane0, pi, sc),
        jnp.where(lane0, mi, ss),
    )


def times(hr, hi, real, imag, first, conj):
    second = hr
    if first:
        lane0, _ = special(hr.shape, False)
        corner = jnp.logical_and(lane0, lax.broadcasted_iota(jnp.int32, hr.shape, 0) == 0)
        second = jnp.where(corner, hi, hr)
        hi = jnp.where(corner, 0.0, hi)
    if conj:
        return hr * real - hi * imag, second * imag + hi * real
    return hr * real + hi * imag, second * imag - hi * real


def ramp(margin):
    margin = margin.astype(f32)
    row = lax.broadcasted_iota(jnp.int32, (WIDTH, SIDE), 0).astype(f32)
    return jnp.clip((row + 0.5 - (WIDTH - margin) / 2.0) / margin, 0.0, 1.0)


def kernel(
    phases,
    margins,
    transfer,
    volume_hbm,
    measured_hbm,
    background_hbm,
    mats_hbm,
    pair_ref,
    out_hbm,
    vol,
    packed,
    table,
    mats,
    measured,
    background,
    halves,
    mine,
    other,
    other0,
    pos,
    neg,
    sums,
    image,
    scattered,
    zsend,
    zrecv,
    ratio,
    ratio_quads,
    quads,
    part_high,
    part_low,
    top_send,
    bottom_send,
    after_recv,
    before_recv,
    vol_sem,
    in_sem,
    ex_send,
    ex_recv,
    ag_send,
    ag_recv,
    rs_send,
    rs_recv,
    z_send,
    z_recv,
    xg_send,
    xg_recv,
    halo_send,
    halo_recv,
    out_sem,
):
    tile = lax.axis_index("tile")
    depth = lax.axis_index("depth")
    core = lax.rem(tile, 2)
    zlo = lax.rem(tile // 2, 4)
    yrow = tile // 8
    xpos = lax.rem(depth, 4)
    zhi = depth // 4
    negative = tile >= 16
    block = jnp.where(negative, 31 - tile, tile)

    def at(y, z, c):
        return lax.rem(y, 4) * 8 + lax.rem(z, 4) * 2 + c

    def xpeer(d):
        return zhi * 4 + lax.rem(xpos + d, 4)

    after = lax.rem(tile + 1, 32)
    before = lax.rem(tile + 31, 32)
    zpartner = (1 - zhi) * 4 + xpos

    volume_copies = []
    for p in range(LOCAL_PLANES):
        volume_copies.append(
            pltpu.make_async_copy(volume_hbm.at[:, p], vol.at[:, p], vol_sem.at[p])
        )
    local = [
        pltpu.make_async_copy(mats_hbm, mats, in_sem.at[0]),
        pltpu.make_async_copy(measured_hbm, measured, in_sem.at[1]),
        pltpu.make_async_copy(background_hbm, background, in_sem.at[2]),
    ]
    local[0].start()
    for copy in volume_copies:
        copy.start()
    local[1].start()
    local[2].start()

    barrier = pltpu.get_barrier_semaphore()

    def greet(t, d):
        pl.semaphore_signal(barrier, inc=1, device_id=(t, d), device_id_type=MESH)

    greet(31 - tile, depth)
    for dz in range(1, 4):
        greet(at(yrow, zlo + dz, core), depth)
    greet(at(yrow + 1, zlo, core), depth)
    greet(at(yrow + 3, zlo, core), depth)
    greet(at(yrow, zlo, 1 - core), depth)
    for d in range(1, 4):
        greet(tile, xpeer(d))
    greet(tile, zpartner)
    greet(after, depth)
    greet(before, depth)
    first_of = lax.rem(32 - tile, 16)
    last_to = jnp.where(tile == 16, 31, tile - 1)
    last_from = jnp.where(tile == 31, 16, tile + 1)
    row0_from = jnp.where(tile == 0, 16, 32 - tile)

    @pl.when(negative)
    def _():
        greet(first_of, depth)
        greet(last_to, depth)
        greet(last_from, depth)

    @pl.when(jnp.logical_not(negative))
    def _():
        greet(row0_from, depth)

    whole = transfer[...].reshape(LOCAL_PLANES * 2 * 8, SIDE)
    halves[0] = whole[:, :HALF]
    rest = whole[:, HALF:]
    high, low = split(rest)
    lowest = ((rest - high.astype(f32)) - low.astype(f32)).astype(bf16)
    move = pair_ref[...]
    halves[1] = dot(high, move) + dot(low, move) + dot(lowest, move)
    for r in range(8):
        to = jnp.where(negative, (8 - r) % 8, r)
        for ph in range(2):
            for e in range(2):
                for c in range(2):
                    piece = halves[e, pl.ds(ph * 64 + c * 8 + r, 4, stride=16), :]
                    mine[ph, to, pl.ds((e * 2 + c) * 4, 4), :] = piece

    pl.semaphore_wait(barrier, 14 + 2 * (tile // 16))

    def remote(src, dst, send, recv, t, d):
        return pltpu.make_async_remote_copy(
            src_ref=src,
            dst_ref=dst,
            send_sem=send,
            recv_sem=recv,
            device_id=(t, d),
            device_id_type=MESH,
        )

    rows7 = pl.ds(1, 7)
    row1 = pl.ds(0, 1)
    up_all = remote(mine.at[1], other, ex_send.at[0], ex_recv.at[0], 31 - tile, depth)
    down_rest = remote(
        mine.at[0, rows7], other.at[rows7], ex_send.at[0], ex_recv.at[0], 31 - tile, depth
    )
    down_first = remote(
        mine.at[0, row1], other.at[row1], ex_send.at[1], ex_recv.at[1], first_of, depth
    )
    down_last = remote(mine.at[1, row1], other0, ex_send.at[2], ex_recv.at[1], last_to, depth)

    @pl.when(jnp.logical_not(negative))
    def _():
        up_all.start()

    @pl.when(negative)
    def _():
        down_rest.start()
        down_first.start()
        down_last.start()

    left = lambda: (mats[0], mats[1])
    right = lambda: (mats[2], mats[3])
    inv_left = lambda: (mats[4], mats[5])
    inv_right = lambda: (mats[6], mats[7])
    local[0].wait()

    def forward(p, carry):
        pltpu.make_async_copy(volume_hbm.at[:, p], vol.at[:, p], vol_sem.at[p]).wait()
        for t in range(LOCAL_TILES):
            half = dot3(split(vol[t, p]), right())
            packed[t, p] = dot3(left(), split(half))
        return carry

    lax.fori_loop(0, 4, forward, 0)

    @pl.when(jnp.logical_not(negative))
    def _():
        down_rest.wait_recv()
        down_first.wait_recv()
        pos[...] = mine[0]
        neg[...] = other[...]

    @pl.when(negative)
    def _():
        up_all.wait_recv()
        down_last.wait_recv()
        pos[...] = other[...]
        neg[0] = other0[0]
        neg[1:8] = mine[1, 1:8]

    plane0 = jnp.where(negative, 4, 0)
    column = lax.broadcasted_iota(jnp.int32, (4, HALF), 1)
    row4 = lax.broadcasted_iota(jnp.int32, (4, HALF), 0)
    phase = jnp.zeros((4, HALF), jnp.int32)
    for q in range(4):
        phase = jnp.where(row4 == q, phases[plane0 + q], phase)
    lane0 = column == 0

    def rotor(columns):
        angle = ((phase * columns) & (SIDE - 1)).astype(f32) * (2.0 * math.pi / SIDE)
        return jnp.cos(angle), jnp.sin(angle)

    cos_p, sin_p = rotor(column)
    cos_m, sin_m = rotor(jnp.where(lane0, HALF, column))
    sin_m = jnp.where(lane0, 0.0, sin_m)
    is_first = block == 0
    for r in range(8):
        epr, epi, fpr, fpi = (pos[r, pl.ds(c * 4, 4), :] for c in range(4))
        enr, eni, fnr, fni = (neg[r, pl.ds(c * 4, 4), :] for c in range(4))
        hpr, hpi = 0.25 * (epr + fnr), 0.25 * (epi - fni)
        hmr, hmi = 0.25 * (enr + fpr), 0.25 * (eni - fpi)
        if r == 0:
            at0 = jnp.logical_and(is_first, jnp.logical_not(lane0))
            hpr = jnp.where(at0, 0.5 * (epr + fpr), hpr)
            hpi = jnp.where(at0, 0.5 * (epi - fpi), hpi)
            hmr = jnp.where(at0, 0.5 * (enr + fnr), hmr)
            hmi = jnp.where(at0, 0.5 * (eni - fni), hmi)
        lpr, lpi = 0.5 * (epr + enr), 0.5 * (epi - eni)
        lmr, lmi = 0.5 * (fpr + fnr), 0.5 * (fpi - fni)
        if r == 0:
            lpr, lpi = jnp.where(is_first, epr, lpr), jnp.where(is_first, enr, lpi)
            lmr, lmi = jnp.where(is_first, fpr, lmr), jnp.where(is_first, fnr, lmi)
        hpr, hpi = jnp.where(lane0, lpr, hpr), jnp.where(lane0, lpi, hpi)
        hmr, hmi = jnp.where(lane0, lmr, hmr), jnp.where(lane0, lmi, hmi)
        parts = (
            hpr * cos_p + hpi * sin_p,
            hpi * cos_p - hpr * sin_p,
            hmr * cos_m + hmi * sin_m,
            hmi * cos_m - hmr * sin_m,
        )
        for c in range(4):
            for q in range(4):
                table[tile, q, c, pl.ds(r, 1), :] = parts[c][q : q + 1]

    started = []

    def pass_on(which, t):
        copy = remote(
            table.at[which],
            table.at[which],
            ag_send.at[len(started)],
            ag_recv.at[which],
            t,
            depth,
        )
        copy.start()
        started.append(copy)

    def arrived(which):
        remote(
            table.at[which], table.at[which], ag_send.at[0], ag_recv.at[which], tile, depth
        ).wait_recv()

    above = at(yrow + 1, zlo, core)
    below = at(yrow + 3, zlo, core)
    sibling = at(yrow, zlo, 1 - core)
    z_order = (1, 3, 2)
    pass_on(tile, above)
    pass_on(tile, below)
    for dz in z_order:
        pass_on(tile, at(yrow, zlo + dz, core))
    pass_on(tile, sibling)

    lax.fori_loop(4, 6, forward, 0)

    for dz in z_order:
        which = at(yrow, zlo + dz, core)
        arrived(which)
        pass_on(which, above)
        pass_on(which, below)
        pass_on(which, sibling)

    lax.fori_loop(6, 8, forward, 0)

    for dz in (0, 1, 3, 2):
        which = at(yrow + 3, zlo + dz, core)
        arrived(which)
        if dz in (0, 1):
            pass_on(which, above)
        pass_on(which, sibling)
        which = at(yrow + 1, zlo + dz, core)
        arrived(which)
        if dz in (2, 3):
            pass_on(which, below)
        pass_on(which, sibling)
    for dz in (0, 1, 3, 2):
        which = at(yrow + 2, zlo + dz, core)
        arrived(which)
        pass_on(which, sibling)
    for dy in range(4):
        for dz in range(4):
            arrived(at(yrow + dy, zlo + dz, 1 - core))

    def read_quads(ref, rows, rows2):
        return (
            ref[rows, pl.ds(0, HALF)],
            ref[rows, pl.ds(HALF, HALF)],
            ref[rows2, pl.ds(0, HALF)],
            ref[rows2, pl.ds(HALF, HALF)],
        )

    def rows_of(k):
        if isinstance(k, int):
            return pl.ds(8 * k, 8), pl.ds(HALF + 8 * k, 8)
        return pl.ds(pl.multiple_of(8 * k, 8), 8), pl.ds(pl.multiple_of(HALF + 8 * k, 8), 8)

    def table_of(p, k):
        which = k if p < 4 else 31 - k
        return tuple(table[which, p % 4, c] for c in range(4))

    def spectrum_block(t, k, first):
        rows, rows2 = rows_of(k)
        total = None
        for p in range(LOCAL_PLANES):
            hpr, hpi, hmr, hmi = table_of(p, k)
            pr, pi, mr, mi = quads_in(*read_quads(packed.at[t, p], rows, rows2), first)
            terms = times(hpr, hpi, pr, pi, first, False) + times(hmr, hmi, mr, mi, first, False)
            total = terms if total is None else tuple(a + b for a, b in zip(total, terms))
        cc, cs, sc, ss = quads_out(*total, first)
        sums[t, rows, pl.ds(0, HALF)] = cc
        sums[t, rows, pl.ds(HALF, HALF)] = cs
        sums[t, rows2, pl.ds(0, HALF)] = sc
        sums[t, rows2, pl.ds(HALF, HALF)] = ss

    for t in range(LOCAL_TILES):
        spectrum_block(t, 0, True)

        def later_blocks(k, carry, t=t):
            spectrum_block(t, k, False)
            return carry

        lax.fori_loop(1, 16, later_blocks, 0)
        half = dot3(split(sums[t]), inv_right())
        image[pl.ds(t * SIDE, SIDE), :] = dot3(inv_left(), split(half))

    rs_copies = []
    for s in range(SUBS):
        for d in (1, 3, 2):
            peer = lax.rem(xpos + d, 4)
            slot = (d - 1) * SUBS + s
            copy = remote(
                image.at[pl.ds(peer * 128 + s * SUB_ROWS, SUB_ROWS)],
                scattered.at[d - 1, pl.ds(s * SUB_ROWS, SUB_ROWS)],
                rs_send.at[slot],
                rs_recv.at[slot],
                tile,
                xpeer(d),
            )
            copy.start()
            rs_copies.append(copy)
    z_copies = []
    for s in range(SUBS):
        for copy in rs_copies[3 * s : 3 * s + 3]:
            copy.wait_recv()
        rows = pl.ds(s * SUB_ROWS, SUB_ROWS)
        own = image[pl.ds(xpos * 128 + s * SUB_ROWS, SUB_ROWS), :]
        zsend[rows, :] = own + scattered[0, rows, :] + scattered[1, rows, :] + scattered[2, rows, :]
        copy = remote(zsend.at[rows], zrecv.at[rows], z_send.at[s], z_recv.at[s], tile, zpartner)
        copy.start()
        z_copies.append(copy)
    local[1].wait()
    local[2].wait()
    xg_copies = []
    for s in range(SUBS):
        z_copies[s].wait_recv()
        rows = pl.ds(s * SUB_ROWS, SUB_ROWS)
        here = pl.ds(xpos * 128 + s * SUB_ROWS, SUB_ROWS)
        projection = background[here, :] + (zsend[rows, :] + zrecv[rows, :])
        ratio[here, :] = measured[here, :] / jnp.maximum(projection, FLOOR_LEVEL) - 1.0
        for d in (1, 3, 2):
            slot = (d - 1) * SUBS + s
            copy = remote(
                ratio.at[here], ratio.at[here], xg_send.at[slot], xg_recv.at[slot], tile, xpeer(d)
            )
            copy.start()
            xg_copies.append(copy)
    for copy in xg_copies:
        copy.wait_recv()

    for t in range(LOCAL_TILES):
        half = dot3(split(ratio[pl.ds(t * SIDE, SIDE), :]), right())
        sums[t] = dot3(left(), split(half))
        for k in range(16):
            rows, rows2 = rows_of(k)
            found = quads_in(*read_quads(sums.at[t], rows, rows2), k == 0)
            for c in range(4):
                ratio_quads[t, c, rows, :] = found[c]

    def strip(p, t, image_part, rows):
        values = vol[t, p, rows, :]
        return jnp.maximum(values * (1.0 + STEP_GAIN * image_part), 0.0)

    def send_halo(p):
        return (
            remote(
                top_send.at[p],
                after_recv.at[p],
                halo_send.at[p],
                halo_recv.at[p],
                before,
                depth,
            ),
            remote(
                bottom_send.at[p],
                before_recv.at[p],
                halo_send.at[LOCAL_PLANES + p],
                halo_recv.at[LOCAL_PLANES + p],
                after,
                depth,
            ),
        )

    def backward_plane(p, source):
        for t in range(LOCAL_TILES):
            for k in range(16):
                rows, rows2 = rows_of(k)
                hpr, hpi, hmr, hmi = (table[source(k), lax.rem(p, 4), c] for c in range(4))
                pr, pi, mr, mi = (ratio_quads[t, c, rows, :] for c in range(4))
                plus = times(hpr, hpi, pr, pi, k == 0, True)
                minus = times(hmr, hmi, mr, mi, k == 0, True)
                cc, cs, sc, ss = quads_out(*plus, *minus, k == 0)
                quads[t, rows, pl.ds(0, HALF)] = cc
                quads[t, rows, pl.ds(HALF, HALF)] = cs
                quads[t, rows2, pl.ds(0, HALF)] = sc
                quads[t, rows2, pl.ds(HALF, HALF)] = ss
            half = split(dot3(split(quads[t]), inv_right()))
            part_high[t, p] = half[0]
            part_low[t, p] = half[1]
            rows = slice(0, WIDTH) if t == 0 else slice(SIDE - WIDTH, SIDE)
            edge = strip(p, t, dot3((mats[4, rows], mats[5, rows]), half), rows)
            if t == 0:
                top_send[p] = edge
            else:
                bottom_send[p] = edge
        for copy in send_halo(p):
            copy.start()

    def backward_low(p, carry):
        backward_plane(p, lambda k: k)
        return carry

    def backward_high(p, carry):
        backward_plane(p, lambda k: 31 - k)
        return carry

    lax.fori_loop(0, 4, backward_low, 0)
    lax.fori_loop(4, 8, backward_high, 0)

    base = tile * LOCAL_TILES
    w_inner = ramp(margins[base])
    w_after = ramp(margins[base + 1])
    w_before = ramp(margins[lax.rem(base + TILES - 1, TILES)])

    def out_copies(p):
        return (
            pltpu.make_async_copy(
                vol.at[0, p, pl.ds(WIDTH, SIDE - WIDTH)],
                out_hbm.at[0, p, pl.ds(WIDTH, SIDE - WIDTH)],
                out_sem.at[2 * p],
            ),
            pltpu.make_async_copy(
                vol.at[1, p, pl.ds(0, SIDE - WIDTH)],
                out_hbm.at[1, p, pl.ds(0, SIDE - WIDTH)],
                out_sem.at[2 * p + 1],
            ),
        )

    def finish_plane(p, carry):
        half = (part_high[0, p], part_low[0, p])
        rows = slice(WIDTH, SIDE)
        upper = strip(p, 0, dot3((mats[4, rows], mats[5, rows]), half), rows)
        half = (part_high[1, p], part_low[1, p])
        rows = slice(0, SIDE - WIDTH)
        lower = strip(p, 1, dot3((mats[4, rows], mats[5, rows]), half), rows)
        inner = SIDE - 2 * WIDTH
        shared = (1.0 - w_inner) * upper[inner:] + w_inner * lower[:WIDTH]
        vol[0, p, WIDTH : SIDE - WIDTH, :] = upper[:inner]
        vol[0, p, SIDE - WIDTH :, :] = shared
        vol[1, p, :WIDTH, :] = shared
        vol[1, p, WIDTH : SIDE - WIDTH, :] = lower[WIDTH:]
        for copy in out_copies(p):
            copy.start()
        return carry

    lax.fori_loop(0, LOCAL_PLANES, finish_plane, 0)

    def outer_strips(p, carry):
        to_before, to_after = send_halo(p)
        to_before.wait_recv()
        to_after.wait_recv()
        vol[0, p, :WIDTH, :] = (1.0 - w_before) * before_recv[p] + w_before * top_send[p]
        vol[1, p, SIDE - WIDTH :, :] = (1.0 - w_after) * bottom_send[p] + w_after * after_recv[p]
        return carry

    lax.fori_loop(0, LOCAL_PLANES, outer_strips, 0)
    top_out = pltpu.make_async_copy(
        vol.at[0, :, pl.ds(0, WIDTH)], out_hbm.at[0, :, pl.ds(0, WIDTH)], out_sem.at[16]
    )
    bottom_out = pltpu.make_async_copy(
        vol.at[1, :, pl.ds(SIDE - WIDTH, WIDTH)],
        out_hbm.at[1, :, pl.ds(SIDE - WIDTH, WIDTH)],
        out_sem.at[17],
    )
    top_out.start()
    bottom_out.start()

    @pl.when(jnp.logical_not(negative))
    def _():
        up_all.wait_send()

    @pl.when(negative)
    def _():
        down_rest.wait_send()
        down_first.wait_send()
        down_last.wait_send()

    for copy in started + rs_copies + z_copies + xg_copies:
        copy.wait_send()

    def drain(p, carry):
        for copy in send_halo(p):
            copy.wait_send()
        for copy in out_copies(p):
            copy.wait()
        return carry

    lax.fori_loop(0, LOCAL_PLANES, drain, 0)
    top_out.wait()
    bottom_out.wait()


def on_device(volume, transfer, measured, background, margins, phases):
    mats = packed_tables()
    hbm = pl.BlockSpec(memory_space=pl.ANY)
    vmem = pl.BlockSpec(memory_space=pltpu.VMEM)
    smem = pl.BlockSpec(memory_space=pltpu.SMEM)
    dma = pltpu.SemaphoreType.DMA
    tall = LOCAL_TILES * SIDE
    return pl.pallas_call(
        kernel,
        name="update",
        out_shape=jax.ShapeDtypeStruct(volume.shape, f32),
        in_specs=[smem, smem, vmem, hbm, hbm, hbm, hbm, vmem],
        out_specs=hbm,
        scratch_shapes=[
            pltpu.VMEM((LOCAL_TILES, LOCAL_PLANES, SIDE, SIDE), f32),
            pltpu.VMEM((LOCAL_TILES, LOCAL_PLANES, SIDE, SIDE), f32),
            pltpu.VMEM((32, 4, 4, 8, HALF), f32),
            pltpu.VMEM((8, SIDE, SIDE), bf16),
            pltpu.VMEM((tall, SIDE), f32),
            pltpu.VMEM((tall, SIDE), f32),
            pltpu.VMEM((2, HALF, HALF), f32),
            pltpu.VMEM((2, 8, 16, HALF), f32),
            pltpu.VMEM((8, 16, HALF), f32),
            pltpu.VMEM((1, 16, HALF), f32),
            pltpu.VMEM((8, 16, HALF), f32),
            pltpu.VMEM((8, 16, HALF), f32),
            pltpu.VMEM((LOCAL_TILES, SIDE, SIDE), f32),
            pltpu.VMEM((tall, SIDE), f32),
            pltpu.VMEM((3, 128, SIDE), f32),
            pltpu.VMEM((128, SIDE), f32),
            pltpu.VMEM((128, SIDE), f32),
            pltpu.VMEM((tall, SIDE), f32),
            pltpu.VMEM((LOCAL_TILES, 4, HALF, HALF), f32),
            pltpu.VMEM((LOCAL_TILES, SIDE, SIDE), f32),
            pltpu.VMEM((LOCAL_TILES, LOCAL_PLANES, SIDE, SIDE), bf16),
            pltpu.VMEM((LOCAL_TILES, LOCAL_PLANES, SIDE, SIDE), bf16),
            pltpu.VMEM((LOCAL_PLANES, WIDTH, SIDE), f32),
            pltpu.VMEM((LOCAL_PLANES, WIDTH, SIDE), f32),
            pltpu.VMEM((LOCAL_PLANES, WIDTH, SIDE), f32),
            pltpu.VMEM((LOCAL_PLANES, WIDTH, SIDE), f32),
            dma((LOCAL_PLANES,)),
            dma((3,)),
            dma((3,)),
            dma((2,)),
            dma((31,)),
            dma((32,)),
            dma((3 * SUBS,)),
            dma((3 * SUBS,)),
            dma((SUBS,)),
            dma((SUBS,)),
            dma((3 * SUBS,)),
            dma((3 * SUBS,)),
            dma((2 * LOCAL_PLANES,)),
            dma((2 * LOCAL_PLANES,)),
            dma((2 * LOCAL_PLANES + 2,)),
        ],
        compiler_params=pltpu.CompilerParams(
            collective_id=0, has_side_effects=True, vmem_limit_bytes=40 * 1024 * 1024
        ),
    )(
        phases,
        margins,
        transfer,
        volume,
        measured.reshape(tall, SIDE),
        background.reshape(tall, SIDE),
        mats,
        pairing(),
    )


def solution(mesh):
    return jax.shard_map(
        on_device,
        mesh=mesh,
        in_specs=(
            P("tile", "depth", None, None),
            P("depth", None, "tile", None),
            P("tile", None, None),
            P("tile", None, None),
            P(),
            P("depth"),
        ),
        out_specs=P("tile", "depth", None, None),
        check_vma=False,
    )
```

```python
import functools
import math

import jax
import jax.numpy as jnp
import numpy as np
from jax import lax
from jax.experimental import pallas as pl
from jax.experimental.pallas import tpu as pltpu
from jax.sharding import PartitionSpec as P

SIDE = 256
HALF = 128
WIDTH = 32
TILES = 64
LOCAL_TILES = 2
LOCAL_PLANES = 8
SUBS = 2
SUB_ROWS = 128 // SUBS
FLOOR_LEVEL = 0.5
STEP_GAIN = 2.0
MESH = pl.DeviceIdType.MESH
f32 = jnp.float32
bf16 = jnp.bfloat16


def packed_tables():
    place = np.arange(SIDE)
    table = np.zeros((SIDE, SIDE))
    for a in range(HALF):
        table[a] = np.cos(2 * np.pi * (a * place % SIDE) / SIDE)
    table[HALF] = 1.0 - 2.0 * (place % 2)
    for a in range(1, HALF):
        table[HALF + a] = np.sin(2 * np.pi * (a * place % SIDE) / SIDE)
    weight = np.full(SIDE, 2.0)
    weight[0] = weight[HALF] = 1.0
    inverse = table.T * weight / SIDE
    pieces = []
    for matrix in (table, table.T, inverse, inverse.T):
        high = matrix.astype(bf16)
        pieces += [high, (matrix - high.astype(np.float64)).astype(bf16)]
    return jnp.asarray(np.stack(pieces))


def pairing():
    move = np.zeros((HALF, HALF), np.float32)
    move[0, 0] = 1.0
    for b in range(1, HALF):
        move[HALF - b, b] = 1.0
    return jnp.asarray(move.astype(bf16))


def split(values):
    high = values.astype(bf16)
    return high, (values - high.astype(f32)).astype(bf16)


def dot(a, b):
    return jnp.dot(a, b, preferred_element_type=f32)


def dot3(a, b):
    return dot(a[0], b[0]) + dot(a[1], b[0]) + dot(a[0], b[1])


def special(shape, first):
    lane0 = lax.broadcasted_iota(jnp.int32, shape, 1) == 0
    row0 = None
    if first:
        row0 = jnp.logical_and(
            lax.broadcasted_iota(jnp.int32, shape, 0) == 0, jnp.logical_not(lane0)
        )
    return lane0, row0


def quads_in(cc, cs, sc, ss, first):
    lane0, row0 = special(cc.shape, first)
    pr, pi, mr, mi = cc - ss, cs + sc, cc + ss, cs - sc
    if first:
        pr = jnp.where(row0, cc, pr)
        pi = jnp.where(row0, cs, pi)
        mr = jnp.where(row0, sc, mr)
        mi = jnp.where(row0, ss, mi)
    return (
        jnp.where(lane0, cc, pr),
        jnp.where(lane0, sc, pi),
        jnp.where(lane0, cs, mr),
        jnp.where(lane0, ss, mi),
    )


def quads_out(pr, pi, mr, mi, first):
    lane0, row0 = special(pr.shape, first)
    cc, ss, cs, sc = pr + mr, mr - pr, pi + mi, pi - mi
    if first:
        cc = jnp.where(row0, pr, cc)
        cs = jnp.where(row0, pi, cs)
        sc = jnp.where(row0, mr, sc)
        ss = jnp.where(row0, mi, ss)
    return (
        jnp.where(lane0, pr, cc),
        jnp.where(lane0, mr, cs),
        jnp.where(lane0, pi, sc),
        jnp.where(lane0, mi, ss),
    )


def times(hr, hi, real, imag, first, conj):
    second = hr
    if first:
        lane0, _ = special(hr.shape, False)
        corner = jnp.logical_and(lane0, lax.broadcasted_iota(jnp.int32, hr.shape, 0) == 0)
        second = jnp.where(corner, hi, hr)
        hi = jnp.where(corner, 0.0, hi)
    if conj:
        return hr * real - hi * imag, second * imag + hi * real
    return hr * real + hi * imag, second * imag - hi * real


def ramp(margin):
    margin = margin.astype(f32)
    row = lax.broadcasted_iota(jnp.int32, (WIDTH, SIDE), 0).astype(f32)
    return jnp.clip((row + 0.5 - (WIDTH - margin) / 2.0) / margin, 0.0, 1.0)


def kernel(
    phases_hbm,
    margins_hbm,
    transfer_hbm,
    volume_hbm,
    measured_hbm,
    background_hbm,
    mats_hbm,
    pair_hbm,
    out_hbm,
    phases,
    margins,
    transfer,
    pair_ref,
    vol,
    packed,
    table,
    mats,
    measured,
    background,
    halves,
    mine,
    other,
    other0,
    pos,
    neg,
    sums,
    image,
    scattered,
    zsend,
    zrecv,
    ratio,
    ratio_quads,
    quads,
    part_high,
    part_low,
    top_send,
    bottom_send,
    after_recv,
    before_recv,
    vol_sem,
    in_sem,
    ex_send,
    ex_recv,
    ag_send,
    ag_recv,
    rs_send,
    rs_recv,
    z_send,
    z_recv,
    xg_send,
    xg_recv,
    halo_send,
    halo_recv,
    out_sem,
):
    tile = lax.axis_index("tile")
    depth = lax.axis_index("depth")
    core = lax.rem(tile, 2)
    zlo = lax.rem(tile // 2, 4)
    yrow = tile // 8
    xpos = lax.rem(depth, 4)
    zhi = depth // 4
    negative = tile >= 16
    block = jnp.where(negative, 31 - tile, tile)

    def at(y, z, c):
        return lax.rem(y, 4) * 8 + lax.rem(z, 4) * 2 + c

    def xpeer(d):
        return zhi * 4 + lax.rem(xpos + d, 4)

    after = lax.rem(tile + 1, 32)
    before = lax.rem(tile + 31, 32)
    zpartner = (1 - zhi) * 4 + xpos

    volume_copies = []
    for p in range(LOCAL_PLANES):
        volume_copies.append(
            pltpu.make_async_copy(volume_hbm.at[:, p], vol.at[:, p], vol_sem.at[p])
        )
    local = [
        pltpu.make_async_copy(mats_hbm, mats, in_sem.at[0]),
        pltpu.make_async_copy(measured_hbm, measured, in_sem.at[1]),
        pltpu.make_async_copy(background_hbm, background, in_sem.at[2]),
        pltpu.make_async_copy(transfer_hbm, transfer, in_sem.at[3]),
        pltpu.make_async_copy(pair_hbm, pair_ref, in_sem.at[4]),
        pltpu.make_async_copy(phases_hbm, phases, in_sem.at[5]),
        pltpu.make_async_copy(margins_hbm, margins, in_sem.at[6]),
    ]
    for which in (3, 4, 0, 5, 6):
        local[which].start()
    for copy in volume_copies:
        copy.start()
    local[1].start()
    local[2].start()

    barrier = pltpu.get_barrier_semaphore()

    def greet(t, d):
        pl.semaphore_signal(barrier, inc=1, device_id=(t, d), device_id_type=MESH)

    greet(31 - tile, depth)
    for dz in range(1, 4):
        greet(at(yrow, zlo + dz, core), depth)
    greet(at(yrow + 1, zlo, core), depth)
    greet(at(yrow + 3, zlo, core), depth)
    greet(at(yrow, zlo, 1 - core), depth)
    for d in range(1, 4):
        greet(tile, xpeer(d))
    greet(tile, zpartner)
    greet(after, depth)
    greet(before, depth)
    first_of = lax.rem(32 - tile, 16)
    last_to = jnp.where(tile == 16, 31, tile - 1)
    last_from = jnp.where(tile == 31, 16, tile + 1)
    row0_from = jnp.where(tile == 0, 16, 32 - tile)

    @pl.when(negative)
    def _():
        greet(first_of, depth)
        greet(last_to, depth)
        greet(last_from, depth)

    @pl.when(jnp.logical_not(negative))
    def _():
        greet(row0_from, depth)

    local[3].wait()
    local[4].wait()
    whole = transfer[...].reshape(LOCAL_PLANES * 2 * 8, SIDE)
    halves[0] = whole[:, :HALF]
    rest = whole[:, HALF:]
    high, low = split(rest)
    lowest = ((rest - high.astype(f32)) - low.astype(f32)).astype(bf16)
    move = pair_ref[...]
    halves[1] = dot(high, move) + dot(low, move) + dot(lowest, move)
    for r in range(8):
        to = jnp.where(negative, (8 - r) % 8, r)
        for ph in range(2):
            for e in range(2):
                for c in range(2):
                    piece = halves[e, pl.ds(ph * 64 + c * 8 + r, 4, stride=16), :]
                    mine[ph, to, pl.ds((e * 2 + c) * 4, 4), :] = piece

    pl.semaphore_wait(barrier, 14 + 2 * (tile // 16))

    def remote(src, dst, send, recv, t, d):
        return pltpu.make_async_remote_copy(
            src_ref=src,
            dst_ref=dst,
            send_sem=send,
            recv_sem=recv,
            device_id=(t, d),
            device_id_type=MESH,
        )

    rows7 = pl.ds(1, 7)
    row1 = pl.ds(0, 1)
    up_all = remote(mine.at[1], other, ex_send.at[0], ex_recv.at[0], 31 - tile, depth)
    down_rest = remote(
        mine.at[0, rows7], other.at[rows7], ex_send.at[0], ex_recv.at[0], 31 - tile, depth
    )
    down_first = remote(
        mine.at[0, row1], other.at[row1], ex_send.at[1], ex_recv.at[1], first_of, depth
    )
    down_last = remote(mine.at[1, row1], other0, ex_send.at[2], ex_recv.at[1], last_to, depth)

    @pl.when(jnp.logical_not(negative))
    def _():
        up_all.start()

    @pl.when(negative)
    def _():
        down_rest.start()
        down_first.start()
        down_last.start()

    left = lambda: (mats[0], mats[1])
    right = lambda: (mats[2], mats[3])
    inv_left = lambda: (mats[4], mats[5])
    inv_right = lambda: (mats[6], mats[7])
    local[0].wait()

    def forward(p, carry):
        pltpu.make_async_copy(volume_hbm.at[:, p], vol.at[:, p], vol_sem.at[p]).wait()
        for t in range(LOCAL_TILES):
            half = dot3(split(vol[t, p]), right())
            packed[t, p] = dot3(left(), split(half))
        return carry

    lax.fori_loop(0, 4, forward, 0)

    @pl.when(jnp.logical_not(negative))
    def _():
        down_rest.wait_recv()
        down_first.wait_recv()
        pos[...] = mine[0]
        neg[...] = other[...]

    @pl.when(negative)
    def _():
        up_all.wait_recv()
        down_last.wait_recv()
        pos[...] = other[...]
        neg[0] = other0[0]
        neg[1:8] = mine[1, 1:8]

    local[5].wait()
    local[6].wait()
    plane0 = jnp.where(negative, 4, 0)
    column = lax.broadcasted_iota(jnp.int32, (4, HALF), 1)
    row4 = lax.broadcasted_iota(jnp.int32, (4, HALF), 0)
    phase = jnp.zeros((4, HALF), jnp.int32)
    for q in range(4):
        phase = jnp.where(row4 == q, phases[plane0 + q], phase)
    lane0 = column == 0

    def rotor(columns):
        angle = ((phase * columns) & (SIDE - 1)).astype(f32) * (2.0 * math.pi / SIDE)
        return jnp.cos(angle), jnp.sin(angle)

    cos_p, sin_p = rotor(column)
    cos_m, sin_m = rotor(jnp.where(lane0, HALF, column))
    sin_m = jnp.where(lane0, 0.0, sin_m)
    is_first = block == 0
    for r in range(8):
        epr, epi, fpr, fpi = (pos[r, pl.ds(c * 4, 4), :] for c in range(4))
        enr, eni, fnr, fni = (neg[r, pl.ds(c * 4, 4), :] for c in range(4))
        hpr, hpi = 0.25 * (epr + fnr), 0.25 * (epi - fni)
        hmr, hmi = 0.25 * (enr + fpr), 0.25 * (eni - fpi)
        if r == 0:
            at0 = jnp.logical_and(is_first, jnp.logical_not(lane0))
            hpr = jnp.where(at0, 0.5 * (epr + fpr), hpr)
            hpi = jnp.where(at0, 0.5 * (epi - fpi), hpi)
            hmr = jnp.where(at0, 0.5 * (enr + fnr), hmr)
            hmi = jnp.where(at0, 0.5 * (eni - fni), hmi)
        lpr, lpi = 0.5 * (epr + enr), 0.5 * (epi - eni)
        lmr, lmi = 0.5 * (fpr + fnr), 0.5 * (fpi - fni)
        if r == 0:
            lpr, lpi = jnp.where(is_first, epr, lpr), jnp.where(is_first, enr, lpi)
            lmr, lmi = jnp.where(is_first, fpr, lmr), jnp.where(is_first, fnr, lmi)
        hpr, hpi = jnp.where(lane0, lpr, hpr), jnp.where(lane0, lpi, hpi)
        hmr, hmi = jnp.where(lane0, lmr, hmr), jnp.where(lane0, lmi, hmi)
        parts = (
            hpr * cos_p + hpi * sin_p,
            hpi * cos_p - hpr * sin_p,
            hmr * cos_m + hmi * sin_m,
            hmi * cos_m - hmr * sin_m,
        )
        for c in range(4):
            for q in range(4):
                table[tile, q, c, pl.ds(r, 1), :] = parts[c][q : q + 1]

    started = []

    def pass_on(which, t):
        copy = remote(
            table.at[which],
            table.at[which],
            ag_send.at[len(started)],
            ag_recv.at[which],
            t,
            depth,
        )
        copy.start()
        started.append(copy)

    def arrived(which):
        remote(
            table.at[which], table.at[which], ag_send.at[0], ag_recv.at[which], tile, depth
        ).wait_recv()

    above = at(yrow + 1, zlo, core)
    below = at(yrow + 3, zlo, core)
    sibling = at(yrow, zlo, 1 - core)
    z_order = (1, 3, 2)
    pass_on(tile, above)
    pass_on(tile, below)
    for dz in z_order:
        pass_on(tile, at(yrow, zlo + dz, core))
    pass_on(tile, sibling)

    lax.fori_loop(4, 6, forward, 0)

    for dz in z_order:
        which = at(yrow, zlo + dz, core)
        arrived(which)
        pass_on(which, above)
        pass_on(which, below)
        pass_on(which, sibling)

    lax.fori_loop(6, 8, forward, 0)

    for dz in (0, 1, 3, 2):
        which = at(yrow + 3, zlo + dz, core)
        arrived(which)
        if dz in (0, 1):
            pass_on(which, above)
        pass_on(which, sibling)
        which = at(yrow + 1, zlo + dz, core)
        arrived(which)
        if dz in (2, 3):
            pass_on(which, below)
        pass_on(which, sibling)
    for dz in (0, 1, 3, 2):
        which = at(yrow + 2, zlo + dz, core)
        arrived(which)
        pass_on(which, sibling)
    for dy in range(4):
        for dz in range(4):
            arrived(at(yrow + dy, zlo + dz, 1 - core))

    def read_quads(ref, rows, rows2):
        return (
            ref[rows, pl.ds(0, HALF)],
            ref[rows, pl.ds(HALF, HALF)],
            ref[rows2, pl.ds(0, HALF)],
            ref[rows2, pl.ds(HALF, HALF)],
        )

    def rows_of(k):
        if isinstance(k, int):
            return pl.ds(8 * k, 8), pl.ds(HALF + 8 * k, 8)
        return pl.ds(pl.multiple_of(8 * k, 8), 8), pl.ds(pl.multiple_of(HALF + 8 * k, 8), 8)

    def table_of(p, k):
        which = k if p < 4 else 31 - k
        return tuple(table[which, p % 4, c] for c in range(4))

    def spectrum_block(t, k, first):
        rows, rows2 = rows_of(k)
        total = None
        for p in range(LOCAL_PLANES):
            hpr, hpi, hmr, hmi = table_of(p, k)
            pr, pi, mr, mi = quads_in(*read_quads(packed.at[t, p], rows, rows2), first)
            terms = times(hpr, hpi, pr, pi, first, False) + times(hmr, hmi, mr, mi, first, False)
            total = terms if total is None else tuple(a + b for a, b in zip(total, terms))
        cc, cs, sc, ss = quads_out(*total, first)
        sums[t, rows, pl.ds(0, HALF)] = cc
        sums[t, rows, pl.ds(HALF, HALF)] = cs
        sums[t, rows2, pl.ds(0, HALF)] = sc
        sums[t, rows2, pl.ds(HALF, HALF)] = ss

    for t in range(LOCAL_TILES):
        spectrum_block(t, 0, True)

        def later_blocks(k, carry, t=t):
            spectrum_block(t, k, False)
            return carry

        lax.fori_loop(1, 16, later_blocks, 0)
        half = dot3(split(sums[t]), inv_right())
        image[pl.ds(t * SIDE, SIDE), :] = dot3(inv_left(), split(half))

    rs_copies = []
    for s in range(SUBS):
        for d in (1, 3, 2):
            peer = lax.rem(xpos + d, 4)
            slot = (d - 1) * SUBS + s
            copy = remote(
                image.at[pl.ds(peer * 128 + s * SUB_ROWS, SUB_ROWS)],
                scattered.at[d - 1, pl.ds(s * SUB_ROWS, SUB_ROWS)],
                rs_send.at[slot],
                rs_recv.at[slot],
                tile,
                xpeer(d),
            )
            copy.start()
            rs_copies.append(copy)
    z_copies = []
    for s in range(SUBS):
        for copy in rs_copies[3 * s : 3 * s + 3]:
            copy.wait_recv()
        rows = pl.ds(s * SUB_ROWS, SUB_ROWS)
        own = image[pl.ds(xpos * 128 + s * SUB_ROWS, SUB_ROWS), :]
        zsend[rows, :] = own + scattered[0, rows, :] + scattered[1, rows, :] + scattered[2, rows, :]
        copy = remote(zsend.at[rows], zrecv.at[rows], z_send.at[s], z_recv.at[s], tile, zpartner)
        copy.start()
        z_copies.append(copy)
    local[1].wait()
    local[2].wait()
    xg_copies = []
    for s in range(SUBS):
        z_copies[s].wait_recv()
        rows = pl.ds(s * SUB_ROWS, SUB_ROWS)
        here = pl.ds(xpos * 128 + s * SUB_ROWS, SUB_ROWS)
        projection = background[here, :] + (zsend[rows, :] + zrecv[rows, :])
        ratio[here, :] = measured[here, :] / jnp.maximum(projection, FLOOR_LEVEL) - 1.0
        for d in (1, 3, 2):
            slot = (d - 1) * SUBS + s
            copy = remote(
                ratio.at[here], ratio.at[here], xg_send.at[slot], xg_recv.at[slot], tile, xpeer(d)
            )
            copy.start()
            xg_copies.append(copy)
    for copy in xg_copies:
        copy.wait_recv()

    for t in range(LOCAL_TILES):
        half = dot3(split(ratio[pl.ds(t * SIDE, SIDE), :]), right())
        sums[t] = dot3(left(), split(half))
        for k in range(16):
            rows, rows2 = rows_of(k)
            found = quads_in(*read_quads(sums.at[t], rows, rows2), k == 0)
            for c in range(4):
                ratio_quads[t, c, rows, :] = found[c]

    def strip(p, t, image_part, rows):
        values = vol[t, p, rows, :]
        return jnp.maximum(values * (1.0 + STEP_GAIN * image_part), 0.0)

    def send_halo(p):
        return (
            remote(
                top_send.at[p],
                after_recv.at[p],
                halo_send.at[p],
                halo_recv.at[p],
                before,
                depth,
            ),
            remote(
                bottom_send.at[p],
                before_recv.at[p],
                halo_send.at[LOCAL_PLANES + p],
                halo_recv.at[LOCAL_PLANES + p],
                after,
                depth,
            ),
        )

    def backward_plane(p, source):
        for t in range(LOCAL_TILES):
            for k in range(16):
                rows, rows2 = rows_of(k)
                hpr, hpi, hmr, hmi = (table[source(k), lax.rem(p, 4), c] for c in range(4))
                pr, pi, mr, mi = (ratio_quads[t, c, rows, :] for c in range(4))
                plus = times(hpr, hpi, pr, pi, k == 0, True)
                minus = times(hmr, hmi, mr, mi, k == 0, True)
                cc, cs, sc, ss = quads_out(*plus, *minus, k == 0)
                quads[t, rows, pl.ds(0, HALF)] = cc
                quads[t, rows, pl.ds(HALF, HALF)] = cs
                quads[t, rows2, pl.ds(0, HALF)] = sc
                quads[t, rows2, pl.ds(HALF, HALF)] = ss
            half = split(dot3(split(quads[t]), inv_right()))
            part_high[t, p] = half[0]
            part_low[t, p] = half[1]
            rows = slice(0, WIDTH) if t == 0 else slice(SIDE - WIDTH, SIDE)
            edge = strip(p, t, dot3((mats[4, rows], mats[5, rows]), half), rows)
            if t == 0:
                top_send[p] = edge
            else:
                bottom_send[p] = edge
        for copy in send_halo(p):
            copy.start()

    def backward_low(p, carry):
        backward_plane(p, lambda k: k)
        return carry

    def backward_high(p, carry):
        backward_plane(p, lambda k: 31 - k)
        return carry

    lax.fori_loop(0, 4, backward_low, 0)
    lax.fori_loop(4, 8, backward_high, 0)

    base = tile * LOCAL_TILES
    w_inner = ramp(margins[base])
    w_after = ramp(margins[base + 1])
    w_before = ramp(margins[lax.rem(base + TILES - 1, TILES)])

    def out_copies(p):
        return (
            pltpu.make_async_copy(
                vol.at[0, p, pl.ds(WIDTH, SIDE - WIDTH)],
                out_hbm.at[0, p, pl.ds(WIDTH, SIDE - WIDTH)],
                out_sem.at[2 * p],
            ),
            pltpu.make_async_copy(
                vol.at[1, p, pl.ds(0, SIDE - WIDTH)],
                out_hbm.at[1, p, pl.ds(0, SIDE - WIDTH)],
                out_sem.at[2 * p + 1],
            ),
        )

    def finish_plane(p, carry):
        half = (part_high[0, p], part_low[0, p])
        rows = slice(WIDTH, SIDE)
        upper = strip(p, 0, dot3((mats[4, rows], mats[5, rows]), half), rows)
        half = (part_high[1, p], part_low[1, p])
        rows = slice(0, SIDE - WIDTH)
        lower = strip(p, 1, dot3((mats[4, rows], mats[5, rows]), half), rows)
        inner = SIDE - 2 * WIDTH
        shared = (1.0 - w_inner) * upper[inner:] + w_inner * lower[:WIDTH]
        vol[0, p, WIDTH : SIDE - WIDTH, :] = upper[:inner]
        vol[0, p, SIDE - WIDTH :, :] = shared
        vol[1, p, :WIDTH, :] = shared
        vol[1, p, WIDTH : SIDE - WIDTH, :] = lower[WIDTH:]
        for copy in out_copies(p):
            copy.start()
        return carry

    lax.fori_loop(0, LOCAL_PLANES, finish_plane, 0)

    def outer_strips(p, carry):
        to_before, to_after = send_halo(p)
        to_before.wait_recv()
        to_after.wait_recv()
        vol[0, p, :WIDTH, :] = (1.0 - w_before) * before_recv[p] + w_before * top_send[p]
        vol[1, p, SIDE - WIDTH :, :] = (1.0 - w_after) * bottom_send[p] + w_after * after_recv[p]
        return carry

    lax.fori_loop(0, LOCAL_PLANES, outer_strips, 0)
    top_out = pltpu.make_async_copy(
        vol.at[0, :, pl.ds(0, WIDTH)], out_hbm.at[0, :, pl.ds(0, WIDTH)], out_sem.at[16]
    )
    bottom_out = pltpu.make_async_copy(
        vol.at[1, :, pl.ds(SIDE - WIDTH, WIDTH)],
        out_hbm.at[1, :, pl.ds(SIDE - WIDTH, WIDTH)],
        out_sem.at[17],
    )
    top_out.start()
    bottom_out.start()

    @pl.when(jnp.logical_not(negative))
    def _():
        up_all.wait_send()

    @pl.when(negative)
    def _():
        down_rest.wait_send()
        down_first.wait_send()
        down_last.wait_send()

    for copy in started + rs_copies + z_copies + xg_copies:
        copy.wait_send()

    def drain(p, carry):
        for copy in send_halo(p):
            copy.wait_send()
        for copy in out_copies(p):
            copy.wait()
        return carry

    lax.fori_loop(0, LOCAL_PLANES, drain, 0)
    top_out.wait()
    bottom_out.wait()


def on_device(volume, transfer, measured, background, margins, phases):
    mats = packed_tables()
    hbm = pl.BlockSpec(memory_space=pltpu.HBM)
    dma = pltpu.SemaphoreType.DMA
    tall = LOCAL_TILES * SIDE
    return pl.pallas_call(
        kernel,
        name="update",
        out_shape=jax.ShapeDtypeStruct(volume.shape, f32),
        in_specs=[hbm] * 8,
        out_specs=pl.BlockSpec(memory_space=pl.ANY),
        scratch_shapes=[
            pltpu.SMEM((LOCAL_PLANES,), jnp.int32),
            pltpu.SMEM((TILES,), jnp.int32),
            pltpu.VMEM((LOCAL_PLANES, 2, 8, SIDE), f32),
            pltpu.VMEM((HALF, HALF), bf16),
            pltpu.VMEM((LOCAL_TILES, LOCAL_PLANES, SIDE, SIDE), f32),
            pltpu.VMEM((LOCAL_TILES, LOCAL_PLANES, SIDE, SIDE), f32),
            pltpu.VMEM((32, 4, 4, 8, HALF), f32),
            pltpu.VMEM((8, SIDE, SIDE), bf16),
            pltpu.VMEM((tall, SIDE), f32),
            pltpu.VMEM((tall, SIDE), f32),
            pltpu.VMEM((2, HALF, HALF), f32),
            pltpu.VMEM((2, 8, 16, HALF), f32),
            pltpu.VMEM((8, 16, HALF), f32),
            pltpu.VMEM((1, 16, HALF), f32),
            pltpu.VMEM((8, 16, HALF), f32),
            pltpu.VMEM((8, 16, HALF), f32),
            pltpu.VMEM((LOCAL_TILES, SIDE, SIDE), f32),
            pltpu.VMEM((tall, SIDE), f32),
            pltpu.VMEM((3, 128, SIDE), f32),
            pltpu.VMEM((128, SIDE), f32),
            pltpu.VMEM((128, SIDE), f32),
            pltpu.VMEM((tall, SIDE), f32),
            pltpu.VMEM((LOCAL_TILES, 4, HALF, HALF), f32),
            pltpu.VMEM((LOCAL_TILES, SIDE, SIDE), f32),
            pltpu.VMEM((LOCAL_TILES, LOCAL_PLANES, SIDE, SIDE), bf16),
            pltpu.VMEM((LOCAL_TILES, LOCAL_PLANES, SIDE, SIDE), bf16),
            pltpu.VMEM((LOCAL_PLANES, WIDTH, SIDE), f32),
            pltpu.VMEM((LOCAL_PLANES, WIDTH, SIDE), f32),
            pltpu.VMEM((LOCAL_PLANES, WIDTH, SIDE), f32),
            pltpu.VMEM((LOCAL_PLANES, WIDTH, SIDE), f32),
            dma((LOCAL_PLANES,)),
            dma((7,)),
            dma((3,)),
            dma((2,)),
            dma((31,)),
            dma((32,)),
            dma((3 * SUBS,)),
            dma((3 * SUBS,)),
            dma((SUBS,)),
            dma((SUBS,)),
            dma((3 * SUBS,)),
            dma((3 * SUBS,)),
            dma((2 * LOCAL_PLANES,)),
            dma((2 * LOCAL_PLANES,)),
            dma((2 * LOCAL_PLANES + 2,)),
        ],
        compiler_params=pltpu.CompilerParams(
            collective_id=0, has_side_effects=True, vmem_limit_bytes=67043328
        ),
    )(
        phases,
        margins,
        transfer,
        volume,
        measured.reshape(tall, SIDE),
        background.reshape(tall, SIDE),
        mats,
        pairing(),
    )


def solution(mesh):
    return jax.shard_map(
        on_device,
        mesh=mesh,
        in_specs=(
            P("tile", "depth", None, None),
            P("depth", None, "tile", None),
            P("tile", None, None),
            P("tile", None, None),
            P(),
            P("depth"),
        ),
        out_specs=P("tile", "depth", None, None),
        check_vma=False,
    )
```

```python
import functools
import math

import jax
import jax.numpy as jnp
import numpy as np
from jax import lax
from jax.experimental import pallas as pl
from jax.experimental.pallas import tpu as pltpu
from jax.sharding import PartitionSpec as P

SIDE = 256
HALF = 128
WIDTH = 32
TILES = 64
LOCAL_TILES = 2
LOCAL_PLANES = 8
SUBS = 4
SUB_ROWS = 128 // SUBS
FLOOR_LEVEL = 0.5
STEP_GAIN = 2.0
MESH = pl.DeviceIdType.MESH
f32 = jnp.float32
bf16 = jnp.bfloat16


def packed_tables():
    place = np.arange(SIDE)
    table = np.zeros((SIDE, SIDE))
    for a in range(HALF):
        table[a] = np.cos(2 * np.pi * (a * place % SIDE) / SIDE)
    table[HALF] = 1.0 - 2.0 * (place % 2)
    for a in range(1, HALF):
        table[HALF + a] = np.sin(2 * np.pi * (a * place % SIDE) / SIDE)
    weight = np.full(SIDE, 2.0)
    weight[0] = weight[HALF] = 1.0
    inverse = table.T * weight / SIDE
    pieces = []
    for matrix in (table, table.T, inverse, inverse.T):
        high = matrix.astype(bf16)
        pieces += [high, (matrix - high.astype(np.float64)).astype(bf16)]
    return jnp.asarray(np.stack(pieces))


def pairing():
    move = np.zeros((HALF, HALF), np.float32)
    move[0, 0] = 1.0
    for b in range(1, HALF):
        move[HALF - b, b] = 1.0
    return jnp.asarray(move.astype(bf16))


def split(values):
    high = values.astype(bf16)
    return high, (values - high.astype(f32)).astype(bf16)


def dot(a, b):
    return jnp.dot(a, b, preferred_element_type=f32)


def dot3(a, b):
    return dot(a[0], b[0]) + dot(a[1], b[0]) + dot(a[0], b[1])


def special(shape, first):
    lane0 = lax.broadcasted_iota(jnp.int32, shape, 1) == 0
    row0 = None
    if first:
        row0 = jnp.logical_and(
            lax.broadcasted_iota(jnp.int32, shape, 0) == 0, jnp.logical_not(lane0)
        )
    return lane0, row0


def quads_in(cc, cs, sc, ss, first):
    lane0, row0 = special(cc.shape, first)
    pr, pi, mr, mi = cc - ss, cs + sc, cc + ss, cs - sc
    if first:
        pr = jnp.where(row0, cc, pr)
        pi = jnp.where(row0, cs, pi)
        mr = jnp.where(row0, sc, mr)
        mi = jnp.where(row0, ss, mi)
    return (
        jnp.where(lane0, cc, pr),
        jnp.where(lane0, sc, pi),
        jnp.where(lane0, cs, mr),
        jnp.where(lane0, ss, mi),
    )


def quads_out(pr, pi, mr, mi, first):
    lane0, row0 = special(pr.shape, first)
    cc, ss, cs, sc = pr + mr, mr - pr, pi + mi, pi - mi
    if first:
        cc = jnp.where(row0, pr, cc)
        cs = jnp.where(row0, pi, cs)
        sc = jnp.where(row0, mr, sc)
        ss = jnp.where(row0, mi, ss)
    return (
        jnp.where(lane0, pr, cc),
        jnp.where(lane0, mr, cs),
        jnp.where(lane0, pi, sc),
        jnp.where(lane0, mi, ss),
    )


def times(hr, hi, real, imag, first, conj):
    second = hr
    if first:
        lane0, _ = special(hr.shape, False)
        corner = jnp.logical_and(lane0, lax.broadcasted_iota(jnp.int32, hr.shape, 0) == 0)
        second = jnp.where(corner, hi, hr)
        hi = jnp.where(corner, 0.0, hi)
    if conj:
        return hr * real - hi * imag, second * imag + hi * real
    return hr * real + hi * imag, second * imag - hi * real


def ramp(margin):
    margin = margin.astype(f32)
    row = lax.broadcasted_iota(jnp.int32, (WIDTH, SIDE), 0).astype(f32)
    return jnp.clip((row + 0.5 - (WIDTH - margin) / 2.0) / margin, 0.0, 1.0)


def kernel(
    phases_hbm,
    margins_hbm,
    transfer_hbm,
    volume_hbm,
    measured_hbm,
    background_hbm,
    mats_hbm,
    pair_hbm,
    out_hbm,
    phases,
    margins,
    transfer,
    pair_ref,
    vol,
    packed,
    table,
    mats,
    measured,
    background,
    halves,
    mine,
    other,
    other0,
    pos,
    neg,
    sums,
    image,
    scattered,
    zsend,
    zrecv,
    ratio,
    ratio_quads,
    quads,
    part_high,
    part_low,
    top_send,
    bottom_send,
    after_recv,
    before_recv,
    vol_sem,
    in_sem,
    ex_send,
    ex_recv,
    ag_send,
    ag_recv,
    rs_send,
    rs_recv,
    z_send,
    z_recv,
    xg_send,
    xg_recv,
    halo_send,
    halo_recv,
    out_sem,
):
    tile = lax.axis_index("tile")
    depth = lax.axis_index("depth")
    core = lax.rem(tile, 2)
    zlo = lax.rem(tile // 2, 4)
    yrow = tile // 8
    xpos = lax.rem(depth, 4)
    zhi = depth // 4
    negative = tile >= 16
    block = jnp.where(negative, 31 - tile, tile)

    def at(y, z, c):
        return lax.rem(y, 4) * 8 + lax.rem(z, 4) * 2 + c

    def xpeer(d):
        return zhi * 4 + lax.rem(xpos + d, 4)

    after = lax.rem(tile + 1, 32)
    before = lax.rem(tile + 31, 32)
    zpartner = (1 - zhi) * 4 + xpos

    volume_copies = []
    for p in range(LOCAL_PLANES):
        volume_copies.append(
            pltpu.make_async_copy(volume_hbm.at[:, p], vol.at[:, p], vol_sem.at[p])
        )
    local = [
        pltpu.make_async_copy(mats_hbm, mats, in_sem.at[0]),
        pltpu.make_async_copy(measured_hbm, measured, in_sem.at[1]),
        pltpu.make_async_copy(background_hbm, background, in_sem.at[2]),
        pltpu.make_async_copy(transfer_hbm, transfer, in_sem.at[3]),
        pltpu.make_async_copy(pair_hbm, pair_ref, in_sem.at[4]),
        pltpu.make_async_copy(phases_hbm, phases, in_sem.at[5]),
        pltpu.make_async_copy(margins_hbm, margins, in_sem.at[6]),
    ]
    for which in (3, 4, 0, 5, 6):
        local[which].start()
    for copy in volume_copies:
        copy.start()
    local[1].start()
    local[2].start()

    barrier = pltpu.get_barrier_semaphore()

    def greet(t, d):
        pl.semaphore_signal(barrier, inc=1, device_id=(t, d), device_id_type=MESH)

    greet(31 - tile, depth)
    for dz in range(1, 4):
        greet(at(yrow, zlo + dz, core), depth)
    greet(at(yrow + 1, zlo, core), depth)
    greet(at(yrow + 3, zlo, core), depth)
    greet(at(yrow, zlo, 1 - core), depth)
    for d in range(1, 4):
        greet(tile, xpeer(d))
    greet(tile, zpartner)
    greet(after, depth)
    greet(before, depth)
    first_of = lax.rem(32 - tile, 16)
    last_to = jnp.where(tile == 16, 31, tile - 1)
    last_from = jnp.where(tile == 31, 16, tile + 1)
    row0_from = jnp.where(tile == 0, 16, 32 - tile)

    @pl.when(negative)
    def _():
        greet(first_of, depth)
        greet(last_to, depth)
        greet(last_from, depth)

    @pl.when(jnp.logical_not(negative))
    def _():
        greet(row0_from, depth)

    local[3].wait()
    local[4].wait()
    whole = transfer[...].reshape(LOCAL_PLANES * 2 * 8, SIDE)
    halves[0] = whole[:, :HALF]
    rest = whole[:, HALF:]
    high, low = split(rest)
    lowest = ((rest - high.astype(f32)) - low.astype(f32)).astype(bf16)
    move = pair_ref[...]
    halves[1] = dot(high, move) + dot(low, move) + dot(lowest, move)
    for r in range(8):
        to = jnp.where(negative, (8 - r) % 8, r)
        for ph in range(2):
            for e in range(2):
                for c in range(2):
                    piece = halves[e, pl.ds(ph * 64 + c * 8 + r, 4, stride=16), :]
                    mine[ph, to, pl.ds((e * 2 + c) * 4, 4), :] = piece

    pl.semaphore_wait(barrier, 14 + 2 * (tile // 16))

    def remote(src, dst, send, recv, t, d):
        return pltpu.make_async_remote_copy(
            src_ref=src,
            dst_ref=dst,
            send_sem=send,
            recv_sem=recv,
            device_id=(t, d),
            device_id_type=MESH,
        )

    rows7 = pl.ds(1, 7)
    row1 = pl.ds(0, 1)
    up_all = remote(mine.at[1], other, ex_send.at[0], ex_recv.at[0], 31 - tile, depth)
    down_rest = remote(
        mine.at[0, rows7], other.at[rows7], ex_send.at[0], ex_recv.at[0], 31 - tile, depth
    )
    down_first = remote(
        mine.at[0, row1], other.at[row1], ex_send.at[1], ex_recv.at[1], first_of, depth
    )
    down_last = remote(mine.at[1, row1], other0, ex_send.at[2], ex_recv.at[1], last_to, depth)

    @pl.when(jnp.logical_not(negative))
    def _():
        up_all.start()

    @pl.when(negative)
    def _():
        down_rest.start()
        down_first.start()
        down_last.start()

    left = lambda: (mats[0], mats[1])
    right = lambda: (mats[2], mats[3])
    inv_left = lambda: (mats[4], mats[5])
    inv_right = lambda: (mats[6], mats[7])
    local[0].wait()

    def forward(p, carry):
        pltpu.make_async_copy(volume_hbm.at[:, p], vol.at[:, p], vol_sem.at[p]).wait()
        for t in range(LOCAL_TILES):
            half = dot3(split(vol[t, p]), right())
            packed[t, p] = dot3(left(), split(half))
        return carry

    lax.fori_loop(0, LOCAL_PLANES, forward, 0)

    @pl.when(jnp.logical_not(negative))
    def _():
        down_rest.wait_recv()
        down_first.wait_recv()
        pos[...] = mine[0]
        neg[...] = other[...]

    @pl.when(negative)
    def _():
        up_all.wait_recv()
        down_last.wait_recv()
        pos[...] = other[...]
        neg[0] = other0[0]
        neg[1:8] = mine[1, 1:8]

    local[5].wait()
    local[6].wait()
    plane0 = jnp.where(negative, 4, 0)
    column = lax.broadcasted_iota(jnp.int32, (4, HALF), 1)
    row4 = lax.broadcasted_iota(jnp.int32, (4, HALF), 0)
    phase = jnp.zeros((4, HALF), jnp.int32)
    for q in range(4):
        phase = jnp.where(row4 == q, phases[plane0 + q], phase)
    lane0 = column == 0

    def rotor(columns):
        angle = ((phase * columns) & (SIDE - 1)).astype(f32) * (2.0 * math.pi / SIDE)
        return jnp.cos(angle), jnp.sin(angle)

    cos_p, sin_p = rotor(column)
    cos_m, sin_m = rotor(jnp.where(lane0, HALF, column))
    sin_m = jnp.where(lane0, 0.0, sin_m)
    is_first = block == 0
    for r in range(8):
        epr, epi, fpr, fpi = (pos[r, pl.ds(c * 4, 4), :] for c in range(4))
        enr, eni, fnr, fni = (neg[r, pl.ds(c * 4, 4), :] for c in range(4))
        hpr, hpi = 0.25 * (epr + fnr), 0.25 * (epi - fni)
        hmr, hmi = 0.25 * (enr + fpr), 0.25 * (eni - fpi)
        if r == 0:
            at0 = jnp.logical_and(is_first, jnp.logical_not(lane0))
            hpr = jnp.where(at0, 0.5 * (epr + fpr), hpr)
            hpi = jnp.where(at0, 0.5 * (epi - fpi), hpi)
            hmr = jnp.where(at0, 0.5 * (enr + fnr), hmr)
            hmi = jnp.where(at0, 0.5 * (eni - fni), hmi)
        lpr, lpi = 0.5 * (epr + enr), 0.5 * (epi - eni)
        lmr, lmi = 0.5 * (fpr + fnr), 0.5 * (fpi - fni)
        if r == 0:
            lpr, lpi = jnp.where(is_first, epr, lpr), jnp.where(is_first, enr, lpi)
            lmr, lmi = jnp.where(is_first, fpr, lmr), jnp.where(is_first, fnr, lmi)
        hpr, hpi = jnp.where(lane0, lpr, hpr), jnp.where(lane0, lpi, hpi)
        hmr, hmi = jnp.where(lane0, lmr, hmr), jnp.where(lane0, lmi, hmi)
        parts = (
            hpr * cos_p + hpi * sin_p,
            hpi * cos_p - hpr * sin_p,
            hmr * cos_m + hmi * sin_m,
            hmi * cos_m - hmr * sin_m,
        )
        for c in range(4):
            for q in range(4):
                table[tile, q, c, pl.ds(r, 1), :] = parts[c][q : q + 1]

    started = []

    def pass_on(which, t):
        copy = remote(
            table.at[which],
            table.at[which],
            ag_send.at[len(started)],
            ag_recv.at[which],
            t,
            depth,
        )
        copy.start()
        started.append(copy)

    def arrived(which):
        remote(
            table.at[which], table.at[which], ag_send.at[0], ag_recv.at[which], tile, depth
        ).wait_recv()

    above = at(yrow + 1, zlo, core)
    below = at(yrow + 3, zlo, core)
    sibling = at(yrow, zlo, 1 - core)
    z_order = (1, 3, 2)
    pass_on(tile, above)
    pass_on(tile, below)
    for dz in z_order:
        pass_on(tile, at(yrow, zlo + dz, core))
    pass_on(tile, sibling)

    for dz in z_order:
        which = at(yrow, zlo + dz, core)
        arrived(which)
        pass_on(which, above)
        pass_on(which, below)
        pass_on(which, sibling)

    for dz in (0, 1, 3, 2):
        which = at(yrow + 3, zlo + dz, core)
        arrived(which)
        if dz in (0, 1):
            pass_on(which, above)
        pass_on(which, sibling)
        which = at(yrow + 1, zlo + dz, core)
        arrived(which)
        if dz in (2, 3):
            pass_on(which, below)
        pass_on(which, sibling)
    def read_quads(ref, rows, rows2):
        return (
            ref[rows, pl.ds(0, HALF)],
            ref[rows, pl.ds(HALF, HALF)],
            ref[rows2, pl.ds(0, HALF)],
            ref[rows2, pl.ds(HALF, HALF)],
        )

    def rows_of(k):
        if isinstance(k, int):
            return pl.ds(8 * k, 8), pl.ds(HALF + 8 * k, 8)
        return pl.ds(pl.multiple_of(8 * k, 8), 8), pl.ds(pl.multiple_of(HALF + 8 * k, 8), 8)

    def table_of(p, k):
        which = k if p < 4 else 31 - k
        return tuple(table[which, p % 4, c] for c in range(4))

    def spectrum_block(t, k, first):
        rows, rows2 = rows_of(k)
        total = None
        for p in range(LOCAL_PLANES):
            hpr, hpi, hmr, hmi = table_of(p, k)
            pr, pi, mr, mi = quads_in(*read_quads(packed.at[t, p], rows, rows2), first)
            terms = times(hpr, hpi, pr, pi, first, False) + times(hmr, hmi, mr, mi, first, False)
            total = terms if total is None else tuple(a + b for a, b in zip(total, terms))
        cc, cs, sc, ss = quads_out(*total, first)
        sums[t, rows, pl.ds(0, HALF)] = cc
        sums[t, rows, pl.ds(HALF, HALF)] = cs
        sums[t, rows2, pl.ds(0, HALF)] = sc
        sums[t, rows2, pl.ds(HALF, HALF)] = ss

    def spectrum_group(t, start):
        for j in range(1, 8):
            spectrum_block(t, start + j, False)

    near = 8 * jnp.where(jnp.logical_or(yrow == 0, yrow == 3), 0, 1)
    far = 8 - near
    for dy in (0, 1, 3):
        for dz in range(4):
            arrived(at(yrow + dy, zlo + dz, 1 - core))
    spectrum_group(0, near)
    for dz in (0, 1, 3, 2):
        which = at(yrow + 2, zlo + dz, core)
        arrived(which)
        pass_on(which, sibling)
    spectrum_group(1, near)
    for dz in range(4):
        arrived(at(yrow + 2, zlo + dz, 1 - core))

    def rows_at(x, s):
        return pl.ds((s // 2) * SIDE + x * 64 + (s % 2) * SUB_ROWS, SUB_ROWS)

    rs_copies = []
    for t in range(LOCAL_TILES):
        spectrum_block(t, 0, True)
        spectrum_block(t, 8, False)
        spectrum_group(t, far)
        half = dot3(split(sums[t]), inv_right())
        image[pl.ds(t * SIDE, SIDE), :] = dot3(inv_left(), split(half))
        for s in (2 * t, 2 * t + 1):
            for d in (1, 3, 2):
                slot = (d - 1) * SUBS + s
                copy = remote(
                    image.at[rows_at(lax.rem(xpos + d, 4), s)],
                    scattered.at[d - 1, pl.ds(s * SUB_ROWS, SUB_ROWS)],
                    rs_send.at[slot],
                    rs_recv.at[slot],
                    tile,
                    xpeer(d),
                )
                copy.start()
                rs_copies.append(copy)
    z_copies = []
    for s in range(SUBS):
        for copy in rs_copies[3 * s : 3 * s + 3]:
            copy.wait_recv()
        rows = pl.ds(s * SUB_ROWS, SUB_ROWS)
        own = image[rows_at(xpos, s), :]
        zsend[rows, :] = own + scattered[0, rows, :] + scattered[1, rows, :] + scattered[2, rows, :]
        copy = remote(zsend.at[rows], zrecv.at[rows], z_send.at[s], z_recv.at[s], tile, zpartner)
        copy.start()
        z_copies.append(copy)
    local[1].wait()
    local[2].wait()
    xg_copies = []
    for s in range(SUBS):
        z_copies[s].wait_recv()
        rows = pl.ds(s * SUB_ROWS, SUB_ROWS)
        here = rows_at(xpos, s)
        projection = background[here, :] + (zsend[rows, :] + zrecv[rows, :])
        ratio[here, :] = measured[here, :] / jnp.maximum(projection, FLOOR_LEVEL) - 1.0
        for d in (1, 3, 2):
            slot = (d - 1) * SUBS + s
            copy = remote(
                ratio.at[here], ratio.at[here], xg_send.at[slot], xg_recv.at[slot], tile, xpeer(d)
            )
            copy.start()
            xg_copies.append(copy)

    def strip(p, t, image_part, rows):
        values = vol[t, p, rows, :]
        return jnp.maximum(values * (1.0 + STEP_GAIN * image_part), 0.0)

    def to_before(p):
        return remote(
            top_send.at[p], after_recv.at[p], halo_send.at[p], halo_recv.at[p], before, depth
        )

    def to_after(p):
        slot = LOCAL_PLANES + p
        return remote(
            bottom_send.at[p], before_recv.at[p], halo_send.at[slot], halo_recv.at[slot], after, depth
        )

    for t in range(LOCAL_TILES):
        for copy in xg_copies[6 * t : 6 * t + 6]:
            copy.wait_recv()
        half = dot3(split(ratio[pl.ds(t * SIDE, SIDE), :]), right())
        sums[t] = dot3(left(), split(half))
        for k in range(16):
            rows, rows2 = rows_of(k)
            found = quads_in(*read_quads(sums.at[t], rows, rows2), k == 0)
            for c in range(4):
                ratio_quads[t, c, rows, :] = found[c]

        def backward(q, carry, t=t):
            for h in range(2):
                p = q + 4 * h
                for k in range(16):
                    rows, rows2 = rows_of(k)
                    which = 31 - k if h else k
                    hpr, hpi, hmr, hmi = (table[which, q, c] for c in range(4))
                    pr, pi, mr, mi = (ratio_quads[t, c, rows, :] for c in range(4))
                    plus = times(hpr, hpi, pr, pi, k == 0, True)
                    minus = times(hmr, hmi, mr, mi, k == 0, True)
                    cc, cs, sc, ss = quads_out(*plus, *minus, k == 0)
                    quads[h, rows, pl.ds(0, HALF)] = cc
                    quads[h, rows, pl.ds(HALF, HALF)] = cs
                    quads[h, rows2, pl.ds(0, HALF)] = sc
                    quads[h, rows2, pl.ds(HALF, HALF)] = ss
                half = split(dot3(split(quads[h]), inv_right()))
                part_high[t, p] = half[0]
                part_low[t, p] = half[1]
                rows = slice(0, WIDTH) if t == 0 else slice(SIDE - WIDTH, SIDE)
                edge = strip(p, t, dot3((mats[4, rows], mats[5, rows]), half), rows)
                if t == 0:
                    top_send[p] = edge
                else:
                    bottom_send[p] = edge
            for h in range(2):
                (to_after if t else to_before)(q + 4 * h).start()
            return carry

        lax.fori_loop(0, 4, backward, 0)

    base = tile * LOCAL_TILES
    w_inner = ramp(margins[base])
    w_after = ramp(margins[base + 1])
    w_before = ramp(margins[lax.rem(base + TILES - 1, TILES)])

    def out_copies(p):
        return (
            pltpu.make_async_copy(
                vol.at[0, p, pl.ds(WIDTH, SIDE - WIDTH)],
                out_hbm.at[0, p, pl.ds(WIDTH, SIDE - WIDTH)],
                out_sem.at[2 * p],
            ),
            pltpu.make_async_copy(
                vol.at[1, p, pl.ds(0, SIDE - WIDTH)],
                out_hbm.at[1, p, pl.ds(0, SIDE - WIDTH)],
                out_sem.at[2 * p + 1],
            ),
        )

    def finish_plane(p, carry):
        half = (part_high[0, p], part_low[0, p])
        rows = slice(WIDTH, SIDE)
        upper = strip(p, 0, dot3((mats[4, rows], mats[5, rows]), half), rows)
        half = (part_high[1, p], part_low[1, p])
        rows = slice(0, SIDE - WIDTH)
        lower = strip(p, 1, dot3((mats[4, rows], mats[5, rows]), half), rows)
        inner = SIDE - 2 * WIDTH
        shared = (1.0 - w_inner) * upper[inner:] + w_inner * lower[:WIDTH]
        vol[0, p, WIDTH : SIDE - WIDTH, :] = upper[:inner]
        vol[0, p, SIDE - WIDTH :, :] = shared
        vol[1, p, :WIDTH, :] = shared
        vol[1, p, WIDTH : SIDE - WIDTH, :] = lower[WIDTH:]
        for copy in out_copies(p):
            copy.start()
        return carry

    lax.fori_loop(0, LOCAL_PLANES, finish_plane, 0)

    top_out = pltpu.make_async_copy(
        vol.at[0, :, pl.ds(0, WIDTH)], out_hbm.at[0, :, pl.ds(0, WIDTH)], out_sem.at[16]
    )
    bottom_out = pltpu.make_async_copy(
        vol.at[1, :, pl.ds(SIDE - WIDTH, WIDTH)],
        out_hbm.at[1, :, pl.ds(SIDE - WIDTH, WIDTH)],
        out_sem.at[17],
    )

    def last_strip(p, carry):
        to_before(p).wait_recv()
        vol[1, p, SIDE - WIDTH :, :] = (1.0 - w_after) * bottom_send[p] + w_after * after_recv[p]
        return carry

    lax.fori_loop(0, LOCAL_PLANES, last_strip, 0)
    bottom_out.start()

    def first_strip(p, carry):
        to_after(p).wait_recv()
        vol[0, p, :WIDTH, :] = (1.0 - w_before) * before_recv[p] + w_before * top_send[p]
        return carry

    lax.fori_loop(0, LOCAL_PLANES, first_strip, 0)
    top_out.start()

    @pl.when(jnp.logical_not(negative))
    def _():
        up_all.wait_send()

    @pl.when(negative)
    def _():
        down_rest.wait_send()
        down_first.wait_send()
        down_last.wait_send()

    for copy in started + rs_copies + z_copies + xg_copies:
        copy.wait_send()

    def drain(p, carry):
        to_before(p).wait_send()
        to_after(p).wait_send()
        for copy in out_copies(p):
            copy.wait()
        return carry

    lax.fori_loop(0, LOCAL_PLANES, drain, 0)
    top_out.wait()
    bottom_out.wait()


def on_device(volume, transfer, measured, background, margins, phases):
    mats = packed_tables()
    hbm = pl.BlockSpec(memory_space=pltpu.HBM)
    dma = pltpu.SemaphoreType.DMA
    tall = LOCAL_TILES * SIDE
    return pl.pallas_call(
        kernel,
        name="update",
        out_shape=jax.ShapeDtypeStruct(volume.shape, f32),
        in_specs=[hbm] * 8,
        out_specs=pl.BlockSpec(memory_space=pl.ANY),
        scratch_shapes=[
            pltpu.SMEM((LOCAL_PLANES,), jnp.int32),
            pltpu.SMEM((TILES,), jnp.int32),
            pltpu.VMEM((LOCAL_PLANES, 2, 8, SIDE), f32),
            pltpu.VMEM((HALF, HALF), bf16),
            pltpu.VMEM((LOCAL_TILES, LOCAL_PLANES, SIDE, SIDE), f32),
            pltpu.VMEM((LOCAL_TILES, LOCAL_PLANES, SIDE, SIDE), f32),
            pltpu.VMEM((32, 4, 4, 8, HALF), f32),
            pltpu.VMEM((8, SIDE, SIDE), bf16),
            pltpu.VMEM((tall, SIDE), f32),
            pltpu.VMEM((tall, SIDE), f32),
            pltpu.VMEM((2, HALF, HALF), f32),
            pltpu.VMEM((2, 8, 16, HALF), f32),
            pltpu.VMEM((8, 16, HALF), f32),
            pltpu.VMEM((1, 16, HALF), f32),
            pltpu.VMEM((8, 16, HALF), f32),
            pltpu.VMEM((8, 16, HALF), f32),
            pltpu.VMEM((LOCAL_TILES, SIDE, SIDE), f32),
            pltpu.VMEM((tall, SIDE), f32),
            pltpu.VMEM((3, 128, SIDE), f32),
            pltpu.VMEM((128, SIDE), f32),
            pltpu.VMEM((128, SIDE), f32),
            pltpu.VMEM((tall, SIDE), f32),
            pltpu.VMEM((LOCAL_TILES, 4, HALF, HALF), f32),
            pltpu.VMEM((LOCAL_TILES, SIDE, SIDE), f32),
            pltpu.VMEM((LOCAL_TILES, LOCAL_PLANES, SIDE, SIDE), bf16),
            pltpu.VMEM((LOCAL_TILES, LOCAL_PLANES, SIDE, SIDE), bf16),
            pltpu.VMEM((LOCAL_PLANES, WIDTH, SIDE), f32),
            pltpu.VMEM((LOCAL_PLANES, WIDTH, SIDE), f32),
            pltpu.VMEM((LOCAL_PLANES, WIDTH, SIDE), f32),
            pltpu.VMEM((LOCAL_PLANES, WIDTH, SIDE), f32),
            dma((LOCAL_PLANES,)),
            dma((7,)),
            dma((3,)),
            dma((2,)),
            dma((31,)),
            dma((32,)),
            dma((3 * SUBS,)),
            dma((3 * SUBS,)),
            dma((SUBS,)),
            dma((SUBS,)),
            dma((3 * SUBS,)),
            dma((3 * SUBS,)),
            dma((2 * LOCAL_PLANES,)),
            dma((2 * LOCAL_PLANES,)),
            dma((2 * LOCAL_PLANES + 2,)),
        ],
        compiler_params=pltpu.CompilerParams(
            collective_id=0, has_side_effects=True, vmem_limit_bytes=67043328
        ),
    )(
        phases,
        margins,
        transfer,
        volume,
        measured.reshape(tall, SIDE),
        background.reshape(tall, SIDE),
        mats,
        pairing(),
    )


def solution(mesh):
    return jax.shard_map(
        on_device,
        mesh=mesh,
        in_specs=(
            P("tile", "depth", None, None),
            P("depth", None, "tile", None),
            P("tile", None, None),
            P("tile", None, None),
            P(),
            P("depth"),
        ),
        out_specs=P("tile", "depth", None, None),
        check_vma=False,
    )
```

```python
import functools
import math

import jax
import jax.numpy as jnp
import numpy as np
from jax import lax
from jax.experimental import pallas as pl
from jax.experimental.pallas import tpu as pltpu
from jax.sharding import PartitionSpec as P

SIDE = 256
HALF = 128
WIDTH = 32
TILES = 64
LOCAL_TILES = 2
LOCAL_PLANES = 8
PIECES = 4
FLOOR_LEVEL = 0.5
STEP_GAIN = 2.0
MESH = pl.DeviceIdType.MESH
f32 = jnp.float32
bf16 = jnp.bfloat16


def packed_tables():
    place = np.arange(SIDE)
    table = np.zeros((SIDE, SIDE))
    for a in range(HALF):
        table[a] = np.cos(2 * np.pi * (a * place % SIDE) / SIDE)
    table[HALF] = 1.0 - 2.0 * (place % 2)
    for a in range(1, HALF):
        table[HALF + a] = np.sin(2 * np.pi * (a * place % SIDE) / SIDE)
    weight = np.full(SIDE, 2.0)
    weight[0] = weight[HALF] = 1.0
    inverse = table.T * weight / SIDE
    pieces = []
    for matrix in (table, table.T, inverse, inverse.T):
        high = matrix.astype(bf16)
        pieces += [high, (matrix - high.astype(np.float64)).astype(bf16)]
    return jnp.asarray(np.stack(pieces))


def pairing():
    move = np.zeros((HALF, HALF), np.float32)
    move[0, 0] = 1.0
    for b in range(1, HALF):
        move[HALF - b, b] = 1.0
    return jnp.asarray(move.astype(bf16))


def split(values):
    high = values.astype(bf16)
    return high, (values - high.astype(f32)).astype(bf16)


def dot(a, b):
    return jnp.dot(a, b, preferred_element_type=f32)


def dot3(a, b):
    return dot(a[0], b[0]) + dot(a[1], b[0]) + dot(a[0], b[1])


def special(shape, first):
    lane0 = lax.broadcasted_iota(jnp.int32, shape, 1) == 0
    row0 = None
    if first:
        row0 = jnp.logical_and(
            lax.broadcasted_iota(jnp.int32, shape, 0) == 0, jnp.logical_not(lane0)
        )
    return lane0, row0


def quads_in(cc, cs, sc, ss, first):
    lane0, row0 = special(cc.shape, first)
    pr, pi, mr, mi = cc - ss, cs + sc, cc + ss, cs - sc
    if first:
        pr = jnp.where(row0, cc, pr)
        pi = jnp.where(row0, cs, pi)
        mr = jnp.where(row0, sc, mr)
        mi = jnp.where(row0, ss, mi)
    return (
        jnp.where(lane0, cc, pr),
        jnp.where(lane0, sc, pi),
        jnp.where(lane0, cs, mr),
        jnp.where(lane0, ss, mi),
    )


def quads_out(pr, pi, mr, mi, first):
    lane0, row0 = special(pr.shape, first)
    cc, ss, cs, sc = pr + mr, mr - pr, pi + mi, pi - mi
    if first:
        cc = jnp.where(row0, pr, cc)
        cs = jnp.where(row0, pi, cs)
        sc = jnp.where(row0, mr, sc)
        ss = jnp.where(row0, mi, ss)
    return (
        jnp.where(lane0, pr, cc),
        jnp.where(lane0, mr, cs),
        jnp.where(lane0, pi, sc),
        jnp.where(lane0, mi, ss),
    )


def times(hr, hi, real, imag, first, conj):
    second = hr
    if first:
        lane0, _ = special(hr.shape, False)
        corner = jnp.logical_and(lane0, lax.broadcasted_iota(jnp.int32, hr.shape, 0) == 0)
        second = jnp.where(corner, hi, hr)
        hi = jnp.where(corner, 0.0, hi)
    if conj:
        return hr * real - hi * imag, second * imag + hi * real
    return hr * real + hi * imag, second * imag - hi * real


def ramp(margin):
    margin = margin.astype(f32)
    row = lax.broadcasted_iota(jnp.int32, (WIDTH, SIDE), 0).astype(f32)
    return jnp.clip((row + 0.5 - (WIDTH - margin) / 2.0) / margin, 0.0, 1.0)


def kernel(
    phases_hbm,
    margins_hbm,
    transfer_hbm,
    volume_hbm,
    measured_hbm,
    background_hbm,
    mats_hbm,
    pair_hbm,
    out_hbm,
    phases,
    margins,
    transfer,
    pair_ref,
    vol,
    packed,
    table,
    mats,
    measured,
    background,
    halves,
    mine,
    other,
    other0,
    pos,
    neg,
    sums,
    partial,
    scattered,
    zsend,
    zrecv,
    spectrum,
    ratio_quads,
    quads,
    part_high,
    part_low,
    top_send,
    bottom_send,
    after_recv,
    before_recv,
    vol_sem,
    in_sem,
    ex_send,
    ex_recv,
    ag_send,
    ag_recv,
    rs_send,
    rs_recv,
    z_send,
    z_recv,
    xg_send,
    xg_recv,
    halo_send,
    halo_recv,
    out_sem,
):
    tile = lax.axis_index("tile")
    depth = lax.axis_index("depth")
    core = lax.rem(tile, 2)
    zlo = lax.rem(tile // 2, 4)
    yrow = tile // 8
    xpos = lax.rem(depth, 4)
    zhi = depth // 4
    negative = tile >= 16
    block = jnp.where(negative, 31 - tile, tile)

    def at(y, z, c):
        return lax.rem(y, 4) * 8 + lax.rem(z, 4) * 2 + c

    def xpeer(d):
        return zhi * 4 + lax.rem(xpos + d, 4)

    after = lax.rem(tile + 1, 32)
    before = lax.rem(tile + 31, 32)
    zpartner = (1 - zhi) * 4 + xpos

    volume_copies = []
    for p in range(LOCAL_PLANES):
        volume_copies.append(
            pltpu.make_async_copy(volume_hbm.at[:, p], vol.at[:, p], vol_sem.at[p])
        )
    local = [
        pltpu.make_async_copy(mats_hbm, mats, in_sem.at[0]),
        pltpu.make_async_copy(measured_hbm, measured, in_sem.at[1]),
        pltpu.make_async_copy(background_hbm, background, in_sem.at[2]),
        pltpu.make_async_copy(transfer_hbm, transfer, in_sem.at[3]),
        pltpu.make_async_copy(pair_hbm, pair_ref, in_sem.at[4]),
        pltpu.make_async_copy(phases_hbm, phases, in_sem.at[5]),
        pltpu.make_async_copy(margins_hbm, margins, in_sem.at[6]),
    ]
    for which in (3, 4, 0, 5, 6):
        local[which].start()
    for copy in volume_copies:
        copy.start()
    local[1].start()
    local[2].start()

    barrier = pltpu.get_barrier_semaphore()

    def greet(t, d):
        pl.semaphore_signal(barrier, inc=1, device_id=(t, d), device_id_type=MESH)

    greet(31 - tile, depth)
    for dz in range(1, 4):
        greet(at(yrow, zlo + dz, core), depth)
    greet(at(yrow + 1, zlo, core), depth)
    greet(at(yrow + 3, zlo, core), depth)
    greet(at(yrow, zlo, 1 - core), depth)
    for d in range(1, 4):
        greet(tile, xpeer(d))
    greet(tile, zpartner)
    greet(after, depth)
    greet(before, depth)
    first_of = lax.rem(32 - tile, 16)
    last_to = jnp.where(tile == 16, 31, tile - 1)
    last_from = jnp.where(tile == 31, 16, tile + 1)
    row0_from = jnp.where(tile == 0, 16, 32 - tile)

    @pl.when(negative)
    def _():
        greet(first_of, depth)
        greet(last_to, depth)
        greet(last_from, depth)

    @pl.when(jnp.logical_not(negative))
    def _():
        greet(row0_from, depth)

    local[3].wait()
    local[4].wait()
    whole = transfer[...].reshape(LOCAL_PLANES * 2 * 8, SIDE)
    halves[0] = whole[:, :HALF]
    rest = whole[:, HALF:]
    high, low = split(rest)
    lowest = ((rest - high.astype(f32)) - low.astype(f32)).astype(bf16)
    move = pair_ref[...]
    halves[1] = dot(high, move) + dot(low, move) + dot(lowest, move)
    for r in range(8):
        to = jnp.where(negative, (8 - r) % 8, r)
        for ph in range(2):
            for e in range(2):
                for c in range(2):
                    piece = halves[e, pl.ds(ph * 64 + c * 8 + r, 4, stride=16), :]
                    mine[ph, to, pl.ds((e * 2 + c) * 4, 4), :] = piece

    pl.semaphore_wait(barrier, 14 + 2 * (tile // 16))

    def remote(src, dst, send, recv, t, d):
        return pltpu.make_async_remote_copy(
            src_ref=src,
            dst_ref=dst,
            send_sem=send,
            recv_sem=recv,
            device_id=(t, d),
            device_id_type=MESH,
        )

    rows7 = pl.ds(1, 7)
    row1 = pl.ds(0, 1)
    up_all = remote(mine.at[1], other, ex_send.at[0], ex_recv.at[0], 31 - tile, depth)
    down_rest = remote(
        mine.at[0, rows7], other.at[rows7], ex_send.at[0], ex_recv.at[0], 31 - tile, depth
    )
    down_first = remote(
        mine.at[0, row1], other.at[row1], ex_send.at[1], ex_recv.at[1], first_of, depth
    )
    down_last = remote(mine.at[1, row1], other0, ex_send.at[2], ex_recv.at[1], last_to, depth)

    @pl.when(jnp.logical_not(negative))
    def _():
        up_all.start()

    @pl.when(negative)
    def _():
        down_rest.start()
        down_first.start()
        down_last.start()

    left = lambda: (mats[0], mats[1])
    right = lambda: (mats[2], mats[3])
    inv_left = lambda: (mats[4], mats[5])
    inv_right = lambda: (mats[6], mats[7])
    local[0].wait()

    def forward(p, carry):
        pltpu.make_async_copy(volume_hbm.at[:, p], vol.at[:, p], vol_sem.at[p]).wait()
        for t in range(LOCAL_TILES):
            half = dot3(split(vol[t, p]), right())
            packed[t, p] = dot3(left(), split(half))
        return carry

    lax.fori_loop(0, LOCAL_PLANES, forward, 0)

    @pl.when(jnp.logical_not(negative))
    def _():
        down_rest.wait_recv()
        down_first.wait_recv()
        pos[...] = mine[0]
        neg[...] = other[...]

    @pl.when(negative)
    def _():
        up_all.wait_recv()
        down_last.wait_recv()
        pos[...] = other[...]
        neg[0] = other0[0]
        neg[1:8] = mine[1, 1:8]

    local[5].wait()
    local[6].wait()
    plane0 = jnp.where(negative, 4, 0)
    column = lax.broadcasted_iota(jnp.int32, (4, HALF), 1)
    row4 = lax.broadcasted_iota(jnp.int32, (4, HALF), 0)
    phase = jnp.zeros((4, HALF), jnp.int32)
    for q in range(4):
        phase = jnp.where(row4 == q, phases[plane0 + q], phase)
    lane0 = column == 0

    def rotor(columns):
        angle = ((phase * columns) & (SIDE - 1)).astype(f32) * (2.0 * math.pi / SIDE)
        return jnp.cos(angle), jnp.sin(angle)

    cos_p, sin_p = rotor(column)
    cos_m, sin_m = rotor(jnp.where(lane0, HALF, column))
    sin_m = jnp.where(lane0, 0.0, sin_m)
    is_first = block == 0
    for r in range(8):
        epr, epi, fpr, fpi = (pos[r, pl.ds(c * 4, 4), :] for c in range(4))
        enr, eni, fnr, fni = (neg[r, pl.ds(c * 4, 4), :] for c in range(4))
        hpr, hpi = 0.25 * (epr + fnr), 0.25 * (epi - fni)
        hmr, hmi = 0.25 * (enr + fpr), 0.25 * (eni - fpi)
        if r == 0:
            at0 = jnp.logical_and(is_first, jnp.logical_not(lane0))
            hpr = jnp.where(at0, 0.5 * (epr + fpr), hpr)
            hpi = jnp.where(at0, 0.5 * (epi - fpi), hpi)
            hmr = jnp.where(at0, 0.5 * (enr + fnr), hmr)
            hmi = jnp.where(at0, 0.5 * (eni - fni), hmi)
        lpr, lpi = 0.5 * (epr + enr), 0.5 * (epi - eni)
        lmr, lmi = 0.5 * (fpr + fnr), 0.5 * (fpi - fni)
        if r == 0:
            lpr, lpi = jnp.where(is_first, epr, lpr), jnp.where(is_first, enr, lpi)
            lmr, lmi = jnp.where(is_first, fpr, lmr), jnp.where(is_first, fnr, lmi)
        hpr, hpi = jnp.where(lane0, lpr, hpr), jnp.where(lane0, lpi, hpi)
        hmr, hmi = jnp.where(lane0, lmr, hmr), jnp.where(lane0, lmi, hmi)
        parts = (
            hpr * cos_p + hpi * sin_p,
            hpi * cos_p - hpr * sin_p,
            hmr * cos_m + hmi * sin_m,
            hmi * cos_m - hmr * sin_m,
        )
        for c in range(4):
            for q in range(4):
                table[tile, q, c, pl.ds(r, 1), :] = parts[c][q : q + 1]

    started = []

    def pass_on(which, t):
        copy = remote(
            table.at[which],
            table.at[which],
            ag_send.at[len(started)],
            ag_recv.at[which],
            t,
            depth,
        )
        copy.start()
        started.append(copy)

    def arrived(which):
        remote(
            table.at[which], table.at[which], ag_send.at[0], ag_recv.at[which], tile, depth
        ).wait_recv()

    above = at(yrow + 1, zlo, core)
    below = at(yrow + 3, zlo, core)
    sibling = at(yrow, zlo, 1 - core)
    z_order = (1, 3, 2)
    pass_on(tile, above)
    pass_on(tile, below)
    for dz in z_order:
        pass_on(tile, at(yrow, zlo + dz, core))
    pass_on(tile, sibling)

    for dz in z_order:
        which = at(yrow, zlo + dz, core)
        arrived(which)
        pass_on(which, above)
        pass_on(which, below)
        pass_on(which, sibling)

    for dz in (0, 1, 3, 2):
        which = at(yrow + 3, zlo + dz, core)
        arrived(which)
        if dz in (0, 1):
            pass_on(which, above)
        pass_on(which, sibling)
        which = at(yrow + 1, zlo + dz, core)
        arrived(which)
        if dz in (2, 3):
            pass_on(which, below)
        pass_on(which, sibling)
    def read_quads(ref, rows, rows2):
        return (
            ref[rows, pl.ds(0, HALF)],
            ref[rows, pl.ds(HALF, HALF)],
            ref[rows2, pl.ds(0, HALF)],
            ref[rows2, pl.ds(HALF, HALF)],
        )

    def rows_of(k):
        if isinstance(k, int):
            return pl.ds(8 * k, 8), pl.ds(HALF + 8 * k, 8)
        return pl.ds(pl.multiple_of(8 * k, 8), 8), pl.ds(pl.multiple_of(HALF + 8 * k, 8), 8)

    def table_of(p, k):
        which = k if p < 4 else 31 - k
        return tuple(table[which, p % 4, c] for c in range(4))

    def spectrum_block(t, g, j, first):
        k = 8 * g + j
        rows, rows2 = rows_of(k)
        total = None
        for p in range(LOCAL_PLANES):
            hpr, hpi, hmr, hmi = table_of(p, k)
            pr, pi, mr, mi = quads_in(*read_quads(packed.at[t, p], rows, rows2), first)
            terms = times(hpr, hpi, pr, pi, first, False) + times(hmr, hmi, mr, mi, first, False)
            total = terms if total is None else tuple(a + b for a, b in zip(total, terms))
        cc, cs, sc, ss = quads_out(*total, first)
        upper, lower = pl.ds(8 * (j % 2), 8), pl.ds(16 + 8 * (j % 2), 8)
        partial[t, g, j // 2, upper, pl.ds(0, HALF)] = cc
        partial[t, g, j // 2, upper, pl.ds(HALF, HALF)] = cs
        partial[t, g, j // 2, lower, pl.ds(0, HALF)] = sc
        partial[t, g, j // 2, lower, pl.ds(HALF, HALF)] = ss

    rs_copies = []

    def spectrum_group(t, g):
        for j in range(1, 8):
            spectrum_block(t, g, j, False)

        @pl.when(g == 0)
        def _():
            spectrum_block(t, 0, 0, True)

        @pl.when(g == 1)
        def _():
            spectrum_block(t, 1, 0, False)

        s = len(rs_copies) // 3
        for d in (1, 3, 2):
            copy = remote(
                partial.at[t, g, lax.rem(xpos + d, 4)],
                scattered.at[d - 1, s],
                rs_send.at[3 * s + d - 1],
                rs_recv.at[3 * s + d - 1],
                tile,
                xpeer(d),
            )
            copy.start()
            rs_copies.append(copy)

    near = jnp.where(jnp.logical_or(yrow == 0, yrow == 3), 0, 1)
    far = 1 - near
    for dy in (0, 1, 3):
        for dz in range(4):
            arrived(at(yrow + dy, zlo + dz, 1 - core))
    spectrum_group(0, near)
    for dz in (0, 1, 3, 2):
        which = at(yrow + 2, zlo + dz, core)
        arrived(which)
        pass_on(which, sibling)
    spectrum_group(1, near)
    for dz in range(4):
        arrived(at(yrow + 2, zlo + dz, 1 - core))
    spectrum_group(0, far)
    spectrum_group(1, far)
    pieces = ((0, near), (1, near), (0, far), (1, far))
    z_copies = []
    for s, (t, g) in enumerate(pieces):
        for copy in rs_copies[3 * s : 3 * s + 3]:
            copy.wait_recv()
        zsend[s] = partial[t, g, xpos] + scattered[0, s] + scattered[1, s] + scattered[2, s]
        copy = remote(zsend.at[s], zrecv.at[s], z_send.at[s], z_recv.at[s], tile, zpartner)
        copy.start()
        z_copies.append(copy)
    local[1].wait()
    local[2].wait()
    xg_copies = []
    for s, (t, g) in enumerate(pieces):
        z_copies[s].wait_recv()
        spectrum[t, g, xpos] = zsend[s] + zrecv[s]
        for d in (1, 3, 2):
            copy = remote(
                spectrum.at[t, g, xpos],
                spectrum.at[t, g, xpos],
                xg_send.at[3 * s + d - 1],
                xg_recv.at[3 * s + d - 1],
                tile,
                xpeer(d),
            )
            copy.start()
            xg_copies.append(copy)

    def strip(p, t, image_part, rows):
        values = vol[t, p, rows, :]
        return jnp.maximum(values * (1.0 + STEP_GAIN * image_part), 0.0)

    def to_before(p):
        return remote(
            top_send.at[p], after_recv.at[p], halo_send.at[p], halo_recv.at[p], before, depth
        )

    def to_after(p):
        slot = LOCAL_PLANES + p
        return remote(
            bottom_send.at[p], before_recv.at[p], halo_send.at[slot], halo_recv.at[slot], after, depth
        )

    for t in range(LOCAL_TILES):
        for copy in xg_copies[3 * t : 3 * t + 3] + xg_copies[3 * t + 6 : 3 * t + 9]:
            copy.wait_recv()
        for k in range(16):
            rows, rows2 = rows_of(k)
            found = spectrum.at[t, k // 8, (k % 8) // 2]
            sums[t, rows, :] = found[pl.ds(8 * (k % 2), 8), :]
            sums[t, rows2, :] = found[pl.ds(16 + 8 * (k % 2), 8), :]
        half = dot3(split(sums[t]), inv_right())
        here = pl.ds(t * SIDE, SIDE)
        projection = background[here, :] + dot3(inv_left(), split(half))
        ratio = measured[here, :] / jnp.maximum(projection, FLOOR_LEVEL)
        half = dot3(split(ratio - 1.0), right())
        sums[t] = dot3(left(), split(half))
        for k in range(16):
            rows, rows2 = rows_of(k)
            found = quads_in(*read_quads(sums.at[t], rows, rows2), k == 0)
            for c in range(4):
                ratio_quads[t, c, rows, :] = found[c]

        def backward(q, carry, t=t):
            for h in range(2):
                p = q + 4 * h
                for k in range(16):
                    rows, rows2 = rows_of(k)
                    which = 31 - k if h else k
                    hpr, hpi, hmr, hmi = (table[which, q, c] for c in range(4))
                    pr, pi, mr, mi = (ratio_quads[t, c, rows, :] for c in range(4))
                    plus = times(hpr, hpi, pr, pi, k == 0, True)
                    minus = times(hmr, hmi, mr, mi, k == 0, True)
                    cc, cs, sc, ss = quads_out(*plus, *minus, k == 0)
                    quads[h, rows, pl.ds(0, HALF)] = cc
                    quads[h, rows, pl.ds(HALF, HALF)] = cs
                    quads[h, rows2, pl.ds(0, HALF)] = sc
                    quads[h, rows2, pl.ds(HALF, HALF)] = ss
                half = split(dot3(split(quads[h]), inv_right()))
                part_high[t, p] = half[0]
                part_low[t, p] = half[1]
                rows = slice(0, WIDTH) if t == 0 else slice(SIDE - WIDTH, SIDE)
                edge = strip(p, t, dot3((mats[4, rows], mats[5, rows]), half), rows)
                if t == 0:
                    top_send[p] = edge
                else:
                    bottom_send[p] = edge
            for h in range(2):
                (to_after if t else to_before)(q + 4 * h).start()
            return carry

        lax.fori_loop(0, 4, backward, 0)

    base = tile * LOCAL_TILES
    w_inner = ramp(margins[base])
    w_after = ramp(margins[base + 1])
    w_before = ramp(margins[lax.rem(base + TILES - 1, TILES)])

    def out_copies(p):
        return (
            pltpu.make_async_copy(
                vol.at[0, p, pl.ds(WIDTH, SIDE - WIDTH)],
                out_hbm.at[0, p, pl.ds(WIDTH, SIDE - WIDTH)],
                out_sem.at[2 * p],
            ),
            pltpu.make_async_copy(
                vol.at[1, p, pl.ds(0, SIDE - WIDTH)],
                out_hbm.at[1, p, pl.ds(0, SIDE - WIDTH)],
                out_sem.at[2 * p + 1],
            ),
        )

    def finish_plane(p, carry):
        half = (part_high[0, p], part_low[0, p])
        rows = slice(WIDTH, SIDE)
        upper = strip(p, 0, dot3((mats[4, rows], mats[5, rows]), half), rows)
        half = (part_high[1, p], part_low[1, p])
        rows = slice(0, SIDE - WIDTH)
        lower = strip(p, 1, dot3((mats[4, rows], mats[5, rows]), half), rows)
        inner = SIDE - 2 * WIDTH
        shared = (1.0 - w_inner) * upper[inner:] + w_inner * lower[:WIDTH]
        vol[0, p, WIDTH : SIDE - WIDTH, :] = upper[:inner]
        vol[0, p, SIDE - WIDTH :, :] = shared
        vol[1, p, :WIDTH, :] = shared
        vol[1, p, WIDTH : SIDE - WIDTH, :] = lower[WIDTH:]
        for copy in out_copies(p):
            copy.start()
        return carry

    lax.fori_loop(0, LOCAL_PLANES, finish_plane, 0)

    top_out = pltpu.make_async_copy(
        vol.at[0, :, pl.ds(0, WIDTH)], out_hbm.at[0, :, pl.ds(0, WIDTH)], out_sem.at[16]
    )
    bottom_out = pltpu.make_async_copy(
        vol.at[1, :, pl.ds(SIDE - WIDTH, WIDTH)],
        out_hbm.at[1, :, pl.ds(SIDE - WIDTH, WIDTH)],
        out_sem.at[17],
    )

    def last_strip(p, carry):
        to_before(p).wait_recv()
        vol[1, p, SIDE - WIDTH :, :] = (1.0 - w_after) * bottom_send[p] + w_after * after_recv[p]
        return carry

    lax.fori_loop(0, LOCAL_PLANES, last_strip, 0)
    bottom_out.start()

    def first_strip(p, carry):
        to_after(p).wait_recv()
        vol[0, p, :WIDTH, :] = (1.0 - w_before) * before_recv[p] + w_before * top_send[p]
        return carry

    lax.fori_loop(0, LOCAL_PLANES, first_strip, 0)
    top_out.start()

    @pl.when(jnp.logical_not(negative))
    def _():
        up_all.wait_send()

    @pl.when(negative)
    def _():
        down_rest.wait_send()
        down_first.wait_send()
        down_last.wait_send()

    for copy in started + rs_copies + z_copies + xg_copies:
        copy.wait_send()

    def drain(p, carry):
        to_before(p).wait_send()
        to_after(p).wait_send()
        for copy in out_copies(p):
            copy.wait()
        return carry

    lax.fori_loop(0, LOCAL_PLANES, drain, 0)
    top_out.wait()
    bottom_out.wait()


def on_device(volume, transfer, measured, background, margins, phases):
    mats = packed_tables()
    hbm = pl.BlockSpec(memory_space=pltpu.HBM)
    dma = pltpu.SemaphoreType.DMA
    tall = LOCAL_TILES * SIDE
    return pl.pallas_call(
        kernel,
        name="update",
        out_shape=jax.ShapeDtypeStruct(volume.shape, f32),
        in_specs=[hbm] * 8,
        out_specs=pl.BlockSpec(memory_space=pl.ANY),
        scratch_shapes=[
            pltpu.SMEM((LOCAL_PLANES,), jnp.int32),
            pltpu.SMEM((TILES,), jnp.int32),
            pltpu.VMEM((LOCAL_PLANES, 2, 8, SIDE), f32),
            pltpu.VMEM((HALF, HALF), bf16),
            pltpu.VMEM((LOCAL_TILES, LOCAL_PLANES, SIDE, SIDE), f32),
            pltpu.VMEM((LOCAL_TILES, LOCAL_PLANES, SIDE, SIDE), f32),
            pltpu.VMEM((32, 4, 4, 8, HALF), f32),
            pltpu.VMEM((8, SIDE, SIDE), bf16),
            pltpu.VMEM((tall, SIDE), f32),
            pltpu.VMEM((tall, SIDE), f32),
            pltpu.VMEM((2, HALF, HALF), f32),
            pltpu.VMEM((2, 8, 16, HALF), f32),
            pltpu.VMEM((8, 16, HALF), f32),
            pltpu.VMEM((1, 16, HALF), f32),
            pltpu.VMEM((8, 16, HALF), f32),
            pltpu.VMEM((8, 16, HALF), f32),
            pltpu.VMEM((LOCAL_TILES, SIDE, SIDE), f32),
            pltpu.VMEM((LOCAL_TILES, 2, 4, WIDTH, SIDE), f32),
            pltpu.VMEM((3, PIECES, WIDTH, SIDE), f32),
            pltpu.VMEM((PIECES, WIDTH, SIDE), f32),
            pltpu.VMEM((PIECES, WIDTH, SIDE), f32),
            pltpu.VMEM((LOCAL_TILES, 2, 4, WIDTH, SIDE), f32),
            pltpu.VMEM((LOCAL_TILES, 4, HALF, HALF), f32),
            pltpu.VMEM((LOCAL_TILES, SIDE, SIDE), f32),
            pltpu.VMEM((LOCAL_TILES, LOCAL_PLANES, SIDE, SIDE), bf16),
            pltpu.VMEM((LOCAL_TILES, LOCAL_PLANES, SIDE, SIDE), bf16),
            pltpu.VMEM((LOCAL_PLANES, WIDTH, SIDE), f32),
            pltpu.VMEM((LOCAL_PLANES, WIDTH, SIDE), f32),
            pltpu.VMEM((LOCAL_PLANES, WIDTH, SIDE), f32),
            pltpu.VMEM((LOCAL_PLANES, WIDTH, SIDE), f32),
            dma((LOCAL_PLANES,)),
            dma((7,)),
            dma((3,)),
            dma((2,)),
            dma((31,)),
            dma((32,)),
            dma((3 * PIECES,)),
            dma((3 * PIECES,)),
            dma((PIECES,)),
            dma((PIECES,)),
            dma((3 * PIECES,)),
            dma((3 * PIECES,)),
            dma((2 * LOCAL_PLANES,)),
            dma((2 * LOCAL_PLANES,)),
            dma((2 * LOCAL_PLANES + 2,)),
        ],
        compiler_params=pltpu.CompilerParams(
            collective_id=0, has_side_effects=True, vmem_limit_bytes=48 * 1024 * 1024
        ),
    )(
        *(
            pltpu.with_memory_space_constraint(array, pltpu.HBM)
            for array in (
                phases,
                margins,
                transfer,
                volume,
                measured.reshape(tall, SIDE),
                background.reshape(tall, SIDE),
                mats,
                pairing(),
            )
        )
    )


def solution(mesh):
    return jax.shard_map(
        on_device,
        mesh=mesh,
        in_specs=(
            P("tile", "depth", None, None),
            P("depth", None, "tile", None),
            P("tile", None, None),
            P("tile", None, None),
            P(),
            P("depth"),
        ),
        out_specs=P("tile", "depth", None, None),
        check_vma=False,
    )
```

```python
import functools
import math

import jax
import jax.numpy as jnp
import numpy as np
from jax import lax
from jax.experimental import pallas as pl
from jax.experimental.pallas import tpu as pltpu
from jax.sharding import PartitionSpec as P

SIDE = 256
HALF = 128
WIDTH = 32
TILES = 64
LOCAL_TILES = 2
LOCAL_PLANES = 8
PIECES = 4
FLOOR_LEVEL = 0.5
STEP_GAIN = 2.0
MESH = pl.DeviceIdType.MESH
f32 = jnp.float32
bf16 = jnp.bfloat16


def packed_tables():
    place = np.arange(SIDE)
    table = np.zeros((SIDE, SIDE))
    for a in range(HALF):
        table[a] = np.cos(2 * np.pi * (a * place % SIDE) / SIDE)
    table[HALF] = 1.0 - 2.0 * (place % 2)
    for a in range(1, HALF):
        table[HALF + a] = np.sin(2 * np.pi * (a * place % SIDE) / SIDE)
    weight = np.full(SIDE, 2.0)
    weight[0] = weight[HALF] = 1.0
    inverse = table.T * weight / SIDE
    pieces = []
    for matrix in (table, table.T, inverse, inverse.T):
        high = matrix.astype(bf16)
        pieces += [high, (matrix - high.astype(np.float64)).astype(bf16)]
    return jnp.asarray(np.stack(pieces))


def pairing():
    move = np.zeros((HALF, HALF), np.float32)
    move[0, 0] = 1.0
    for b in range(1, HALF):
        move[HALF - b, b] = 1.0
    return jnp.asarray(move.astype(bf16))


def split(values):
    high = values.astype(bf16)
    return high, (values - high.astype(f32)).astype(bf16)


def dot(a, b):
    return jnp.dot(a, b, preferred_element_type=f32)


def dot3(a, b):
    return dot(a[0], b[0]) + dot(a[1], b[0]) + dot(a[0], b[1])


def special(shape, first):
    lane0 = lax.broadcasted_iota(jnp.int32, shape, 1) == 0
    row0 = None
    if first:
        row0 = jnp.logical_and(
            lax.broadcasted_iota(jnp.int32, shape, 0) == 0, jnp.logical_not(lane0)
        )
    return lane0, row0


def quads_in(cc, cs, sc, ss, first):
    lane0, row0 = special(cc.shape, first)
    pr, pi, mr, mi = cc - ss, cs + sc, cc + ss, cs - sc
    if first:
        pr = jnp.where(row0, cc, pr)
        pi = jnp.where(row0, cs, pi)
        mr = jnp.where(row0, sc, mr)
        mi = jnp.where(row0, ss, mi)
    return (
        jnp.where(lane0, cc, pr),
        jnp.where(lane0, sc, pi),
        jnp.where(lane0, cs, mr),
        jnp.where(lane0, ss, mi),
    )


def quads_out(pr, pi, mr, mi, first):
    lane0, row0 = special(pr.shape, first)
    cc, ss, cs, sc = pr + mr, mr - pr, pi + mi, pi - mi
    if first:
        cc = jnp.where(row0, pr, cc)
        cs = jnp.where(row0, pi, cs)
        sc = jnp.where(row0, mr, sc)
        ss = jnp.where(row0, mi, ss)
    return (
        jnp.where(lane0, pr, cc),
        jnp.where(lane0, mr, cs),
        jnp.where(lane0, pi, sc),
        jnp.where(lane0, mi, ss),
    )


def times(hr, hi, real, imag, first, conj):
    second = hr
    if first:
        lane0, _ = special(hr.shape, False)
        corner = jnp.logical_and(lane0, lax.broadcasted_iota(jnp.int32, hr.shape, 0) == 0)
        second = jnp.where(corner, hi, hr)
        hi = jnp.where(corner, 0.0, hi)
    if conj:
        return hr * real - hi * imag, second * imag + hi * real
    return hr * real + hi * imag, second * imag - hi * real


def ramp(margin):
    margin = margin.astype(f32)
    row = lax.broadcasted_iota(jnp.int32, (WIDTH, SIDE), 0).astype(f32)
    return jnp.clip((row + 0.5 - (WIDTH - margin) / 2.0) / margin, 0.0, 1.0)


def kernel(
    phases_hbm,
    margins_hbm,
    transfer_hbm,
    volume_hbm,
    measured_hbm,
    background_hbm,
    mats_hbm,
    pair_hbm,
    out,
    phases,
    margins,
    transfer,
    pair_ref,
    vol,
    packed,
    table,
    mats,
    measured,
    background,
    halves,
    mine,
    other,
    other0,
    pos,
    neg,
    sums,
    partial,
    scattered,
    zsend,
    zrecv,
    spectrum,
    ratio_quads,
    quads,
    part_high,
    part_low,
    top_send,
    bottom_send,
    after_recv,
    before_recv,
    vol_sem,
    in_sem,
    ex_send,
    ex_recv,
    ag_send,
    ag_recv,
    rs_send,
    rs_recv,
    z_send,
    z_recv,
    xg_send,
    xg_recv,
    halo_send,
    halo_recv,
):
    tile = lax.axis_index("tile")
    depth = lax.axis_index("depth")
    core = lax.rem(tile, 2)
    zlo = lax.rem(tile // 2, 4)
    yrow = tile // 8
    xpos = lax.rem(depth, 4)
    zhi = depth // 4
    negative = tile >= 16
    block = jnp.where(negative, 31 - tile, tile)

    def at(y, z, c):
        return lax.rem(y, 4) * 8 + lax.rem(z, 4) * 2 + c

    def xpeer(d):
        return zhi * 4 + lax.rem(xpos + d, 4)

    after = lax.rem(tile + 1, 32)
    before = lax.rem(tile + 31, 32)
    zpartner = (1 - zhi) * 4 + xpos

    volume_copies = []
    for p in range(LOCAL_PLANES):
        volume_copies.append(
            pltpu.make_async_copy(volume_hbm.at[:, p], vol.at[:, p], vol_sem.at[p])
        )
    local = [
        pltpu.make_async_copy(mats_hbm, mats, in_sem.at[0]),
        pltpu.make_async_copy(measured_hbm, measured, in_sem.at[1]),
        pltpu.make_async_copy(background_hbm, background, in_sem.at[2]),
        pltpu.make_async_copy(transfer_hbm, transfer, in_sem.at[3]),
        pltpu.make_async_copy(pair_hbm, pair_ref, in_sem.at[4]),
        pltpu.make_async_copy(phases_hbm, phases, in_sem.at[5]),
        pltpu.make_async_copy(margins_hbm, margins, in_sem.at[6]),
    ]
    for which in (3, 4, 0, 5, 6):
        local[which].start()
    for copy in volume_copies:
        copy.start()
    local[1].start()
    local[2].start()

    barrier = pltpu.get_barrier_semaphore()

    def greet(t, d):
        pl.semaphore_signal(barrier, inc=1, device_id=(t, d), device_id_type=MESH)

    greet(31 - tile, depth)
    for dz in range(1, 4):
        greet(at(yrow, zlo + dz, core), depth)
    greet(at(yrow + 1, zlo, core), depth)
    greet(at(yrow + 3, zlo, core), depth)
    greet(at(yrow, zlo, 1 - core), depth)
    for d in range(1, 4):
        greet(tile, xpeer(d))
    greet(tile, zpartner)
    greet(after, depth)
    greet(before, depth)
    first_of = lax.rem(32 - tile, 16)
    last_to = jnp.where(tile == 16, 31, tile - 1)
    last_from = jnp.where(tile == 31, 16, tile + 1)
    row0_from = jnp.where(tile == 0, 16, 32 - tile)

    @pl.when(negative)
    def _():
        greet(first_of, depth)
        greet(last_to, depth)
        greet(last_from, depth)

    @pl.when(jnp.logical_not(negative))
    def _():
        greet(row0_from, depth)

    local[3].wait()
    local[4].wait()
    whole = transfer[...].reshape(LOCAL_PLANES * 2 * 8, SIDE)
    halves[0] = whole[:, :HALF]
    rest = whole[:, HALF:]
    high, low = split(rest)
    lowest = ((rest - high.astype(f32)) - low.astype(f32)).astype(bf16)
    move = pair_ref[...]
    halves[1] = dot(high, move) + dot(low, move) + dot(lowest, move)
    for r in range(8):
        to = jnp.where(negative, (8 - r) % 8, r)
        for ph in range(2):
            for e in range(2):
                for c in range(2):
                    piece = halves[e, pl.ds(ph * 64 + c * 8 + r, 4, stride=16), :]
                    mine[ph, to, pl.ds((e * 2 + c) * 4, 4), :] = piece

    pl.semaphore_wait(barrier, 14 + 2 * (tile // 16))

    def remote(src, dst, send, recv, t, d):
        return pltpu.make_async_remote_copy(
            src_ref=src,
            dst_ref=dst,
            send_sem=send,
            recv_sem=recv,
            device_id=(t, d),
            device_id_type=MESH,
        )

    rows7 = pl.ds(1, 7)
    row1 = pl.ds(0, 1)
    up_all = remote(mine.at[1], other, ex_send.at[0], ex_recv.at[0], 31 - tile, depth)
    down_rest = remote(
        mine.at[0, rows7], other.at[rows7], ex_send.at[0], ex_recv.at[0], 31 - tile, depth
    )
    down_first = remote(
        mine.at[0, row1], other.at[row1], ex_send.at[1], ex_recv.at[1], first_of, depth
    )
    down_last = remote(mine.at[1, row1], other0, ex_send.at[2], ex_recv.at[1], last_to, depth)

    @pl.when(jnp.logical_not(negative))
    def _():
        up_all.start()

    @pl.when(negative)
    def _():
        down_rest.start()
        down_first.start()
        down_last.start()

    left = lambda: (mats[0], mats[1])
    right = lambda: (mats[2], mats[3])
    inv_left = lambda: (mats[4], mats[5])
    inv_right = lambda: (mats[6], mats[7])
    local[0].wait()

    def forward(p, carry):
        pltpu.make_async_copy(volume_hbm.at[:, p], vol.at[:, p], vol_sem.at[p]).wait()
        for t in range(LOCAL_TILES):
            half = dot3(split(vol[t, p]), right())
            packed[t, p] = dot3(left(), split(half))
        return carry

    lax.fori_loop(0, LOCAL_PLANES, forward, 0)

    @pl.when(jnp.logical_not(negative))
    def _():
        down_rest.wait_recv()
        down_first.wait_recv()
        pos[...] = mine[0]
        neg[...] = other[...]

    @pl.when(negative)
    def _():
        up_all.wait_recv()
        down_last.wait_recv()
        pos[...] = other[...]
        neg[0] = other0[0]
        neg[1:8] = mine[1, 1:8]

    local[5].wait()
    local[6].wait()
    plane0 = jnp.where(negative, 4, 0)
    column = lax.broadcasted_iota(jnp.int32, (4, HALF), 1)
    row4 = lax.broadcasted_iota(jnp.int32, (4, HALF), 0)
    phase = jnp.zeros((4, HALF), jnp.int32)
    for q in range(4):
        phase = jnp.where(row4 == q, phases[plane0 + q], phase)
    lane0 = column == 0

    def rotor(columns):
        angle = ((phase * columns) & (SIDE - 1)).astype(f32) * (2.0 * math.pi / SIDE)
        return jnp.cos(angle), jnp.sin(angle)

    cos_p, sin_p = rotor(column)
    cos_m, sin_m = rotor(jnp.where(lane0, HALF, column))
    sin_m = jnp.where(lane0, 0.0, sin_m)
    is_first = block == 0
    for r in range(8):
        epr, epi, fpr, fpi = (pos[r, pl.ds(c * 4, 4), :] for c in range(4))
        enr, eni, fnr, fni = (neg[r, pl.ds(c * 4, 4), :] for c in range(4))
        hpr, hpi = 0.25 * (epr + fnr), 0.25 * (epi - fni)
        hmr, hmi = 0.25 * (enr + fpr), 0.25 * (eni - fpi)
        if r == 0:
            at0 = jnp.logical_and(is_first, jnp.logical_not(lane0))
            hpr = jnp.where(at0, 0.5 * (epr + fpr), hpr)
            hpi = jnp.where(at0, 0.5 * (epi - fpi), hpi)
            hmr = jnp.where(at0, 0.5 * (enr + fnr), hmr)
            hmi = jnp.where(at0, 0.5 * (eni - fni), hmi)
        lpr, lpi = 0.5 * (epr + enr), 0.5 * (epi - eni)
        lmr, lmi = 0.5 * (fpr + fnr), 0.5 * (fpi - fni)
        if r == 0:
            lpr, lpi = jnp.where(is_first, epr, lpr), jnp.where(is_first, enr, lpi)
            lmr, lmi = jnp.where(is_first, fpr, lmr), jnp.where(is_first, fnr, lmi)
        hpr, hpi = jnp.where(lane0, lpr, hpr), jnp.where(lane0, lpi, hpi)
        hmr, hmi = jnp.where(lane0, lmr, hmr), jnp.where(lane0, lmi, hmi)
        parts = (
            hpr * cos_p + hpi * sin_p,
            hpi * cos_p - hpr * sin_p,
            hmr * cos_m + hmi * sin_m,
            hmi * cos_m - hmr * sin_m,
        )
        for c in range(4):
            for q in range(4):
                table[tile, q, c, pl.ds(r, 1), :] = parts[c][q : q + 1]

    started = []

    def pass_on(which, t):
        copy = remote(
            table.at[which],
            table.at[which],
            ag_send.at[len(started)],
            ag_recv.at[which],
            t,
            depth,
        )
        copy.start()
        started.append(copy)

    def arrived(which):
        remote(
            table.at[which], table.at[which], ag_send.at[0], ag_recv.at[which], tile, depth
        ).wait_recv()

    above = at(yrow + 1, zlo, core)
    below = at(yrow + 3, zlo, core)
    sibling = at(yrow, zlo, 1 - core)
    z_order = (1, 3, 2)
    pass_on(tile, above)
    pass_on(tile, below)
    for dz in z_order:
        pass_on(tile, at(yrow, zlo + dz, core))
    pass_on(tile, sibling)

    for dz in z_order:
        which = at(yrow, zlo + dz, core)
        arrived(which)
        pass_on(which, above)
        pass_on(which, below)
        pass_on(which, sibling)

    for dz in (0, 1, 3, 2):
        which = at(yrow + 3, zlo + dz, core)
        arrived(which)
        if dz in (0, 1):
            pass_on(which, above)
        pass_on(which, sibling)
        which = at(yrow + 1, zlo + dz, core)
        arrived(which)
        if dz in (2, 3):
            pass_on(which, below)
        pass_on(which, sibling)
    def read_quads(ref, rows, rows2):
        return (
            ref[rows, pl.ds(0, HALF)],
            ref[rows, pl.ds(HALF, HALF)],
            ref[rows2, pl.ds(0, HALF)],
            ref[rows2, pl.ds(HALF, HALF)],
        )

    def rows_of(k):
        if isinstance(k, int):
            return pl.ds(8 * k, 8), pl.ds(HALF + 8 * k, 8)
        return pl.ds(pl.multiple_of(8 * k, 8), 8), pl.ds(pl.multiple_of(HALF + 8 * k, 8), 8)

    def table_of(p, k):
        which = k if p < 4 else 31 - k
        return tuple(table[which, p % 4, c] for c in range(4))

    def spectrum_block(t, g, j, first):
        k = 8 * g + j
        rows, rows2 = rows_of(k)
        total = None
        for p in range(LOCAL_PLANES):
            hpr, hpi, hmr, hmi = table_of(p, k)
            pr, pi, mr, mi = quads_in(*read_quads(packed.at[t, p], rows, rows2), first)
            terms = times(hpr, hpi, pr, pi, first, False) + times(hmr, hmi, mr, mi, first, False)
            total = terms if total is None else tuple(a + b for a, b in zip(total, terms))
        cc, cs, sc, ss = quads_out(*total, first)
        upper, lower = pl.ds(8 * (j % 2), 8), pl.ds(16 + 8 * (j % 2), 8)
        partial[t, g, j // 2, upper, pl.ds(0, HALF)] = cc
        partial[t, g, j // 2, upper, pl.ds(HALF, HALF)] = cs
        partial[t, g, j // 2, lower, pl.ds(0, HALF)] = sc
        partial[t, g, j // 2, lower, pl.ds(HALF, HALF)] = ss

    rs_copies = []

    def spectrum_group(t, g):
        for j in range(1, 8):
            spectrum_block(t, g, j, False)

        @pl.when(g == 0)
        def _():
            spectrum_block(t, 0, 0, True)

        @pl.when(g == 1)
        def _():
            spectrum_block(t, 1, 0, False)

        s = len(rs_copies) // 3
        for d in (1, 3, 2):
            copy = remote(
                partial.at[t, g, lax.rem(xpos + d, 4)],
                scattered.at[d - 1, s],
                rs_send.at[3 * s + d - 1],
                rs_recv.at[3 * s + d - 1],
                tile,
                xpeer(d),
            )
            copy.start()
            rs_copies.append(copy)

    near = jnp.where(jnp.logical_or(yrow == 0, yrow == 3), 0, 1)
    far = 1 - near
    for dy in (0, 1, 3):
        for dz in range(4):
            arrived(at(yrow + dy, zlo + dz, 1 - core))
    spectrum_group(0, near)
    for dz in (0, 1, 3, 2):
        which = at(yrow + 2, zlo + dz, core)
        arrived(which)
        pass_on(which, sibling)
    spectrum_group(1, near)
    for dz in range(4):
        arrived(at(yrow + 2, zlo + dz, 1 - core))
    spectrum_group(0, far)
    spectrum_group(1, far)
    pieces = ((0, near), (1, near), (0, far), (1, far))
    z_copies = []
    for s, (t, g) in enumerate(pieces):
        for copy in rs_copies[3 * s : 3 * s + 3]:
            copy.wait_recv()
        zsend[s] = partial[t, g, xpos] + scattered[0, s] + scattered[1, s] + scattered[2, s]
        copy = remote(zsend.at[s], zrecv.at[s], z_send.at[s], z_recv.at[s], tile, zpartner)
        copy.start()
        z_copies.append(copy)
    local[1].wait()
    local[2].wait()
    xg_copies = []
    for s, (t, g) in enumerate(pieces):
        z_copies[s].wait_recv()
        spectrum[t, g, xpos] = zsend[s] + zrecv[s]
        for d in (1, 3, 2):
            copy = remote(
                spectrum.at[t, g, xpos],
                spectrum.at[t, g, xpos],
                xg_send.at[3 * s + d - 1],
                xg_recv.at[3 * s + d - 1],
                tile,
                xpeer(d),
            )
            copy.start()
            xg_copies.append(copy)

    def strip(p, t, image_part, rows):
        values = vol[t, p, rows, :]
        return jnp.maximum(values * (1.0 + STEP_GAIN * image_part), 0.0)

    def to_before(p):
        return remote(
            top_send.at[p], after_recv.at[p], halo_send.at[p], halo_recv.at[p], before, depth
        )

    def to_after(p):
        slot = LOCAL_PLANES + p
        return remote(
            bottom_send.at[p], before_recv.at[p], halo_send.at[slot], halo_recv.at[slot], after, depth
        )

    for t in range(LOCAL_TILES):
        for copy in xg_copies[3 * t : 3 * t + 3] + xg_copies[3 * t + 6 : 3 * t + 9]:
            copy.wait_recv()
        for k in range(16):
            rows, rows2 = rows_of(k)
            found = spectrum.at[t, k // 8, (k % 8) // 2]
            sums[t, rows, :] = found[pl.ds(8 * (k % 2), 8), :]
            sums[t, rows2, :] = found[pl.ds(16 + 8 * (k % 2), 8), :]
        half = dot3(split(sums[t]), inv_right())
        here = pl.ds(t * SIDE, SIDE)
        projection = background[here, :] + dot3(inv_left(), split(half))
        ratio = measured[here, :] / jnp.maximum(projection, FLOOR_LEVEL)
        half = dot3(split(ratio - 1.0), right())
        sums[t] = dot3(left(), split(half))
        for k in range(16):
            rows, rows2 = rows_of(k)
            found = quads_in(*read_quads(sums.at[t], rows, rows2), k == 0)
            for c in range(4):
                ratio_quads[t, c, rows, :] = found[c]

        def backward(q, carry, t=t):
            for h in range(2):
                p = q + 4 * h
                for k in range(16):
                    rows, rows2 = rows_of(k)
                    which = 31 - k if h else k
                    hpr, hpi, hmr, hmi = (table[which, q, c] for c in range(4))
                    pr, pi, mr, mi = (ratio_quads[t, c, rows, :] for c in range(4))
                    plus = times(hpr, hpi, pr, pi, k == 0, True)
                    minus = times(hmr, hmi, mr, mi, k == 0, True)
                    cc, cs, sc, ss = quads_out(*plus, *minus, k == 0)
                    quads[h, rows, pl.ds(0, HALF)] = cc
                    quads[h, rows, pl.ds(HALF, HALF)] = cs
                    quads[h, rows2, pl.ds(0, HALF)] = sc
                    quads[h, rows2, pl.ds(HALF, HALF)] = ss
                half = split(dot3(split(quads[h]), inv_right()))
                part_high[t, p] = half[0]
                part_low[t, p] = half[1]
                rows = slice(0, WIDTH) if t == 0 else slice(SIDE - WIDTH, SIDE)
                edge = strip(p, t, dot3((mats[4, rows], mats[5, rows]), half), rows)
                if t == 0:
                    top_send[p] = edge
                else:
                    bottom_send[p] = edge
            for h in range(2):
                (to_after if t else to_before)(q + 4 * h).start()
            return carry

        lax.fori_loop(0, 4, backward, 0)

    base = tile * LOCAL_TILES
    w_inner = ramp(margins[base])
    w_after = ramp(margins[base + 1])
    w_before = ramp(margins[lax.rem(base + TILES - 1, TILES)])

    def finish_plane(p, carry):
        half = (part_high[0, p], part_low[0, p])
        rows = slice(WIDTH, SIDE)
        upper = strip(p, 0, dot3((mats[4, rows], mats[5, rows]), half), rows)
        half = (part_high[1, p], part_low[1, p])
        rows = slice(0, SIDE - WIDTH)
        lower = strip(p, 1, dot3((mats[4, rows], mats[5, rows]), half), rows)
        inner = SIDE - 2 * WIDTH
        shared = (1.0 - w_inner) * upper[inner:] + w_inner * lower[:WIDTH]
        out[0, p, WIDTH : SIDE - WIDTH, :] = upper[:inner]
        out[0, p, SIDE - WIDTH :, :] = shared
        out[1, p, :WIDTH, :] = shared
        out[1, p, WIDTH : SIDE - WIDTH, :] = lower[WIDTH:]
        return carry

    lax.fori_loop(0, LOCAL_PLANES, finish_plane, 0)

    def last_strip(p, carry):
        to_before(p).wait_recv()
        out[1, p, SIDE - WIDTH :, :] = (1.0 - w_after) * bottom_send[p] + w_after * after_recv[p]
        return carry

    lax.fori_loop(0, LOCAL_PLANES, last_strip, 0)

    def first_strip(p, carry):
        to_after(p).wait_recv()
        out[0, p, :WIDTH, :] = (1.0 - w_before) * before_recv[p] + w_before * top_send[p]
        return carry

    lax.fori_loop(0, LOCAL_PLANES, first_strip, 0)

    @pl.when(jnp.logical_not(negative))
    def _():
        up_all.wait_send()

    @pl.when(negative)
    def _():
        down_rest.wait_send()
        down_first.wait_send()
        down_last.wait_send()

    for copy in started + rs_copies + z_copies + xg_copies:
        copy.wait_send()

    def drain(p, carry):
        to_before(p).wait_send()
        to_after(p).wait_send()
        return carry

    lax.fori_loop(0, LOCAL_PLANES, drain, 0)


def on_device(volume, transfer, measured, background, margins, phases):
    mats = packed_tables()
    hbm = pl.BlockSpec(memory_space=pltpu.HBM)
    dma = pltpu.SemaphoreType.DMA
    tall = LOCAL_TILES * SIDE
    return pl.pallas_call(
        kernel,
        name="update",
        out_shape=jax.ShapeDtypeStruct(volume.shape, f32),
        in_specs=[hbm] * 8,
        out_specs=pl.BlockSpec(memory_space=pltpu.VMEM),
        scratch_shapes=[
            pltpu.SMEM((LOCAL_PLANES,), jnp.int32),
            pltpu.SMEM((TILES,), jnp.int32),
            pltpu.VMEM((LOCAL_PLANES, 2, 8, SIDE), f32),
            pltpu.VMEM((HALF, HALF), bf16),
            pltpu.VMEM((LOCAL_TILES, LOCAL_PLANES, SIDE, SIDE), f32),
            pltpu.VMEM((LOCAL_TILES, LOCAL_PLANES, SIDE, SIDE), f32),
            pltpu.VMEM((32, 4, 4, 8, HALF), f32),
            pltpu.VMEM((8, SIDE, SIDE), bf16),
            pltpu.VMEM((tall, SIDE), f32),
            pltpu.VMEM((tall, SIDE), f32),
            pltpu.VMEM((2, HALF, HALF), f32),
            pltpu.VMEM((2, 8, 16, HALF), f32),
            pltpu.VMEM((8, 16, HALF), f32),
            pltpu.VMEM((1, 16, HALF), f32),
            pltpu.VMEM((8, 16, HALF), f32),
            pltpu.VMEM((8, 16, HALF), f32),
            pltpu.VMEM((LOCAL_TILES, SIDE, SIDE), f32),
            pltpu.VMEM((LOCAL_TILES, 2, 4, WIDTH, SIDE), f32),
            pltpu.VMEM((3, PIECES, WIDTH, SIDE), f32),
            pltpu.VMEM((PIECES, WIDTH, SIDE), f32),
            pltpu.VMEM((PIECES, WIDTH, SIDE), f32),
            pltpu.VMEM((LOCAL_TILES, 2, 4, WIDTH, SIDE), f32),
            pltpu.VMEM((LOCAL_TILES, 4, HALF, HALF), f32),
            pltpu.VMEM((LOCAL_TILES, SIDE, SIDE), f32),
            pltpu.VMEM((LOCAL_TILES, LOCAL_PLANES, SIDE, SIDE), bf16),
            pltpu.VMEM((LOCAL_TILES, LOCAL_PLANES, SIDE, SIDE), bf16),
            pltpu.VMEM((LOCAL_PLANES, WIDTH, SIDE), f32),
            pltpu.VMEM((LOCAL_PLANES, WIDTH, SIDE), f32),
            pltpu.VMEM((LOCAL_PLANES, WIDTH, SIDE), f32),
            pltpu.VMEM((LOCAL_PLANES, WIDTH, SIDE), f32),
            dma((LOCAL_PLANES,)),
            dma((7,)),
            dma((3,)),
            dma((2,)),
            dma((31,)),
            dma((32,)),
            dma((3 * PIECES,)),
            dma((3 * PIECES,)),
            dma((PIECES,)),
            dma((PIECES,)),
            dma((3 * PIECES,)),
            dma((3 * PIECES,)),
            dma((2 * LOCAL_PLANES,)),
            dma((2 * LOCAL_PLANES,)),
        ],
        compiler_params=pltpu.CompilerParams(
            collective_id=0, has_side_effects=True, vmem_limit_bytes=48 * 1024 * 1024
        ),
    )(
        *(
            pltpu.with_memory_space_constraint(array, pltpu.HBM)
            for array in (
                phases,
                margins,
                transfer,
                volume,
                measured.reshape(tall, SIDE),
                background.reshape(tall, SIDE),
                mats,
                pairing(),
            )
        )
    )


def solution(mesh):
    return jax.shard_map(
        on_device,
        mesh=mesh,
        in_specs=(
            P("tile", "depth", None, None),
            P("depth", None, "tile", None),
            P("tile", None, None),
            P("tile", None, None),
            P(),
            P("depth"),
        ),
        out_specs=P("tile", "depth", None, None),
        check_vma=False,
    )
```

```python
import functools
import math

import jax
import jax.numpy as jnp
import numpy as np
from jax import lax
from jax.experimental import pallas as pl
from jax.experimental.pallas import tpu as pltpu
from jax.sharding import PartitionSpec as P

SIDE = 256
HALF = 128
WIDTH = 32
TILES = 64
LOCAL_TILES = 2
LOCAL_PLANES = 8
PIECES = 4
GATHER_SENDS = 62
FLOOR_LEVEL = 0.5
STEP_GAIN = 2.0
MESH = pl.DeviceIdType.MESH
f32 = jnp.float32
bf16 = jnp.bfloat16


def packed_tables():
    place = np.arange(SIDE)
    table = np.zeros((SIDE, SIDE))
    for a in range(HALF):
        table[a] = np.cos(2 * np.pi * (a * place % SIDE) / SIDE)
    table[HALF] = 1.0 - 2.0 * (place % 2)
    for a in range(1, HALF):
        table[HALF + a] = np.sin(2 * np.pi * (a * place % SIDE) / SIDE)
    weight = np.full(SIDE, 2.0)
    weight[0] = weight[HALF] = 1.0
    inverse = table.T * weight / SIDE
    pieces = []
    for matrix in (table, table.T, inverse, inverse.T):
        high = matrix.astype(bf16)
        pieces += [high, (matrix - high.astype(np.float64)).astype(bf16)]
    return jnp.asarray(np.stack(pieces))


def pairing():
    move = np.zeros((HALF, HALF), np.float32)
    move[0, 0] = 1.0
    for b in range(1, HALF):
        move[HALF - b, b] = 1.0
    return jnp.asarray(move.astype(bf16))


def split(values):
    high = values.astype(bf16)
    return high, (values - high.astype(f32)).astype(bf16)


def dot(a, b):
    return jnp.dot(a, b, preferred_element_type=f32)


def dot3(a, b):
    return dot(a[0], b[0]) + dot(a[1], b[0]) + dot(a[0], b[1])


def special(shape, first):
    lane0 = lax.broadcasted_iota(jnp.int32, shape, 1) == 0
    row0 = None
    if first:
        row0 = jnp.logical_and(
            lax.broadcasted_iota(jnp.int32, shape, 0) == 0, jnp.logical_not(lane0)
        )
    return lane0, row0


def quads_in(cc, cs, sc, ss, first):
    lane0, row0 = special(cc.shape, first)
    pr, pi, mr, mi = cc - ss, cs + sc, cc + ss, cs - sc
    if first:
        pr = jnp.where(row0, cc, pr)
        pi = jnp.where(row0, cs, pi)
        mr = jnp.where(row0, sc, mr)
        mi = jnp.where(row0, ss, mi)
    return (
        jnp.where(lane0, cc, pr),
        jnp.where(lane0, sc, pi),
        jnp.where(lane0, cs, mr),
        jnp.where(lane0, ss, mi),
    )


def quads_out(pr, pi, mr, mi, first):
    lane0, row0 = special(pr.shape, first)
    cc, ss, cs, sc = pr + mr, mr - pr, pi + mi, pi - mi
    if first:
        cc = jnp.where(row0, pr, cc)
        cs = jnp.where(row0, pi, cs)
        sc = jnp.where(row0, mr, sc)
        ss = jnp.where(row0, mi, ss)
    return (
        jnp.where(lane0, pr, cc),
        jnp.where(lane0, mr, cs),
        jnp.where(lane0, pi, sc),
        jnp.where(lane0, mi, ss),
    )


def times(hr, hi, real, imag, first, conj):
    second = hr
    if first:
        lane0, _ = special(hr.shape, False)
        corner = jnp.logical_and(lane0, lax.broadcasted_iota(jnp.int32, hr.shape, 0) == 0)
        second = jnp.where(corner, hi, hr)
        hi = jnp.where(corner, 0.0, hi)
    if conj:
        return hr * real - hi * imag, second * imag + hi * real
    return hr * real + hi * imag, second * imag - hi * real


def ramp(margin):
    margin = margin.astype(f32)
    row = lax.broadcasted_iota(jnp.int32, (WIDTH, SIDE), 0).astype(f32)
    return jnp.clip((row + 0.5 - (WIDTH - margin) / 2.0) / margin, 0.0, 1.0)


def kernel(
    phases_hbm,
    margins_hbm,
    transfer_hbm,
    volume_hbm,
    measured_hbm,
    background_hbm,
    mats_hbm,
    pair_hbm,
    out,
    phases,
    margins,
    transfer,
    pair_ref,
    vol,
    packed,
    table,
    mats,
    measured,
    background,
    halves,
    mine,
    other,
    other0,
    pos,
    neg,
    sums,
    partial,
    scattered,
    zsend,
    zrecv,
    spectrum,
    ratio_quads,
    quads,
    part_high,
    part_low,
    top_send,
    bottom_send,
    after_recv,
    before_recv,
    vol_sem,
    in_sem,
    ex_send,
    ex_recv,
    ag_send,
    ag_recv,
    rs_send,
    rs_recv,
    z_send,
    z_recv,
    xg_send,
    xg_recv,
    halo_send,
    halo_recv,
):
    tile = lax.axis_index("tile")
    depth = lax.axis_index("depth")
    core = lax.rem(tile, 2)
    zlo = lax.rem(tile // 2, 4)
    yrow = tile // 8
    xpos = lax.rem(depth, 4)
    zhi = depth // 4
    negative = tile >= 16
    block = jnp.where(negative, 31 - tile, tile)

    def at(y, z, c):
        return lax.rem(y, 4) * 8 + lax.rem(z, 4) * 2 + c

    def xpeer(d):
        return zhi * 4 + lax.rem(xpos + d, 4)

    after = lax.rem(tile + 1, 32)
    before = lax.rem(tile + 31, 32)
    zpartner = (1 - zhi) * 4 + xpos

    volume_copies = []
    for p in range(LOCAL_PLANES):
        volume_copies.append(
            pltpu.make_async_copy(volume_hbm.at[:, p], vol.at[:, p], vol_sem.at[p])
        )
    local = [
        pltpu.make_async_copy(mats_hbm, mats, in_sem.at[0]),
        pltpu.make_async_copy(measured_hbm, measured, in_sem.at[1]),
        pltpu.make_async_copy(background_hbm, background, in_sem.at[2]),
        pltpu.make_async_copy(transfer_hbm, transfer, in_sem.at[3]),
        pltpu.make_async_copy(pair_hbm, pair_ref, in_sem.at[4]),
        pltpu.make_async_copy(phases_hbm, phases, in_sem.at[5]),
        pltpu.make_async_copy(margins_hbm, margins, in_sem.at[6]),
    ]
    for which in (3, 4, 0, 5, 6):
        local[which].start()
    for copy in volume_copies:
        copy.start()
    local[1].start()
    local[2].start()

    barrier = pltpu.get_barrier_semaphore()

    def greet(t, d):
        pl.semaphore_signal(barrier, inc=1, device_id=(t, d), device_id_type=MESH)

    greet(31 - tile, depth)
    for dz in range(1, 4):
        greet(at(yrow, zlo + dz, core), depth)
    greet(at(yrow + 1, zlo, core), depth)
    greet(at(yrow + 3, zlo, core), depth)
    greet(at(yrow + 2, zlo, core), depth)
    greet(at(yrow, zlo, 1 - core), depth)
    for d in range(1, 4):
        greet(tile, xpeer(d))
    greet(tile, zpartner)
    greet(after, depth)
    greet(before, depth)
    first_of = lax.rem(32 - tile, 16)
    last_to = jnp.where(tile == 16, 31, tile - 1)
    last_from = jnp.where(tile == 31, 16, tile + 1)
    row0_from = jnp.where(tile == 0, 16, 32 - tile)

    @pl.when(negative)
    def _():
        greet(first_of, depth)
        greet(last_to, depth)
        greet(last_from, depth)

    @pl.when(jnp.logical_not(negative))
    def _():
        greet(row0_from, depth)

    local[3].wait()
    local[4].wait()
    whole = transfer[...].reshape(LOCAL_PLANES * 2 * 8, SIDE)
    halves[0] = whole[:, :HALF]
    rest = whole[:, HALF:]
    high, low = split(rest)
    lowest = ((rest - high.astype(f32)) - low.astype(f32)).astype(bf16)
    move = pair_ref[...]
    halves[1] = dot(high, move) + dot(low, move) + dot(lowest, move)
    for r in range(8):
        to = jnp.where(negative, (8 - r) % 8, r)
        for n in range(4):
            for e in range(2):
                for c in range(2):
                    piece = halves[e, pl.ds(n * 32 + c * 8 + r, 2, stride=16), :]
                    mine[n // 2, n % 2, to, pl.ds((e * 2 + c) * 2, 2), :] = piece

    pl.semaphore_wait(barrier, 15 + 2 * (tile // 16))

    def remote(src, dst, send, recv, t, d):
        return pltpu.make_async_remote_copy(
            src_ref=src,
            dst_ref=dst,
            send_sem=send,
            recv_sem=recv,
            device_id=(t, d),
            device_id_type=MESH,
        )

    rows7 = pl.ds(1, 7)
    row1 = pl.ds(0, 1)

    def exchange(n):
        send = lambda k: ex_send.at[3 * n + k]
        recv = lambda k: ex_recv.at[2 * n + k]
        return (
            remote(mine.at[1, n], other.at[n], send(0), recv(0), 31 - tile, depth),
            remote(
                mine.at[0, n, rows7], other.at[n, rows7], send(0), recv(0), 31 - tile, depth
            ),
            remote(mine.at[0, n, row1], other.at[n, row1], send(1), recv(1), first_of, depth),
            remote(mine.at[1, n, row1], other0.at[n], send(2), recv(1), last_to, depth),
        )

    exchanges = (exchange(0), exchange(1))

    @pl.when(jnp.logical_not(negative))
    def _():
        for n in range(2):
            exchanges[n][0].start()

    @pl.when(negative)
    def _():
        for n in range(2):
            for copy in exchanges[n][1:]:
                copy.start()

    left = lambda: (mats[0], mats[1])
    right = lambda: (mats[2], mats[3])
    inv_left = lambda: (mats[4], mats[5])
    inv_right = lambda: (mats[6], mats[7])
    local[0].wait()

    def forward(p, carry):
        pltpu.make_async_copy(volume_hbm.at[:, p], vol.at[:, p], vol_sem.at[p]).wait()
        for t in range(LOCAL_TILES):
            half = dot3(split(vol[t, p]), right())
            packed[t, p] = dot3(left(), split(half))
        return carry

    lax.fori_loop(0, LOCAL_PLANES, forward, 0)

    started = []

    def pass_on(which, n, t):
        copy = remote(
            table.at[which, pl.ds(2 * n, 2)],
            table.at[which, pl.ds(2 * n, 2)],
            ag_send.at[len(started)],
            ag_recv.at[2 * which + n],
            t,
            depth,
        )
        copy.start()
        started.append(copy)

    def arrived(which, n):
        remote(
            table.at[which, pl.ds(2 * n, 2)],
            table.at[which, pl.ds(2 * n, 2)],
            ag_send.at[0],
            ag_recv.at[2 * which + n],
            tile,
            depth,
        ).wait_recv()

    above = at(yrow + 1, zlo, core)
    below = at(yrow + 3, zlo, core)
    across = at(yrow + 2, zlo, core)
    sibling = at(yrow, zlo, 1 - core)
    z_order = (1, 3, 2)

    local[5].wait()
    local[6].wait()
    plane0 = jnp.where(negative, 4, 0)
    column = lax.broadcasted_iota(jnp.int32, (2, HALF), 1)
    row2 = lax.broadcasted_iota(jnp.int32, (2, HALF), 0)
    lane0 = column == 0
    is_first = block == 0
    for n in range(2):

        @pl.when(jnp.logical_not(negative))
        def _(n=n):
            exchanges[n][1].wait_recv()
            exchanges[n][2].wait_recv()
            pos[n] = mine[0, n]
            neg[n] = other[n]

        @pl.when(negative)
        def _(n=n):
            exchanges[n][0].wait_recv()
            exchanges[n][3].wait_recv()
            pos[n] = other[n]
            neg[n, 0] = other0[n, 0]
            neg[n, 1:8] = mine[1, n, 1:8]

        phase = jnp.where(row2 == 0, phases[plane0 + 2 * n], phases[plane0 + 2 * n + 1])

        def rotor(columns):
            angle = ((phase * columns) & (SIDE - 1)).astype(f32) * (2.0 * math.pi / SIDE)
            return jnp.cos(angle), jnp.sin(angle)

        cos_p, sin_p = rotor(column)
        cos_m, sin_m = rotor(jnp.where(lane0, HALF, column))
        sin_m = jnp.where(lane0, 0.0, sin_m)
        for r in range(8):
            epr, epi, fpr, fpi = (pos[n, r, pl.ds(c * 2, 2), :] for c in range(4))
            enr, eni, fnr, fni = (neg[n, r, pl.ds(c * 2, 2), :] for c in range(4))
            hpr, hpi = 0.25 * (epr + fnr), 0.25 * (epi - fni)
            hmr, hmi = 0.25 * (enr + fpr), 0.25 * (eni - fpi)
            if r == 0:
                at0 = jnp.logical_and(is_first, jnp.logical_not(lane0))
                hpr = jnp.where(at0, 0.5 * (epr + fpr), hpr)
                hpi = jnp.where(at0, 0.5 * (epi - fpi), hpi)
                hmr = jnp.where(at0, 0.5 * (enr + fnr), hmr)
                hmi = jnp.where(at0, 0.5 * (eni - fni), hmi)
            lpr, lpi = 0.5 * (epr + enr), 0.5 * (epi - eni)
            lmr, lmi = 0.5 * (fpr + fnr), 0.5 * (fpi - fni)
            if r == 0:
                lpr, lpi = jnp.where(is_first, epr, lpr), jnp.where(is_first, enr, lpi)
                lmr, lmi = jnp.where(is_first, fpr, lmr), jnp.where(is_first, fnr, lmi)
            hpr, hpi = jnp.where(lane0, lpr, hpr), jnp.where(lane0, lpi, hpi)
            hmr, hmi = jnp.where(lane0, lmr, hmr), jnp.where(lane0, lmi, hmi)
            parts = (
                hpr * cos_p + hpi * sin_p,
                hpi * cos_p - hpr * sin_p,
                hmr * cos_m + hmi * sin_m,
                hmi * cos_m - hmr * sin_m,
            )
            for c in range(4):
                for q in range(2):
                    table[tile, 2 * n + q, c, pl.ds(r, 1), :] = parts[c][q : q + 1]
        for dz in z_order:
            pass_on(tile, n, at(yrow, zlo + dz, core))
        pass_on(tile, n, above)
        pass_on(tile, n, below)
        pass_on(tile, n, sibling)

    def relay(dz, n):
        which = at(yrow + 3, zlo + dz, core)
        arrived(which, n)
        if dz in (0, 1):
            pass_on(which, n, above)
        pass_on(which, n, sibling)
        which = at(yrow + 1, zlo + dz, core)
        arrived(which, n)
        if dz == 3:
            pass_on(which, n, below)
        pass_on(which, n, sibling)

    for n in range(2):
        for dz in z_order:
            which = at(yrow, zlo + dz, core)
            arrived(which, n)
            if dz == 2:
                pass_on(which, n, across)
            pass_on(which, n, above)
            pass_on(which, n, below)
            pass_on(which, n, sibling)
        relay(0, n)
    for n in range(2):
        for dz in z_order:
            relay(dz, n)

    def read_quads(ref, rows, rows2):
        return (
            ref[rows, pl.ds(0, HALF)],
            ref[rows, pl.ds(HALF, HALF)],
            ref[rows2, pl.ds(0, HALF)],
            ref[rows2, pl.ds(HALF, HALF)],
        )

    def rows_of(k):
        if isinstance(k, int):
            return pl.ds(8 * k, 8), pl.ds(HALF + 8 * k, 8)
        return pl.ds(pl.multiple_of(8 * k, 8), 8), pl.ds(pl.multiple_of(HALF + 8 * k, 8), 8)

    def table_of(p, k):
        which = k if p < 4 else 31 - k
        return tuple(table[which, p % 4, c] for c in range(4))

    def spectrum_block(t, g, j, first):
        k = 8 * g + j
        rows, rows2 = rows_of(k)
        total = None
        for p in range(LOCAL_PLANES):
            hpr, hpi, hmr, hmi = table_of(p, k)
            pr, pi, mr, mi = quads_in(*read_quads(packed.at[t, p], rows, rows2), first)
            terms = times(hpr, hpi, pr, pi, first, False) + times(hmr, hmi, mr, mi, first, False)
            total = terms if total is None else tuple(a + b for a, b in zip(total, terms))
        cc, cs, sc, ss = quads_out(*total, first)
        upper, lower = pl.ds(8 * (j % 2), 8), pl.ds(16 + 8 * (j % 2), 8)
        partial[t, g, j // 2, upper, pl.ds(0, HALF)] = cc
        partial[t, g, j // 2, upper, pl.ds(HALF, HALF)] = cs
        partial[t, g, j // 2, lower, pl.ds(0, HALF)] = sc
        partial[t, g, j // 2, lower, pl.ds(HALF, HALF)] = ss

    rs_copies = []

    def spectrum_group(t, g):
        for j in range(1, 8):
            spectrum_block(t, g, j, False)

        @pl.when(g == 0)
        def _():
            spectrum_block(t, 0, 0, True)

        @pl.when(g == 1)
        def _():
            spectrum_block(t, 1, 0, False)

        s = len(rs_copies) // 3
        for d in (1, 3, 2):
            copy = remote(
                partial.at[t, g, lax.rem(xpos + d, 4)],
                scattered.at[d - 1, s],
                rs_send.at[3 * s + d - 1],
                rs_recv.at[3 * s + d - 1],
                tile,
                xpeer(d),
            )
            copy.start()
            rs_copies.append(copy)

    near = jnp.where(jnp.logical_or(yrow == 0, yrow == 3), 0, 1)
    far = 1 - near
    for dy in (0, 1, 3):
        for dz in range(4):
            for n in range(2):
                arrived(at(yrow + dy, zlo + dz, 1 - core), n)
    spectrum_group(0, near)
    for n in range(2):
        for dz in (0, 1, 3, 2):
            which = at(yrow + 2, zlo + dz, core)
            arrived(which, n)
            pass_on(which, n, sibling)
    spectrum_group(1, near)
    for dz in range(4):
        for n in range(2):
            arrived(at(yrow + 2, zlo + dz, 1 - core), n)
    spectrum_group(0, far)
    spectrum_group(1, far)
    pieces = ((0, near), (1, near), (0, far), (1, far))
    z_copies = []
    for s, (t, g) in enumerate(pieces):
        for copy in rs_copies[3 * s : 3 * s + 3]:
            copy.wait_recv()
        zsend[s] = partial[t, g, xpos] + scattered[0, s] + scattered[1, s] + scattered[2, s]
        copy = remote(zsend.at[s], zrecv.at[s], z_send.at[s], z_recv.at[s], tile, zpartner)
        copy.start()
        z_copies.append(copy)
    local[1].wait()
    local[2].wait()
    xg_copies = []
    for s, (t, g) in enumerate(pieces):
        z_copies[s].wait_recv()
        spectrum[t, g, xpos] = zsend[s] + zrecv[s]
        for d in (1, 3, 2):
            copy = remote(
                spectrum.at[t, g, xpos],
                spectrum.at[t, g, xpos],
                xg_send.at[3 * s + d - 1],
                xg_recv.at[3 * s + d - 1],
                tile,
                xpeer(d),
            )
            copy.start()
            xg_copies.append(copy)

    def strip(p, t, image_part, rows):
        values = vol[t, p, rows, :]
        return jnp.maximum(values * (1.0 + STEP_GAIN * image_part), 0.0)

    def to_before(p):
        return remote(
            top_send.at[p], after_recv.at[p], halo_send.at[p], halo_recv.at[p], before, depth
        )

    def to_after(p):
        slot = LOCAL_PLANES + p
        return remote(
            bottom_send.at[p], before_recv.at[p], halo_send.at[slot], halo_recv.at[slot], after, depth
        )

    for t in range(LOCAL_TILES):
        for copy in xg_copies[3 * t : 3 * t + 3] + xg_copies[3 * t + 6 : 3 * t + 9]:
            copy.wait_recv()
        for k in range(16):
            rows, rows2 = rows_of(k)
            found = spectrum.at[t, k // 8, (k % 8) // 2]
            sums[t, rows, :] = found[pl.ds(8 * (k % 2), 8), :]
            sums[t, rows2, :] = found[pl.ds(16 + 8 * (k % 2), 8), :]
        half = dot3(split(sums[t]), inv_right())
        here = pl.ds(t * SIDE, SIDE)
        projection = background[here, :] + dot3(inv_left(), split(half))
        ratio = measured[here, :] / jnp.maximum(projection, FLOOR_LEVEL)
        half = dot3(split(ratio - 1.0), right())
        sums[t] = dot3(left(), split(half))
        for k in range(16):
            rows, rows2 = rows_of(k)
            found = quads_in(*read_quads(sums.at[t], rows, rows2), k == 0)
            for c in range(4):
                ratio_quads[t, c, rows, :] = found[c]

        def backward(q, carry, t=t):
            for h in range(2):
                p = q + 4 * h
                for k in range(16):
                    rows, rows2 = rows_of(k)
                    which = 31 - k if h else k
                    hpr, hpi, hmr, hmi = (table[which, q, c] for c in range(4))
                    pr, pi, mr, mi = (ratio_quads[t, c, rows, :] for c in range(4))
                    plus = times(hpr, hpi, pr, pi, k == 0, True)
                    minus = times(hmr, hmi, mr, mi, k == 0, True)
                    cc, cs, sc, ss = quads_out(*plus, *minus, k == 0)
                    quads[h, rows, pl.ds(0, HALF)] = cc
                    quads[h, rows, pl.ds(HALF, HALF)] = cs
                    quads[h, rows2, pl.ds(0, HALF)] = sc
                    quads[h, rows2, pl.ds(HALF, HALF)] = ss
                half = split(dot3(split(quads[h]), inv_right()))
                part_high[t, p] = half[0]
                part_low[t, p] = half[1]
                rows = slice(0, WIDTH) if t == 0 else slice(SIDE - WIDTH, SIDE)
                edge = strip(p, t, dot3((mats[4, rows], mats[5, rows]), half), rows)
                if t == 0:
                    top_send[p] = edge
                else:
                    bottom_send[p] = edge
            for h in range(2):
                (to_after if t else to_before)(q + 4 * h).start()
            return carry

        lax.fori_loop(0, 4, backward, 0)

    base = tile * LOCAL_TILES
    w_inner = ramp(margins[base])
    w_after = ramp(margins[base + 1])
    w_before = ramp(margins[lax.rem(base + TILES - 1, TILES)])

    def finish_plane(p, carry):
        half = (part_high[0, p], part_low[0, p])
        rows = slice(WIDTH, SIDE)
        upper = strip(p, 0, dot3((mats[4, rows], mats[5, rows]), half), rows)
        half = (part_high[1, p], part_low[1, p])
        rows = slice(0, SIDE - WIDTH)
        lower = strip(p, 1, dot3((mats[4, rows], mats[5, rows]), half), rows)
        inner = SIDE - 2 * WIDTH
        shared = (1.0 - w_inner) * upper[inner:] + w_inner * lower[:WIDTH]
        out[0, p, WIDTH : SIDE - WIDTH, :] = upper[:inner]
        out[0, p, SIDE - WIDTH :, :] = shared
        out[1, p, :WIDTH, :] = shared
        out[1, p, WIDTH : SIDE - WIDTH, :] = lower[WIDTH:]
        return carry

    lax.fori_loop(0, LOCAL_PLANES, finish_plane, 0)

    def last_strip(p, carry):
        to_before(p).wait_recv()
        out[1, p, SIDE - WIDTH :, :] = (1.0 - w_after) * bottom_send[p] + w_after * after_recv[p]
        return carry

    lax.fori_loop(0, LOCAL_PLANES, last_strip, 0)

    def first_strip(p, carry):
        to_after(p).wait_recv()
        out[0, p, :WIDTH, :] = (1.0 - w_before) * before_recv[p] + w_before * top_send[p]
        return carry

    lax.fori_loop(0, LOCAL_PLANES, first_strip, 0)

    @pl.when(jnp.logical_not(negative))
    def _():
        for n in range(2):
            exchanges[n][0].wait_send()

    @pl.when(negative)
    def _():
        for n in range(2):
            for copy in exchanges[n][1:]:
                copy.wait_send()

    for copy in started + rs_copies + z_copies + xg_copies:
        copy.wait_send()

    def drain(p, carry):
        to_before(p).wait_send()
        to_after(p).wait_send()
        return carry

    lax.fori_loop(0, LOCAL_PLANES, drain, 0)


def on_device(volume, transfer, measured, background, margins, phases):
    mats = packed_tables()
    hbm = pl.BlockSpec(memory_space=pltpu.HBM)
    dma = pltpu.SemaphoreType.DMA
    tall = LOCAL_TILES * SIDE
    return pl.pallas_call(
        kernel,
        name="update",
        out_shape=jax.ShapeDtypeStruct(volume.shape, f32),
        in_specs=[hbm] * 8,
        out_specs=pl.BlockSpec(memory_space=pltpu.VMEM),
        scratch_shapes=[
            pltpu.SMEM((LOCAL_PLANES,), jnp.int32),
            pltpu.SMEM((TILES,), jnp.int32),
            pltpu.VMEM((LOCAL_PLANES, 2, 8, SIDE), f32),
            pltpu.VMEM((HALF, HALF), bf16),
            pltpu.VMEM((LOCAL_TILES, LOCAL_PLANES, SIDE, SIDE), f32),
            pltpu.VMEM((LOCAL_TILES, LOCAL_PLANES, SIDE, SIDE), f32),
            pltpu.VMEM((32, 4, 4, 8, HALF), f32),
            pltpu.VMEM((8, SIDE, SIDE), bf16),
            pltpu.VMEM((tall, SIDE), f32),
            pltpu.VMEM((tall, SIDE), f32),
            pltpu.VMEM((2, HALF, HALF), f32),
            pltpu.VMEM((2, 2, 8, 8, HALF), f32),
            pltpu.VMEM((2, 8, 8, HALF), f32),
            pltpu.VMEM((2, 1, 8, HALF), f32),
            pltpu.VMEM((2, 8, 8, HALF), f32),
            pltpu.VMEM((2, 8, 8, HALF), f32),
            pltpu.VMEM((LOCAL_TILES, SIDE, SIDE), f32),
            pltpu.VMEM((LOCAL_TILES, 2, 4, WIDTH, SIDE), f32),
            pltpu.VMEM((3, PIECES, WIDTH, SIDE), f32),
            pltpu.VMEM((PIECES, WIDTH, SIDE), f32),
            pltpu.VMEM((PIECES, WIDTH, SIDE), f32),
            pltpu.VMEM((LOCAL_TILES, 2, 4, WIDTH, SIDE), f32),
            pltpu.VMEM((LOCAL_TILES, 4, HALF, HALF), f32),
            pltpu.VMEM((LOCAL_TILES, SIDE, SIDE), f32),
            pltpu.VMEM((LOCAL_TILES, LOCAL_PLANES, SIDE, SIDE), bf16),
            pltpu.VMEM((LOCAL_TILES, LOCAL_PLANES, SIDE, SIDE), bf16),
            pltpu.VMEM((LOCAL_PLANES, WIDTH, SIDE), f32),
            pltpu.VMEM((LOCAL_PLANES, WIDTH, SIDE), f32),
            pltpu.VMEM((LOCAL_PLANES, WIDTH, SIDE), f32),
            pltpu.VMEM((LOCAL_PLANES, WIDTH, SIDE), f32),
            dma((LOCAL_PLANES,)),
            dma((7,)),
            dma((6,)),
            dma((4,)),
            dma((GATHER_SENDS,)),
            dma((64,)),
            dma((3 * PIECES,)),
            dma((3 * PIECES,)),
            dma((PIECES,)),
            dma((PIECES,)),
            dma((3 * PIECES,)),
            dma((3 * PIECES,)),
            dma((2 * LOCAL_PLANES,)),
            dma((2 * LOCAL_PLANES,)),
        ],
        compiler_params=pltpu.CompilerParams(
            collective_id=0, has_side_effects=True, vmem_limit_bytes=48 * 1024 * 1024
        ),
    )(
        *(
            pltpu.with_memory_space_constraint(array, pltpu.HBM)
            for array in (
                phases,
                margins,
                transfer,
                volume,
                measured.reshape(tall, SIDE),
                background.reshape(tall, SIDE),
                mats,
                pairing(),
            )
        )
    )


def solution(mesh):
    return jax.shard_map(
        on_device,
        mesh=mesh,
        in_specs=(
            P("tile", "depth", None, None),
            P("depth", None, "tile", None),
            P("tile", None, None),
            P("tile", None, None),
            P(),
            P("depth"),
        ),
        out_specs=P("tile", "depth", None, None),
        check_vma=False,
    )
```

```python
import functools
import math

import jax
import jax.numpy as jnp
import numpy as np
from jax import lax
from jax.experimental import pallas as pl
from jax.experimental.pallas import tpu as pltpu
from jax.sharding import PartitionSpec as P

SIDE = 256
HALF = 128
WIDTH = 32
TILES = 64
LOCAL_TILES = 2
LOCAL_PLANES = 8
PIECES = 4
EARLY_PLANES = 3
FLOOR_LEVEL = 0.5
STEP_GAIN = 2.0
MESH = pl.DeviceIdType.MESH
f32 = jnp.float32
bf16 = jnp.bfloat16


def packed_tables():
    place = np.arange(SIDE)
    table = np.zeros((SIDE, SIDE))
    for a in range(HALF):
        table[a] = np.cos(2 * np.pi * (a * place % SIDE) / SIDE)
    table[HALF] = 1.0 - 2.0 * (place % 2)
    for a in range(1, HALF):
        table[HALF + a] = np.sin(2 * np.pi * (a * place % SIDE) / SIDE)
    weight = np.full(SIDE, 2.0)
    weight[0] = weight[HALF] = 1.0
    inverse = table.T * weight / SIDE
    pieces = []
    for matrix in (table, table.T, inverse, inverse.T):
        high = matrix.astype(bf16)
        pieces += [high, (matrix - high.astype(np.float64)).astype(bf16)]
    return jnp.asarray(np.stack(pieces))


def pairing():
    move = np.zeros((HALF, HALF), np.float32)
    move[0, 0] = 1.0
    for b in range(1, HALF):
        move[HALF - b, b] = 1.0
    return jnp.asarray(move.astype(bf16))


def split(values):
    high = values.astype(bf16)
    return high, (values - high.astype(f32)).astype(bf16)


def dot(a, b):
    return jnp.dot(a, b, preferred_element_type=f32)


def dot3(a, b):
    return dot(a[0], b[0]) + dot(a[1], b[0]) + dot(a[0], b[1])


def special(shape, first):
    lane0 = lax.broadcasted_iota(jnp.int32, shape, 1) == 0
    row0 = None
    if first:
        row0 = jnp.logical_and(
            lax.broadcasted_iota(jnp.int32, shape, 0) == 0, jnp.logical_not(lane0)
        )
    return lane0, row0


def quads_in(cc, cs, sc, ss, first):
    lane0, row0 = special(cc.shape, first)
    pr, pi, mr, mi = cc - ss, cs + sc, cc + ss, cs - sc
    if first:
        pr = jnp.where(row0, cc, pr)
        pi = jnp.where(row0, cs, pi)
        mr = jnp.where(row0, sc, mr)
        mi = jnp.where(row0, ss, mi)
    return (
        jnp.where(lane0, cc, pr),
        jnp.where(lane0, sc, pi),
        jnp.where(lane0, cs, mr),
        jnp.where(lane0, ss, mi),
    )


def quads_out(pr, pi, mr, mi, first):
    lane0, row0 = special(pr.shape, first)
    cc, ss, cs, sc = pr + mr, mr - pr, pi + mi, pi - mi
    if first:
        cc = jnp.where(row0, pr, cc)
        cs = jnp.where(row0, pi, cs)
        sc = jnp.where(row0, mr, sc)
        ss = jnp.where(row0, mi, ss)
    return (
        jnp.where(lane0, pr, cc),
        jnp.where(lane0, mr, cs),
        jnp.where(lane0, pi, sc),
        jnp.where(lane0, mi, ss),
    )


def times(hr, hi, real, imag, first, conj):
    second = hr
    if first:
        lane0, _ = special(hr.shape, False)
        corner = jnp.logical_and(lane0, lax.broadcasted_iota(jnp.int32, hr.shape, 0) == 0)
        second = jnp.where(corner, hi, hr)
        hi = jnp.where(corner, 0.0, hi)
    if conj:
        return hr * real - hi * imag, second * imag + hi * real
    return hr * real + hi * imag, second * imag - hi * real


def ramp(margin):
    margin = margin.astype(f32)
    row = lax.broadcasted_iota(jnp.int32, (WIDTH, SIDE), 0).astype(f32)
    return jnp.clip((row + 0.5 - (WIDTH - margin) / 2.0) / margin, 0.0, 1.0)


def kernel(
    phases_hbm,
    margins_hbm,
    transfer_hbm,
    volume_hbm,
    measured_hbm,
    background_hbm,
    mats_hbm,
    pair_hbm,
    out,
    phases,
    margins,
    transfer,
    pair_ref,
    vol,
    packed,
    table,
    mats,
    measured,
    background,
    halves,
    mine,
    other,
    other0,
    pos,
    neg,
    sums,
    partial,
    scattered,
    zsend,
    zrecv,
    spectrum,
    ratio_quads,
    quads,
    part_high,
    part_low,
    top_send,
    bottom_send,
    after_recv,
    before_recv,
    vol_sem,
    in_sem,
    ex_send,
    ex_recv,
    ag_send,
    ag_recv,
    rs_send,
    rs_recv,
    z_send,
    z_recv,
    xg_send,
    xg_recv,
    halo_send,
    halo_recv,
):
    tile = lax.axis_index("tile")
    depth = lax.axis_index("depth")
    core = lax.rem(tile, 2)
    zlo = lax.rem(tile // 2, 4)
    yrow = tile // 8
    xpos = lax.rem(depth, 4)
    zhi = depth // 4
    negative = tile >= 16
    block = jnp.where(negative, 31 - tile, tile)

    def at(y, z, c):
        return lax.rem(y, 4) * 8 + lax.rem(z, 4) * 2 + c

    def xpeer(d):
        return zhi * 4 + lax.rem(xpos + d, 4)

    after = lax.rem(tile + 1, 32)
    before = lax.rem(tile + 31, 32)
    zpartner = (1 - zhi) * 4 + xpos

    volume_copies = []
    for p in range(LOCAL_PLANES):
        volume_copies.append(
            pltpu.make_async_copy(volume_hbm.at[:, p], vol.at[:, p], vol_sem.at[p])
        )
    local = [
        pltpu.make_async_copy(mats_hbm, mats, in_sem.at[0]),
        pltpu.make_async_copy(measured_hbm, measured, in_sem.at[1]),
        pltpu.make_async_copy(background_hbm, background, in_sem.at[2]),
        pltpu.make_async_copy(transfer_hbm, transfer, in_sem.at[3]),
        pltpu.make_async_copy(pair_hbm, pair_ref, in_sem.at[4]),
        pltpu.make_async_copy(phases_hbm, phases, in_sem.at[5]),
        pltpu.make_async_copy(margins_hbm, margins, in_sem.at[6]),
    ]
    for which in (3, 4, 0, 5, 6):
        local[which].start()
    for copy in volume_copies:
        copy.start()
    local[1].start()
    local[2].start()

    barrier = pltpu.get_barrier_semaphore()

    def greet(t, d):
        pl.semaphore_signal(barrier, inc=1, device_id=(t, d), device_id_type=MESH)

    greet(31 - tile, depth)
    for dz in range(1, 4):
        greet(at(yrow, zlo + dz, core), depth)
    greet(at(yrow + 1, zlo, core), depth)
    greet(at(yrow + 3, zlo, core), depth)
    greet(at(yrow, zlo, 1 - core), depth)
    for d in range(1, 4):
        greet(tile, xpeer(d))
    greet(tile, zpartner)
    greet(after, depth)
    greet(before, depth)
    first_of = lax.rem(32 - tile, 16)
    last_to = jnp.where(tile == 16, 31, tile - 1)
    last_from = jnp.where(tile == 31, 16, tile + 1)
    row0_from = jnp.where(tile == 0, 16, 32 - tile)

    @pl.when(negative)
    def _():
        greet(first_of, depth)
        greet(last_to, depth)
        greet(last_from, depth)

    @pl.when(jnp.logical_not(negative))
    def _():
        greet(row0_from, depth)

    local[3].wait()
    local[4].wait()
    whole = transfer[...].reshape(LOCAL_PLANES * 2 * 8, SIDE)
    halves[0] = whole[:, :HALF]
    rest = whole[:, HALF:]
    high, low = split(rest)
    lowest = ((rest - high.astype(f32)) - low.astype(f32)).astype(bf16)
    move = pair_ref[...]
    halves[1] = dot(high, move) + dot(low, move) + dot(lowest, move)
    for r in range(8):
        to = jnp.where(negative, (8 - r) % 8, r)
        for ph in range(2):
            for e in range(2):
                for c in range(2):
                    piece = halves[e, pl.ds(ph * 64 + c * 8 + r, 4, stride=16), :]
                    mine[ph, to, pl.ds((e * 2 + c) * 4, 4), :] = piece

    pl.semaphore_wait(barrier, 14 + 2 * (tile // 16))

    def remote(src, dst, send, recv, t, d):
        return pltpu.make_async_remote_copy(
            src_ref=src,
            dst_ref=dst,
            send_sem=send,
            recv_sem=recv,
            device_id=(t, d),
            device_id_type=MESH,
        )

    rows7 = pl.ds(1, 7)
    row1 = pl.ds(0, 1)
    up_all = remote(mine.at[1], other, ex_send.at[0], ex_recv.at[0], 31 - tile, depth)
    down_rest = remote(
        mine.at[0, rows7], other.at[rows7], ex_send.at[0], ex_recv.at[0], 31 - tile, depth
    )
    down_first = remote(
        mine.at[0, row1], other.at[row1], ex_send.at[1], ex_recv.at[1], first_of, depth
    )
    down_last = remote(mine.at[1, row1], other0, ex_send.at[2], ex_recv.at[1], last_to, depth)

    @pl.when(jnp.logical_not(negative))
    def _():
        up_all.start()

    @pl.when(negative)
    def _():
        down_rest.start()
        down_first.start()
        down_last.start()

    left = lambda: (mats[0], mats[1])
    right = lambda: (mats[2], mats[3])
    inv_left = lambda: (mats[4], mats[5])
    inv_right = lambda: (mats[6], mats[7])
    local[0].wait()

    def forward(p, carry):
        pltpu.make_async_copy(volume_hbm.at[:, p], vol.at[:, p], vol_sem.at[p]).wait()
        for t in range(LOCAL_TILES):
            half = dot3(split(vol[t, p]), right())
            packed[t, p] = dot3(left(), split(half))
        return carry

    lax.fori_loop(0, EARLY_PLANES, forward, 0)

    @pl.when(jnp.logical_not(negative))
    def _():
        down_rest.wait_recv()
        down_first.wait_recv()
        pos[...] = mine[0]
        neg[...] = other[...]

    @pl.when(negative)
    def _():
        up_all.wait_recv()
        down_last.wait_recv()
        pos[...] = other[...]
        neg[0] = other0[0]
        neg[1:8] = mine[1, 1:8]

    local[5].wait()
    local[6].wait()
    plane0 = jnp.where(negative, 4, 0)
    column = lax.broadcasted_iota(jnp.int32, (4, HALF), 1)
    row4 = lax.broadcasted_iota(jnp.int32, (4, HALF), 0)
    phase = jnp.zeros((4, HALF), jnp.int32)
    for q in range(4):
        phase = jnp.where(row4 == q, phases[plane0 + q], phase)
    lane0 = column == 0

    def rotor(columns):
        angle = ((phase * columns) & (SIDE - 1)).astype(f32) * (2.0 * math.pi / SIDE)
        return jnp.cos(angle), jnp.sin(angle)

    cos_p, sin_p = rotor(column)
    cos_m, sin_m = rotor(jnp.where(lane0, HALF, column))
    sin_m = jnp.where(lane0, 0.0, sin_m)
    is_first = block == 0
    for r in range(8):
        epr, epi, fpr, fpi = (pos[r, pl.ds(c * 4, 4), :] for c in range(4))
        enr, eni, fnr, fni = (neg[r, pl.ds(c * 4, 4), :] for c in range(4))
        hpr, hpi = 0.25 * (epr + fnr), 0.25 * (epi - fni)
        hmr, hmi = 0.25 * (enr + fpr), 0.25 * (eni - fpi)
        if r == 0:
            at0 = jnp.logical_and(is_first, jnp.logical_not(lane0))
            hpr = jnp.where(at0, 0.5 * (epr + fpr), hpr)
            hpi = jnp.where(at0, 0.5 * (epi - fpi), hpi)
            hmr = jnp.where(at0, 0.5 * (enr + fnr), hmr)
            hmi = jnp.where(at0, 0.5 * (eni - fni), hmi)
        lpr, lpi = 0.5 * (epr + enr), 0.5 * (epi - eni)
        lmr, lmi = 0.5 * (fpr + fnr), 0.5 * (fpi - fni)
        if r == 0:
            lpr, lpi = jnp.where(is_first, epr, lpr), jnp.where(is_first, enr, lpi)
            lmr, lmi = jnp.where(is_first, fpr, lmr), jnp.where(is_first, fnr, lmi)
        hpr, hpi = jnp.where(lane0, lpr, hpr), jnp.where(lane0, lpi, hpi)
        hmr, hmi = jnp.where(lane0, lmr, hmr), jnp.where(lane0, lmi, hmi)
        parts = (
            hpr * cos_p + hpi * sin_p,
            hpi * cos_p - hpr * sin_p,
            hmr * cos_m + hmi * sin_m,
            hmi * cos_m - hmr * sin_m,
        )
        for c in range(4):
            for q in range(4):
                table[tile, q, c, pl.ds(r, 1), :] = parts[c][q : q + 1]

    started = []

    def pass_on(which, t):
        copy = remote(
            table.at[which],
            table.at[which],
            ag_send.at[len(started)],
            ag_recv.at[which],
            t,
            depth,
        )
        copy.start()
        started.append(copy)

    def arrived(which):
        remote(
            table.at[which], table.at[which], ag_send.at[0], ag_recv.at[which], tile, depth
        ).wait_recv()

    above = at(yrow + 1, zlo, core)
    below = at(yrow + 3, zlo, core)
    sibling = at(yrow, zlo, 1 - core)
    z_order = (1, 3, 2)
    pass_on(tile, above)
    pass_on(tile, below)
    for dz in z_order:
        pass_on(tile, at(yrow, zlo + dz, core))
    pass_on(tile, sibling)

    lax.fori_loop(EARLY_PLANES, LOCAL_PLANES, forward, 0)

    for dz in z_order:
        which = at(yrow, zlo + dz, core)
        arrived(which)
        pass_on(which, above)
        pass_on(which, below)
        pass_on(which, sibling)

    for dz in (0, 1, 3, 2):
        which = at(yrow + 3, zlo + dz, core)
        arrived(which)
        if dz in (0, 1):
            pass_on(which, above)
        pass_on(which, sibling)
        which = at(yrow + 1, zlo + dz, core)
        arrived(which)
        if dz in (2, 3):
            pass_on(which, below)
        pass_on(which, sibling)
    def read_quads(ref, rows, rows2):
        return (
            ref[rows, pl.ds(0, HALF)],
            ref[rows, pl.ds(HALF, HALF)],
            ref[rows2, pl.ds(0, HALF)],
            ref[rows2, pl.ds(HALF, HALF)],
        )

    def rows_of(k):
        if isinstance(k, int):
            return pl.ds(8 * k, 8), pl.ds(HALF + 8 * k, 8)
        return pl.ds(pl.multiple_of(8 * k, 8), 8), pl.ds(pl.multiple_of(HALF + 8 * k, 8), 8)

    def table_of(p, k):
        which = k if p < 4 else 31 - k
        return tuple(table[which, p % 4, c] for c in range(4))

    def spectrum_block(t, g, j, first):
        k = 8 * g + j
        rows, rows2 = rows_of(k)
        total = None
        for p in range(LOCAL_PLANES):
            hpr, hpi, hmr, hmi = table_of(p, k)
            pr, pi, mr, mi = quads_in(*read_quads(packed.at[t, p], rows, rows2), first)
            terms = times(hpr, hpi, pr, pi, first, False) + times(hmr, hmi, mr, mi, first, False)
            total = terms if total is None else tuple(a + b for a, b in zip(total, terms))
        cc, cs, sc, ss = quads_out(*total, first)
        upper, lower = pl.ds(8 * (j % 2), 8), pl.ds(16 + 8 * (j % 2), 8)
        partial[t, g, j // 2, upper, pl.ds(0, HALF)] = cc
        partial[t, g, j // 2, upper, pl.ds(HALF, HALF)] = cs
        partial[t, g, j // 2, lower, pl.ds(0, HALF)] = sc
        partial[t, g, j // 2, lower, pl.ds(HALF, HALF)] = ss

    rs_copies = []

    def spectrum_group(t, g):
        for j in range(1, 8):
            spectrum_block(t, g, j, False)

        @pl.when(g == 0)
        def _():
            spectrum_block(t, 0, 0, True)

        @pl.when(g == 1)
        def _():
            spectrum_block(t, 1, 0, False)

        s = len(rs_copies) // 3
        for d in (1, 3, 2):
            copy = remote(
                partial.at[t, g, lax.rem(xpos + d, 4)],
                scattered.at[d - 1, s],
                rs_send.at[3 * s + d - 1],
                rs_recv.at[3 * s + d - 1],
                tile,
                xpeer(d),
            )
            copy.start()
            rs_copies.append(copy)

    near = jnp.where(jnp.logical_or(yrow == 0, yrow == 3), 0, 1)
    far = 1 - near
    for dy in (0, 1, 3):
        for dz in range(4):
            arrived(at(yrow + dy, zlo + dz, 1 - core))
    spectrum_group(0, near)
    for dz in (0, 1, 3, 2):
        which = at(yrow + 2, zlo + dz, core)
        arrived(which)
        pass_on(which, sibling)
    spectrum_group(1, near)
    for dz in range(4):
        arrived(at(yrow + 2, zlo + dz, 1 - core))
    spectrum_group(0, far)
    spectrum_group(1, far)
    pieces = ((0, near), (1, near), (0, far), (1, far))
    z_copies = []
    for s, (t, g) in enumerate(pieces):
        for copy in rs_copies[3 * s : 3 * s + 3]:
            copy.wait_recv()
        zsend[s] = partial[t, g, xpos] + scattered[0, s] + scattered[1, s] + scattered[2, s]
        copy = remote(zsend.at[s], zrecv.at[s], z_send.at[s], z_recv.at[s], tile, zpartner)
        copy.start()
        z_copies.append(copy)
    local[1].wait()
    local[2].wait()
    xg_copies = []
    for s, (t, g) in enumerate(pieces):
        z_copies[s].wait_recv()
        spectrum[t, g, xpos] = zsend[s] + zrecv[s]
        for d in (1, 3, 2):
            copy = remote(
                spectrum.at[t, g, xpos],
                spectrum.at[t, g, xpos],
                xg_send.at[3 * s + d - 1],
                xg_recv.at[3 * s + d - 1],
                tile,
                xpeer(d),
            )
            copy.start()
            xg_copies.append(copy)

    def strip(p, t, image_part, rows):
        values = vol[t, p, rows, :]
        return jnp.maximum(values * (1.0 + STEP_GAIN * image_part), 0.0)

    def to_before(p):
        return remote(
            top_send.at[p], after_recv.at[p], halo_send.at[p], halo_recv.at[p], before, depth
        )

    def to_after(p):
        slot = LOCAL_PLANES + p
        return remote(
            bottom_send.at[p], before_recv.at[p], halo_send.at[slot], halo_recv.at[slot], after, depth
        )

    for t in range(LOCAL_TILES):
        for copy in xg_copies[3 * t : 3 * t + 3] + xg_copies[3 * t + 6 : 3 * t + 9]:
            copy.wait_recv()
        for k in range(16):
            rows, rows2 = rows_of(k)
            found = spectrum.at[t, k // 8, (k % 8) // 2]
            sums[t, rows, :] = found[pl.ds(8 * (k % 2), 8), :]
            sums[t, rows2, :] = found[pl.ds(16 + 8 * (k % 2), 8), :]
        half = dot3(split(sums[t]), inv_right())
        here = pl.ds(t * SIDE, SIDE)
        projection = background[here, :] + dot3(inv_left(), split(half))
        ratio = measured[here, :] / jnp.maximum(projection, FLOOR_LEVEL)
        half = dot3(split(ratio - 1.0), right())
        sums[t] = dot3(left(), split(half))
        for k in range(16):
            rows, rows2 = rows_of(k)
            found = quads_in(*read_quads(sums.at[t], rows, rows2), k == 0)
            for c in range(4):
                ratio_quads[t, c, rows, :] = found[c]

        def backward(q, carry, t=t):
            for h in range(2):
                p = q + 4 * h
                for k in range(16):
                    rows, rows2 = rows_of(k)
                    which = 31 - k if h else k
                    hpr, hpi, hmr, hmi = (table[which, q, c] for c in range(4))
                    pr, pi, mr, mi = (ratio_quads[t, c, rows, :] for c in range(4))
                    plus = times(hpr, hpi, pr, pi, k == 0, True)
                    minus = times(hmr, hmi, mr, mi, k == 0, True)
                    cc, cs, sc, ss = quads_out(*plus, *minus, k == 0)
                    quads[h, rows, pl.ds(0, HALF)] = cc
                    quads[h, rows, pl.ds(HALF, HALF)] = cs
                    quads[h, rows2, pl.ds(0, HALF)] = sc
                    quads[h, rows2, pl.ds(HALF, HALF)] = ss
                half = split(dot3(split(quads[h]), inv_right()))
                part_high[t, p] = half[0]
                part_low[t, p] = half[1]
                rows = slice(0, WIDTH) if t == 0 else slice(SIDE - WIDTH, SIDE)
                edge = strip(p, t, dot3((mats[4, rows], mats[5, rows]), half), rows)
                if t == 0:
                    top_send[p] = edge
                else:
                    bottom_send[p] = edge
            for h in range(2):
                (to_after if t else to_before)(q + 4 * h).start()
            return carry

        lax.fori_loop(0, 4, backward, 0)

    base = tile * LOCAL_TILES
    w_inner = ramp(margins[base])
    w_after = ramp(margins[base + 1])
    w_before = ramp(margins[lax.rem(base + TILES - 1, TILES)])

    def finish_plane(p, carry):
        half = (part_high[0, p], part_low[0, p])
        rows = slice(WIDTH, SIDE)
        upper = strip(p, 0, dot3((mats[4, rows], mats[5, rows]), half), rows)
        half = (part_high[1, p], part_low[1, p])
        rows = slice(0, SIDE - WIDTH)
        lower = strip(p, 1, dot3((mats[4, rows], mats[5, rows]), half), rows)
        inner = SIDE - 2 * WIDTH
        shared = (1.0 - w_inner) * upper[inner:] + w_inner * lower[:WIDTH]
        out[0, p, WIDTH : SIDE - WIDTH, :] = upper[:inner]
        out[0, p, SIDE - WIDTH :, :] = shared
        out[1, p, :WIDTH, :] = shared
        out[1, p, WIDTH : SIDE - WIDTH, :] = lower[WIDTH:]
        return carry

    lax.fori_loop(0, LOCAL_PLANES, finish_plane, 0)

    @pl.when(jnp.logical_not(negative))
    def _():
        up_all.wait_send()

    @pl.when(negative)
    def _():
        down_rest.wait_send()
        down_first.wait_send()
        down_last.wait_send()

    for copy in started + rs_copies + z_copies + xg_copies:
        copy.wait_send()

    def last_strip(p, carry):
        to_before(p).wait_recv()
        out[1, p, SIDE - WIDTH :, :] = (1.0 - w_after) * bottom_send[p] + w_after * after_recv[p]
        return carry

    lax.fori_loop(0, LOCAL_PLANES, last_strip, 0)

    def first_strip(p, carry):
        to_after(p).wait_recv()
        out[0, p, :WIDTH, :] = (1.0 - w_before) * before_recv[p] + w_before * top_send[p]
        return carry

    lax.fori_loop(0, LOCAL_PLANES, first_strip, 0)

    def drain(p, carry):
        to_before(p).wait_send()
        to_after(p).wait_send()
        return carry

    lax.fori_loop(0, LOCAL_PLANES, drain, 0)


def on_device(volume, transfer, measured, background, margins, phases):
    mats = packed_tables()
    hbm = pl.BlockSpec(memory_space=pltpu.HBM)
    dma = pltpu.SemaphoreType.DMA
    tall = LOCAL_TILES * SIDE
    return pl.pallas_call(
        kernel,
        name="update",
        out_shape=jax.ShapeDtypeStruct(volume.shape, f32),
        in_specs=[hbm] * 8,
        out_specs=pl.BlockSpec(memory_space=pltpu.VMEM),
        scratch_shapes=[
            pltpu.SMEM((LOCAL_PLANES,), jnp.int32),
            pltpu.SMEM((TILES,), jnp.int32),
            pltpu.VMEM((LOCAL_PLANES, 2, 8, SIDE), f32),
            pltpu.VMEM((HALF, HALF), bf16),
            pltpu.VMEM((LOCAL_TILES, LOCAL_PLANES, SIDE, SIDE), f32),
            pltpu.VMEM((LOCAL_TILES, LOCAL_PLANES, SIDE, SIDE), f32),
            pltpu.VMEM((32, 4, 4, 8, HALF), f32),
            pltpu.VMEM((8, SIDE, SIDE), bf16),
            pltpu.VMEM((tall, SIDE), f32),
            pltpu.VMEM((tall, SIDE), f32),
            pltpu.VMEM((2, HALF, HALF), f32),
            pltpu.VMEM((2, 8, 16, HALF), f32),
            pltpu.VMEM((8, 16, HALF), f32),
            pltpu.VMEM((1, 16, HALF), f32),
            pltpu.VMEM((8, 16, HALF), f32),
            pltpu.VMEM((8, 16, HALF), f32),
            pltpu.VMEM((LOCAL_TILES, SIDE, SIDE), f32),
            pltpu.VMEM((LOCAL_TILES, 2, 4, WIDTH, SIDE), f32),
            pltpu.VMEM((3, PIECES, WIDTH, SIDE), f32),
            pltpu.VMEM((PIECES, WIDTH, SIDE), f32),
            pltpu.VMEM((PIECES, WIDTH, SIDE), f32),
            pltpu.VMEM((LOCAL_TILES, 2, 4, WIDTH, SIDE), f32),
            pltpu.VMEM((LOCAL_TILES, 4, HALF, HALF), f32),
            pltpu.VMEM((LOCAL_TILES, SIDE, SIDE), f32),
            pltpu.VMEM((LOCAL_TILES, LOCAL_PLANES, SIDE, SIDE), bf16),
            pltpu.VMEM((LOCAL_TILES, LOCAL_PLANES, SIDE, SIDE), bf16),
            pltpu.VMEM((LOCAL_PLANES, WIDTH, SIDE), f32),
            pltpu.VMEM((LOCAL_PLANES, WIDTH, SIDE), f32),
            pltpu.VMEM((LOCAL_PLANES, WIDTH, SIDE), f32),
            pltpu.VMEM((LOCAL_PLANES, WIDTH, SIDE), f32),
            dma((LOCAL_PLANES,)),
            dma((7,)),
            dma((3,)),
            dma((2,)),
            dma((31,)),
            dma((32,)),
            dma((3 * PIECES,)),
            dma((3 * PIECES,)),
            dma((PIECES,)),
            dma((PIECES,)),
            dma((3 * PIECES,)),
            dma((3 * PIECES,)),
            dma((2 * LOCAL_PLANES,)),
            dma((2 * LOCAL_PLANES,)),
        ],
        compiler_params=pltpu.CompilerParams(
            collective_id=0, has_side_effects=True, vmem_limit_bytes=48 * 1024 * 1024
        ),
    )(
        *(
            pltpu.with_memory_space_constraint(array, pltpu.HBM)
            for array in (
                phases,
                margins,
                transfer,
                volume,
                measured.reshape(tall, SIDE),
                background.reshape(tall, SIDE),
                mats,
                pairing(),
            )
        )
    )


def solution(mesh):
    return jax.shard_map(
        on_device,
        mesh=mesh,
        in_specs=(
            P("tile", "depth", None, None),
            P("depth", None, "tile", None),
            P("tile", None, None),
            P("tile", None, None),
            P(),
            P("depth"),
        ),
        out_specs=P("tile", "depth", None, None),
        check_vma=False,
    )
```

```python
import functools
import math

import jax
import jax.numpy as jnp
import numpy as np
from jax import lax
from jax.experimental import pallas as pl
from jax.experimental.pallas import tpu as pltpu
from jax.sharding import PartitionSpec as P

SIDE = 256
HALF = 128
WIDTH = 32
TILES = 64
LOCAL_TILES = 2
LOCAL_PLANES = 8
PIECES = 4
EARLY_PLANES = 3
FLOOR_LEVEL = 0.5
STEP_GAIN = 2.0
MESH = pl.DeviceIdType.MESH
f32 = jnp.float32
bf16 = jnp.bfloat16


def packed_tables():
    place = np.arange(SIDE)
    table = np.zeros((SIDE, SIDE))
    for a in range(HALF):
        table[a] = np.cos(2 * np.pi * (a * place % SIDE) / SIDE)
    table[HALF] = 1.0 - 2.0 * (place % 2)
    for a in range(1, HALF):
        table[HALF + a] = np.sin(2 * np.pi * (a * place % SIDE) / SIDE)
    weight = np.full(SIDE, 2.0)
    weight[0] = weight[HALF] = 1.0
    inverse = table.T * weight / SIDE
    pieces = []
    for matrix in (table, table.T, inverse, inverse.T):
        high = matrix.astype(bf16)
        pieces += [high, (matrix - high.astype(np.float64)).astype(bf16)]
    return jnp.asarray(np.stack(pieces))


def pairing():
    move = np.zeros((HALF, HALF), np.float32)
    move[0, 0] = 1.0
    for b in range(1, HALF):
        move[HALF - b, b] = 1.0
    return jnp.asarray(move.astype(bf16))


def split(values):
    high = values.astype(bf16)
    return high, (values - high.astype(f32)).astype(bf16)


def dot(a, b):
    return jnp.dot(a, b, preferred_element_type=f32)


def dot3(a, b):
    return dot(a[0], b[0]) + dot(a[1], b[0]) + dot(a[0], b[1])


def special(shape, first):
    lane0 = lax.broadcasted_iota(jnp.int32, shape, 1) == 0
    row0 = None
    if first:
        row0 = jnp.logical_and(
            lax.broadcasted_iota(jnp.int32, shape, 0) == 0, jnp.logical_not(lane0)
        )
    return lane0, row0


def quads_in(cc, cs, sc, ss, first):
    lane0, row0 = special(cc.shape, first)
    pr, pi, mr, mi = cc - ss, cs + sc, cc + ss, cs - sc
    if first:
        pr = jnp.where(row0, cc, pr)
        pi = jnp.where(row0, cs, pi)
        mr = jnp.where(row0, sc, mr)
        mi = jnp.where(row0, ss, mi)
    return (
        jnp.where(lane0, cc, pr),
        jnp.where(lane0, sc, pi),
        jnp.where(lane0, cs, mr),
        jnp.where(lane0, ss, mi),
    )


def quads_out(pr, pi, mr, mi, first):
    lane0, row0 = special(pr.shape, first)
    cc, ss, cs, sc = pr + mr, mr - pr, pi + mi, pi - mi
    if first:
        cc = jnp.where(row0, pr, cc)
        cs = jnp.where(row0, pi, cs)
        sc = jnp.where(row0, mr, sc)
        ss = jnp.where(row0, mi, ss)
    return (
        jnp.where(lane0, pr, cc),
        jnp.where(lane0, mr, cs),
        jnp.where(lane0, pi, sc),
        jnp.where(lane0, mi, ss),
    )


def times(hr, hi, real, imag, first, conj):
    second = hr
    if first:
        lane0, _ = special(hr.shape, False)
        corner = jnp.logical_and(lane0, lax.broadcasted_iota(jnp.int32, hr.shape, 0) == 0)
        second = jnp.where(corner, hi, hr)
        hi = jnp.where(corner, 0.0, hi)
    if conj:
        return hr * real - hi * imag, second * imag + hi * real
    return hr * real + hi * imag, second * imag - hi * real


def ramp(margin):
    margin = margin.astype(f32)
    row = lax.broadcasted_iota(jnp.int32, (WIDTH, SIDE), 0).astype(f32)
    return jnp.clip((row + 0.5 - (WIDTH - margin) / 2.0) / margin, 0.0, 1.0)


def kernel(
    phases_hbm,
    margins_hbm,
    transfer_hbm,
    volume_hbm,
    measured_hbm,
    background_hbm,
    mats_hbm,
    pair_hbm,
    out,
    phases,
    margins,
    transfer,
    pair_ref,
    vol,
    packed,
    table,
    mats,
    measured,
    background,
    halves,
    mine,
    other,
    other0,
    pos,
    neg,
    sums,
    partial,
    scattered,
    zsend,
    zrecv,
    spectrum,
    ratio_quads,
    quads,
    part_high,
    part_low,
    top_send,
    bottom_send,
    after_recv,
    before_recv,
    vol_sem,
    in_sem,
    ex_send,
    ex_recv,
    ag_send,
    ag_recv,
    rs_send,
    rs_recv,
    z_send,
    z_recv,
    xg_send,
    xg_recv,
    halo_send,
    halo_recv,
):
    tile = lax.axis_index("tile")
    depth = lax.axis_index("depth")
    core = lax.rem(tile, 2)
    zlo = lax.rem(tile // 2, 4)
    yrow = tile // 8
    xpos = lax.rem(depth, 4)
    zhi = depth // 4
    negative = tile >= 16
    block = jnp.where(negative, 31 - tile, tile)

    def at(y, z, c):
        return lax.rem(y, 4) * 8 + lax.rem(z, 4) * 2 + c

    def xpeer(d):
        return zhi * 4 + lax.rem(xpos + d, 4)

    after = lax.rem(tile + 1, 32)
    before = lax.rem(tile + 31, 32)
    zpartner = (1 - zhi) * 4 + xpos

    volume_copies = []
    for p in range(LOCAL_PLANES):
        volume_copies.append(
            pltpu.make_async_copy(volume_hbm.at[:, p], vol.at[:, p], vol_sem.at[p])
        )
    local = [
        pltpu.make_async_copy(mats_hbm, mats, in_sem.at[0]),
        pltpu.make_async_copy(measured_hbm, measured, in_sem.at[1]),
        pltpu.make_async_copy(background_hbm, background, in_sem.at[2]),
        pltpu.make_async_copy(transfer_hbm, transfer, in_sem.at[3]),
        pltpu.make_async_copy(pair_hbm, pair_ref, in_sem.at[4]),
        pltpu.make_async_copy(phases_hbm, phases, in_sem.at[5]),
        pltpu.make_async_copy(margins_hbm, margins, in_sem.at[6]),
    ]
    for which in (3, 4, 0, 5, 6):
        local[which].start()
    for copy in volume_copies:
        copy.start()
    local[1].start()
    local[2].start()

    barrier = pltpu.get_barrier_semaphore()

    def greet(t, d):
        pl.semaphore_signal(barrier, inc=1, device_id=(t, d), device_id_type=MESH)

    greet(31 - tile, depth)
    for dz in range(1, 4):
        greet(at(yrow, zlo + dz, core), depth)
    greet(at(yrow + 1, zlo, core), depth)
    greet(at(yrow + 3, zlo, core), depth)
    greet(at(yrow, zlo, 1 - core), depth)
    for d in range(1, 4):
        greet(tile, xpeer(d))
    greet(tile, zpartner)
    greet(after, depth)
    greet(before, depth)
    first_of = lax.rem(32 - tile, 16)
    last_to = jnp.where(tile == 16, 31, tile - 1)
    last_from = jnp.where(tile == 31, 16, tile + 1)
    row0_from = jnp.where(tile == 0, 16, 32 - tile)

    @pl.when(negative)
    def _():
        greet(first_of, depth)
        greet(last_to, depth)
        greet(last_from, depth)

    @pl.when(jnp.logical_not(negative))
    def _():
        greet(row0_from, depth)

    local[3].wait()
    local[4].wait()
    whole = transfer[...].reshape(LOCAL_PLANES * 2 * 8, SIDE)
    halves[0] = whole[:, :HALF]
    rest = whole[:, HALF:]
    high, low = split(rest)
    lowest = ((rest - high.astype(f32)) - low.astype(f32)).astype(bf16)
    move = pair_ref[...]
    halves[1] = dot(high, move) + dot(low, move) + dot(lowest, move)
    for r in range(8):
        to = jnp.where(negative, (8 - r) % 8, r)
        for ph in range(2):
            for e in range(2):
                for c in range(2):
                    piece = halves[e, pl.ds(ph * 64 + c * 8 + r, 4, stride=16), :]
                    mine[ph, to, pl.ds((e * 2 + c) * 4, 4), :] = piece

    pl.semaphore_wait(barrier, 14 + 2 * (tile // 16))

    def remote(src, dst, send, recv, t, d):
        return pltpu.make_async_remote_copy(
            src_ref=src,
            dst_ref=dst,
            send_sem=send,
            recv_sem=recv,
            device_id=(t, d),
            device_id_type=MESH,
        )

    rows7 = pl.ds(1, 7)
    row1 = pl.ds(0, 1)
    up_all = remote(mine.at[1], other, ex_send.at[0], ex_recv.at[0], 31 - tile, depth)
    down_rest = remote(
        mine.at[0, rows7], other.at[rows7], ex_send.at[0], ex_recv.at[0], 31 - tile, depth
    )
    down_first = remote(
        mine.at[0, row1], other.at[row1], ex_send.at[1], ex_recv.at[1], first_of, depth
    )
    down_last = remote(mine.at[1, row1], other0, ex_send.at[2], ex_recv.at[1], last_to, depth)

    @pl.when(jnp.logical_not(negative))
    def _():
        up_all.start()

    @pl.when(negative)
    def _():
        down_rest.start()
        down_first.start()
        down_last.start()

    left = lambda: (mats[0], mats[1])
    right = lambda: (mats[2], mats[3])
    inv_left = lambda: (mats[4], mats[5])
    inv_right = lambda: (mats[6], mats[7])
    local[0].wait()

    def forward(p, carry):
        pltpu.make_async_copy(volume_hbm.at[:, p], vol.at[:, p], vol_sem.at[p]).wait()
        for t in range(LOCAL_TILES):
            half = dot3(split(vol[t, p]), right())
            packed[t, p] = dot3(left(), split(half))
        return carry

    lax.fori_loop(0, EARLY_PLANES, forward, 0)

    @pl.when(jnp.logical_not(negative))
    def _():
        down_rest.wait_recv()
        down_first.wait_recv()
        pos[...] = mine[0]
        neg[...] = other[...]

    @pl.when(negative)
    def _():
        up_all.wait_recv()
        down_last.wait_recv()
        pos[...] = other[...]
        neg[0] = other0[0]
        neg[1:8] = mine[1, 1:8]

    local[5].wait()
    local[6].wait()
    plane0 = jnp.where(negative, 4, 0)
    column = lax.broadcasted_iota(jnp.int32, (4, HALF), 1)
    row4 = lax.broadcasted_iota(jnp.int32, (4, HALF), 0)
    phase = jnp.zeros((4, HALF), jnp.int32)
    for q in range(4):
        phase = jnp.where(row4 == q, phases[plane0 + q], phase)
    lane0 = column == 0

    def rotor(columns):
        angle = ((phase * columns) & (SIDE - 1)).astype(f32) * (2.0 * math.pi / SIDE)
        return jnp.cos(angle), jnp.sin(angle)

    cos_p, sin_p = rotor(column)
    cos_m, sin_m = rotor(jnp.where(lane0, HALF, column))
    sin_m = jnp.where(lane0, 0.0, sin_m)
    is_first = block == 0
    for r in range(8):
        epr, epi, fpr, fpi = (pos[r, pl.ds(c * 4, 4), :] for c in range(4))
        enr, eni, fnr, fni = (neg[r, pl.ds(c * 4, 4), :] for c in range(4))
        hpr, hpi = 0.25 * (epr + fnr), 0.25 * (epi - fni)
        hmr, hmi = 0.25 * (enr + fpr), 0.25 * (eni - fpi)
        if r == 0:
            at0 = jnp.logical_and(is_first, jnp.logical_not(lane0))
            hpr = jnp.where(at0, 0.5 * (epr + fpr), hpr)
            hpi = jnp.where(at0, 0.5 * (epi - fpi), hpi)
            hmr = jnp.where(at0, 0.5 * (enr + fnr), hmr)
            hmi = jnp.where(at0, 0.5 * (eni - fni), hmi)
        lpr, lpi = 0.5 * (epr + enr), 0.5 * (epi - eni)
        lmr, lmi = 0.5 * (fpr + fnr), 0.5 * (fpi - fni)
        if r == 0:
            lpr, lpi = jnp.where(is_first, epr, lpr), jnp.where(is_first, enr, lpi)
            lmr, lmi = jnp.where(is_first, fpr, lmr), jnp.where(is_first, fnr, lmi)
        hpr, hpi = jnp.where(lane0, lpr, hpr), jnp.where(lane0, lpi, hpi)
        hmr, hmi = jnp.where(lane0, lmr, hmr), jnp.where(lane0, lmi, hmi)
        parts = (
            hpr * cos_p + hpi * sin_p,
            hpi * cos_p - hpr * sin_p,
            hmr * cos_m + hmi * sin_m,
            hmi * cos_m - hmr * sin_m,
        )
        for c in range(4):
            for q in range(4):
                table[tile, q, c, pl.ds(r, 1), :] = parts[c][q : q + 1]

    started = []

    def pass_on(which, t):
        copy = remote(
            table.at[which],
            table.at[which],
            ag_send.at[len(started)],
            ag_recv.at[which],
            t,
            depth,
        )
        copy.start()
        started.append(copy)

    def arrived(which):
        remote(
            table.at[which], table.at[which], ag_send.at[0], ag_recv.at[which], tile, depth
        ).wait_recv()

    above = at(yrow + 1, zlo, core)
    below = at(yrow + 3, zlo, core)
    sibling = at(yrow, zlo, 1 - core)
    z_order = (1, 3, 2)
    for dz in z_order:
        pass_on(tile, at(yrow, zlo + dz, core))
    pass_on(tile, above)
    pass_on(tile, below)
    pass_on(tile, sibling)

    lax.fori_loop(EARLY_PLANES, LOCAL_PLANES, forward, 0)

    for dz in z_order:
        which = at(yrow, zlo + dz, core)
        arrived(which)
        pass_on(which, above)
        pass_on(which, below)
        pass_on(which, sibling)

    for dz in (0, 1, 3, 2):
        which = at(yrow + 3, zlo + dz, core)
        arrived(which)
        if dz in (0, 1):
            pass_on(which, above)
        pass_on(which, sibling)
        which = at(yrow + 1, zlo + dz, core)
        arrived(which)
        if dz in (2, 3):
            pass_on(which, below)
        pass_on(which, sibling)
    def read_quads(ref, rows, rows2):
        return (
            ref[rows, pl.ds(0, HALF)],
            ref[rows, pl.ds(HALF, HALF)],
            ref[rows2, pl.ds(0, HALF)],
            ref[rows2, pl.ds(HALF, HALF)],
        )

    def rows_of(k):
        if isinstance(k, int):
            return pl.ds(8 * k, 8), pl.ds(HALF + 8 * k, 8)
        return pl.ds(pl.multiple_of(8 * k, 8), 8), pl.ds(pl.multiple_of(HALF + 8 * k, 8), 8)

    def table_of(p, k):
        which = k if p < 4 else 31 - k
        return tuple(table[which, p % 4, c] for c in range(4))

    def spectrum_block(t, g, j, first):
        k = 8 * g + j
        rows, rows2 = rows_of(k)
        total = None
        for p in range(LOCAL_PLANES):
            hpr, hpi, hmr, hmi = table_of(p, k)
            pr, pi, mr, mi = quads_in(*read_quads(packed.at[t, p], rows, rows2), first)
            terms = times(hpr, hpi, pr, pi, first, False) + times(hmr, hmi, mr, mi, first, False)
            total = terms if total is None else tuple(a + b for a, b in zip(total, terms))
        cc, cs, sc, ss = quads_out(*total, first)
        upper, lower = pl.ds(8 * (j % 2), 8), pl.ds(16 + 8 * (j % 2), 8)
        partial[t, g, j // 2, upper, pl.ds(0, HALF)] = cc
        partial[t, g, j // 2, upper, pl.ds(HALF, HALF)] = cs
        partial[t, g, j // 2, lower, pl.ds(0, HALF)] = sc
        partial[t, g, j // 2, lower, pl.ds(HALF, HALF)] = ss

    rs_copies = []

    def spectrum_group(t, g):
        for j in range(1, 8):
            spectrum_block(t, g, j, False)

        @pl.when(g == 0)
        def _():
            spectrum_block(t, 0, 0, True)

        @pl.when(g == 1)
        def _():
            spectrum_block(t, 1, 0, False)

        s = len(rs_copies) // 3
        for d in (1, 3, 2):
            copy = remote(
                partial.at[t, g, lax.rem(xpos + d, 4)],
                scattered.at[d - 1, s],
                rs_send.at[3 * s + d - 1],
                rs_recv.at[3 * s + d - 1],
                tile,
                xpeer(d),
            )
            copy.start()
            rs_copies.append(copy)

    near = jnp.where(jnp.logical_or(yrow == 0, yrow == 3), 0, 1)
    far = 1 - near
    for dy in (0, 1, 3):
        for dz in range(4):
            arrived(at(yrow + dy, zlo + dz, 1 - core))
    spectrum_group(0, near)
    for dz in (0, 1, 3, 2):
        which = at(yrow + 2, zlo + dz, core)
        arrived(which)
        pass_on(which, sibling)
    spectrum_group(1, near)
    for dz in range(4):
        arrived(at(yrow + 2, zlo + dz, 1 - core))
    spectrum_group(0, far)
    spectrum_group(1, far)
    pieces = ((0, near), (1, near), (0, far), (1, far))
    z_copies = []
    for s, (t, g) in enumerate(pieces):
        for copy in rs_copies[3 * s : 3 * s + 3]:
            copy.wait_recv()
        zsend[s] = partial[t, g, xpos] + scattered[0, s] + scattered[1, s] + scattered[2, s]
        copy = remote(zsend.at[s], zrecv.at[s], z_send.at[s], z_recv.at[s], tile, zpartner)
        copy.start()
        z_copies.append(copy)
    local[1].wait()
    local[2].wait()
    xg_copies = []
    for s, (t, g) in enumerate(pieces):
        z_copies[s].wait_recv()
        spectrum[t, g, xpos] = zsend[s] + zrecv[s]
        for d in (1, 3, 2):
            copy = remote(
                spectrum.at[t, g, xpos],
                spectrum.at[t, g, xpos],
                xg_send.at[3 * s + d - 1],
                xg_recv.at[3 * s + d - 1],
                tile,
                xpeer(d),
            )
            copy.start()
            xg_copies.append(copy)

    def strip(p, t, image_part, rows):
        values = vol[t, p, rows, :]
        return jnp.maximum(values * (1.0 + STEP_GAIN * image_part), 0.0)

    def to_before(p):
        return remote(
            top_send.at[p], after_recv.at[p], halo_send.at[p], halo_recv.at[p], before, depth
        )

    def to_after(p):
        slot = LOCAL_PLANES + p
        return remote(
            bottom_send.at[p], before_recv.at[p], halo_send.at[slot], halo_recv.at[slot], after, depth
        )

    for t in range(LOCAL_TILES):
        for copy in xg_copies[3 * t : 3 * t + 3] + xg_copies[3 * t + 6 : 3 * t + 9]:
            copy.wait_recv()
        for k in range(16):
            rows, rows2 = rows_of(k)
            found = spectrum.at[t, k // 8, (k % 8) // 2]
            sums[t, rows, :] = found[pl.ds(8 * (k % 2), 8), :]
            sums[t, rows2, :] = found[pl.ds(16 + 8 * (k % 2), 8), :]
        half = dot3(split(sums[t]), inv_right())
        here = pl.ds(t * SIDE, SIDE)
        projection = background[here, :] + dot3(inv_left(), split(half))
        ratio = measured[here, :] / jnp.maximum(projection, FLOOR_LEVEL)
        half = dot3(split(ratio - 1.0), right())
        sums[t] = dot3(left(), split(half))
        for k in range(16):
            rows, rows2 = rows_of(k)
            found = quads_in(*read_quads(sums.at[t], rows, rows2), k == 0)
            for c in range(4):
                ratio_quads[t, c, rows, :] = found[c]

        def backward(q, carry, t=t):
            for h in range(2):
                p = q + 4 * h
                for k in range(16):
                    rows, rows2 = rows_of(k)
                    which = 31 - k if h else k
                    hpr, hpi, hmr, hmi = (table[which, q, c] for c in range(4))
                    pr, pi, mr, mi = (ratio_quads[t, c, rows, :] for c in range(4))
                    plus = times(hpr, hpi, pr, pi, k == 0, True)
                    minus = times(hmr, hmi, mr, mi, k == 0, True)
                    cc, cs, sc, ss = quads_out(*plus, *minus, k == 0)
                    quads[h, rows, pl.ds(0, HALF)] = cc
                    quads[h, rows, pl.ds(HALF, HALF)] = cs
                    quads[h, rows2, pl.ds(0, HALF)] = sc
                    quads[h, rows2, pl.ds(HALF, HALF)] = ss
                half = split(dot3(split(quads[h]), inv_right()))
                part_high[t, p] = half[0]
                part_low[t, p] = half[1]
                rows = slice(0, WIDTH) if t == 0 else slice(SIDE - WIDTH, SIDE)
                edge = strip(p, t, dot3((mats[4, rows], mats[5, rows]), half), rows)
                if t == 0:
                    top_send[p] = edge
                else:
                    bottom_send[p] = edge
            for h in range(2):
                (to_after if t else to_before)(q + 4 * h).start()
            return carry

        lax.fori_loop(0, 4, backward, 0)

    base = tile * LOCAL_TILES
    w_inner = ramp(margins[base])
    w_after = ramp(margins[base + 1])
    w_before = ramp(margins[lax.rem(base + TILES - 1, TILES)])

    def finish_plane(p, carry):
        half = (part_high[0, p], part_low[0, p])
        rows = slice(WIDTH, SIDE)
        upper = strip(p, 0, dot3((mats[4, rows], mats[5, rows]), half), rows)
        half = (part_high[1, p], part_low[1, p])
        rows = slice(0, SIDE - WIDTH)
        lower = strip(p, 1, dot3((mats[4, rows], mats[5, rows]), half), rows)
        inner = SIDE - 2 * WIDTH
        shared = (1.0 - w_inner) * upper[inner:] + w_inner * lower[:WIDTH]
        out[0, p, WIDTH : SIDE - WIDTH, :] = upper[:inner]
        out[0, p, SIDE - WIDTH :, :] = shared
        out[1, p, :WIDTH, :] = shared
        out[1, p, WIDTH : SIDE - WIDTH, :] = lower[WIDTH:]
        return carry

    lax.fori_loop(0, LOCAL_PLANES, finish_plane, 0)

    @pl.when(jnp.logical_not(negative))
    def _():
        up_all.wait_send()

    @pl.when(negative)
    def _():
        down_rest.wait_send()
        down_first.wait_send()
        down_last.wait_send()

    for copy in started + rs_copies + z_copies + xg_copies:
        copy.wait_send()

    def last_strip(p, carry):
        to_before(p).wait_recv()
        out[1, p, SIDE - WIDTH :, :] = (1.0 - w_after) * bottom_send[p] + w_after * after_recv[p]
        return carry

    lax.fori_loop(0, LOCAL_PLANES, last_strip, 0)

    def first_strip(p, carry):
        to_after(p).wait_recv()
        out[0, p, :WIDTH, :] = (1.0 - w_before) * before_recv[p] + w_before * top_send[p]
        return carry

    lax.fori_loop(0, LOCAL_PLANES, first_strip, 0)

    def drain(p, carry):
        to_before(p).wait_send()
        to_after(p).wait_send()
        return carry

    lax.fori_loop(0, LOCAL_PLANES, drain, 0)


def on_device(volume, transfer, measured, background, margins, phases):
    mats = packed_tables()
    hbm = pl.BlockSpec(memory_space=pltpu.HBM)
    dma = pltpu.SemaphoreType.DMA
    tall = LOCAL_TILES * SIDE
    return pl.pallas_call(
        kernel,
        name="update",
        out_shape=jax.ShapeDtypeStruct(volume.shape, f32),
        in_specs=[hbm] * 8,
        out_specs=pl.BlockSpec(memory_space=pltpu.VMEM),
        scratch_shapes=[
            pltpu.SMEM((LOCAL_PLANES,), jnp.int32),
            pltpu.SMEM((TILES,), jnp.int32),
            pltpu.VMEM((LOCAL_PLANES, 2, 8, SIDE), f32),
            pltpu.VMEM((HALF, HALF), bf16),
            pltpu.VMEM((LOCAL_TILES, LOCAL_PLANES, SIDE, SIDE), f32),
            pltpu.VMEM((LOCAL_TILES, LOCAL_PLANES, SIDE, SIDE), f32),
            pltpu.VMEM((32, 4, 4, 8, HALF), f32),
            pltpu.VMEM((8, SIDE, SIDE), bf16),
            pltpu.VMEM((tall, SIDE), f32),
            pltpu.VMEM((tall, SIDE), f32),
            pltpu.VMEM((2, HALF, HALF), f32),
            pltpu.VMEM((2, 8, 16, HALF), f32),
            pltpu.VMEM((8, 16, HALF), f32),
            pltpu.VMEM((1, 16, HALF), f32),
            pltpu.VMEM((8, 16, HALF), f32),
            pltpu.VMEM((8, 16, HALF), f32),
            pltpu.VMEM((LOCAL_TILES, SIDE, SIDE), f32),
            pltpu.VMEM((LOCAL_TILES, 2, 4, WIDTH, SIDE), f32),
            pltpu.VMEM((3, PIECES, WIDTH, SIDE), f32),
            pltpu.VMEM((PIECES, WIDTH, SIDE), f32),
            pltpu.VMEM((PIECES, WIDTH, SIDE), f32),
            pltpu.VMEM((LOCAL_TILES, 2, 4, WIDTH, SIDE), f32),
            pltpu.VMEM((LOCAL_TILES, 4, HALF, HALF), f32),
            pltpu.VMEM((LOCAL_TILES, SIDE, SIDE), f32),
            pltpu.VMEM((LOCAL_TILES, LOCAL_PLANES, SIDE, SIDE), bf16),
            pltpu.VMEM((LOCAL_TILES, LOCAL_PLANES, SIDE, SIDE), bf16),
            pltpu.VMEM((LOCAL_PLANES, WIDTH, SIDE), f32),
            pltpu.VMEM((LOCAL_PLANES, WIDTH, SIDE), f32),
            pltpu.VMEM((LOCAL_PLANES, WIDTH, SIDE), f32),
            pltpu.VMEM((LOCAL_PLANES, WIDTH, SIDE), f32),
            dma((LOCAL_PLANES,)),
            dma((7,)),
            dma((3,)),
            dma((2,)),
            dma((31,)),
            dma((32,)),
            dma((3 * PIECES,)),
            dma((3 * PIECES,)),
            dma((PIECES,)),
            dma((PIECES,)),
            dma((3 * PIECES,)),
            dma((3 * PIECES,)),
            dma((2 * LOCAL_PLANES,)),
            dma((2 * LOCAL_PLANES,)),
        ],
        compiler_params=pltpu.CompilerParams(
            collective_id=0, has_side_effects=True, vmem_limit_bytes=48 * 1024 * 1024
        ),
    )(
        *(
            pltpu.with_memory_space_constraint(array, pltpu.HBM)
            for array in (
                phases,
                margins,
                transfer,
                volume,
                measured.reshape(tall, SIDE),
                background.reshape(tall, SIDE),
                mats,
                pairing(),
            )
        )
    )


def solution(mesh):
    return jax.shard_map(
        on_device,
        mesh=mesh,
        in_specs=(
            P("tile", "depth", None, None),
            P("depth", None, "tile", None),
            P("tile", None, None),
            P("tile", None, None),
            P(),
            P("depth"),
        ),
        out_specs=P("tile", "depth", None, None),
        check_vma=False,
    )
```
